32 devices in a mesh: dp: 1 (over z), dcp: 32 (over y, x, core).
Axes of the slice: x: 4, y: 4, z: 1, core: 2. Of those that a mesh axis runs over, the one named last changes fastest.
The devices are a block of a 4x4x8 slice.
Arguments:
- q_abs: bfloat16 [128, 128, 576], P('dp', 'dcp')
- latent_cache: bfloat16 [128, 1, 32, 256, 576], P('dp', None, 'dcp')
- ctx_len: int32 [128], P('dp')
Outputs:
- output: bfloat16 [128, 128, 512], P(('dp', 'dcp'))
All inputs are finite; a program needn't handle non-finite values.
Results may differ from the reference program's by a relative error of at most 0.0061068.
Values are sent between devices in bfloat16 or wider.
A program may use at most 768 MiB of HBM per device.

```python
import math
import jax
import jax.numpy as jnp
from jax import lax

BATCH_SIZE = 128
NUM_HEADS = 128
LATENT_DIM = 512
ROPE_DIM = 64
NOPE_DIM = 128
PAGES_DEV = 1
GROUP_SIZE = 32
PAGE_LEN = 256

WIDTH = LATENT_DIM + ROPE_DIM
SEQ_LEN = PAGES_DEV * GROUP_SIZE * PAGE_LEN


def setup_inputs(seed: int = 0, part: int = 0) -> dict:
    part_key = jax.random.fold_in(jax.random.key(seed), part)
    key_query, key_cache, key_len = jax.random.split(part_key, 3)
    qk_dim = NOPE_DIM + ROPE_DIM
    cache_rope = 1.4
    query_latent = math.sqrt(0.95 * qk_dim / LATENT_DIM)
    query_rope = math.sqrt(0.95 * qk_dim / ROPE_DIM) / cache_rope
    is_latent = jnp.arange(WIDTH) < LATENT_DIM
    query_scale = jnp.where(is_latent, query_latent, query_rope)
    cache_scale = jnp.where(is_latent, 1.0, cache_rope)
    queries = jax.random.normal(key_query, (BATCH_SIZE, NUM_HEADS, WIDTH), jnp.float32) * query_scale
    cache_vals = jax.random.normal(key_cache, (BATCH_SIZE, PAGES_DEV, GROUP_SIZE, PAGE_LEN, WIDTH), jnp.float32) * cache_scale
    len_drop = jax.random.randint(key_len, (BATCH_SIZE,), 0, SEQ_LEN // 2)
    lengths = jnp.where(jnp.arange(BATCH_SIZE) == 0, SEQ_LEN, SEQ_LEN - len_drop)
    return {'q_abs': queries.astype(jnp.bfloat16), 'latent_cache': cache_vals.astype(jnp.bfloat16), 'ctx_len': lengths.astype(jnp.int32)}


def reference(q_abs, latent_cache, ctx_len):
    inv_scale = (NOPE_DIM + ROPE_DIM) ** -0.5
    q_float = q_abs.astype(jnp.float32)
    per_device = jnp.moveaxis(latent_cache, 2, 0)
    page_base = jnp.arange(PAGES_DEV)[:, None] * (GROUP_SIZE * PAGE_LEN) + jnp.arange(PAGE_LEN)[None, :]

    def one_device(carry_in):
        dev_index, cache_blk = carry_in
        cache_float = cache_blk.astype(jnp.float32)
        scores = jnp.einsum('bhw,bjtw->bhjt', q_float, cache_float) * inv_scale
        positions = page_base + dev_index * PAGE_LEN
        is_valid = positions[None, :, :] < ctx_len[:, None, None]
        scores = jnp.where(is_valid[:, None, :, :], scores, -1e30)
        row_max = jnp.max(scores, axis=(2, 3))
        weights_exp = jnp.exp(scores - row_max[:, :, None, None])
        denom_sum = jnp.sum(weights_exp, axis=(2, 3))
        weights_low = weights_exp.astype(jnp.bfloat16).astype(jnp.float32)
        pv_sum = jnp.einsum('bhjt,bjtc->bhc', weights_low, cache_float[..., :LATENT_DIM])
        part_out = (pv_sum / denom_sum[:, :, None]).astype(jnp.bfloat16)
        part_lse = row_max + jnp.log(denom_sum)
        return part_out, part_lse

    part_outs, part_lses = lax.map(one_device, (jnp.arange(GROUP_SIZE), per_device))
    total_lse = jax.nn.logsumexp(part_lses, axis=0)
    merge_weights = jnp.exp(part_lses - total_lse[None])
    merged = jnp.sum(merge_weights[..., None] * part_outs.astype(jnp.float32), axis=0)
    return merged.astype(jnp.bfloat16)
```

```python
import functools
import math

import jax
import jax.numpy as jnp
from jax import lax
from jax.experimental import pallas as pl
from jax.experimental.pallas import tpu as pltpu
from jax.sharding import PartitionSpec as P

ROPE_DIM = 64
QK_DIM = 192
AXIS = 'dcp'
DEPTH = 3
SLICES = 4

FIRST, SECOND = 0, 1
FULL, LOW, HIGH = 0, 1, 2
GATHER = (
    (FIRST, 1, (0, 0), FULL),
    (FIRST, -1, (0, 0), FULL),
    (FIRST, 1, (-1, 0), LOW),
    (FIRST, -1, (1, 0), HIGH),
    (SECOND, 1, (0, 0), FULL),
    (SECOND, 1, (-1, 0), FULL),
    (SECOND, 1, (1, 0), FULL),
    (SECOND, 1, (2, 0), LOW),
    (SECOND, 1, (2, 0), HIGH),
    (SECOND, -1, (0, 0), FULL),
    (SECOND, -1, (-1, 0), FULL),
    (SECOND, -1, (1, 0), FULL),
    (SECOND, -1, (2, 0), LOW),
    (SECOND, -1, (2, 0), HIGH),
    (SECOND, 1, (0, -1), FULL),
    (SECOND, 1, (-1, -1), FULL),
    (SECOND, -1, (1, 1), FULL),
    (SECOND, -1, (2, 1), LOW),
    (SECOND, -1, (2, 1), HIGH),
)
REDUCE = ((2, LOW, 1), (1, HIGH, 1), (2, HIGH, -1), (-1, LOW, -1), (1, LOW, 1), (-1, HIGH, -1))


def _kernel(side, len_ref, q_ref, cache_ref, out_ref, sib_ref, q_own, q_sib, q_all, part, page, xbuf, ybuf, lse_x, lse_y,
            wgt, q_sem, page_sem, swap_send, swap_recv, qs_send, qs_recv, ag_send, ag_recv, rs_send, rs_recv, ls_send,
            ls_recv):
    nj, nt, hc, width = q_own.shape
    heads = part.shape[3]
    latent = part.shape[4]
    page_len = page.shape[3]
    half_t, half_h = nt // 2, heads // 2
    quarter_t, quarter_h = nt // 4, heads // 4

    me = lax.axis_index(AXIS)
    core = lax.rem(me, 2)
    xpos = lax.rem(me // 2, side)
    ypos = me // (2 * side)
    sibling = me + 1 - 2 * core

    def wrap(pos, step):
        return lax.rem(pos + (step + side), side)

    def neighbour(axis, half, step):
        if axis == half:
            return (ypos * side + wrap(xpos, step)) * 2 + core
        return (wrap(ypos, step) * side + xpos) * 2 + core

    def peer(dev):
        return {AXIS: dev}

    def gather_copy(j, half, idx, receive=False):
        axis, step, (df, ds), rng = GATHER[idx]
        dev = neighbour(axis, half, step)
        if receive:
            if axis == FIRST:
                df -= step
            else:
                ds -= step
        if half == 0:
            yy, xx = wrap(ypos, ds), wrap(xpos, df)
        else:
            yy, xx = wrap(ypos, df), wrap(xpos, ds)
        start = half * half_t + (quarter_t if rng == HIGH else 0)
        ref = q_all.at[j, yy, xx, pl.ds(start, half_t if rng == FULL else quarter_t)]
        return pltpu.make_async_remote_copy(
            src_ref=ref, dst_ref=ref, send_sem=ag_send.at[j, half, idx], recv_sem=ag_recv.at[j, half, idx],
            device_id=peer(dev), device_id_type=pl.DeviceIdType.MESH)

    def rows_of(half, rng):
        return half * half_h + (quarter_h if rng == HIGH else 0)

    def first_part(r, half, step, rng, i=None):
        hs = pl.ds(rows_of(half, rng), quarter_h)
        second = slice(None) if i is None else i
        if half == 0:
            return part.at[r, second, wrap(xpos, step), hs]
        return part.at[r, wrap(ypos, step), second, hs]

    def second_part(r, half, step, rng):
        hs = pl.ds(rows_of(half, rng), quarter_h)
        if half == 0:
            return part.at[r, wrap(ypos, step), xpos, hs]
        return part.at[r, ypos, wrap(xpos, step), hs]

    def reduce_copy(r, half, axis, idx):
        dest, rng, step = REDUCE[idx]
        src = (first_part if axis == FIRST else second_part)(r, half, dest, rng)
        dst = (xbuf if axis == FIRST else ybuf).at[r, half, idx]
        return pltpu.make_async_remote_copy(
            src_ref=src, dst_ref=dst, send_sem=rs_send.at[r, half, axis, idx], recv_sem=rs_recv.at[r, half, axis, idx],
            device_id=peer(neighbour(axis, half, step)), device_id_type=pl.DeviceIdType.MESH)

    def lse_copy(j, axis, idx):
        buf = lse_x if axis == 0 else lse_y
        return pltpu.make_async_remote_copy(
            src_ref=buf.at[j, 0], dst_ref=buf.at[j, idx + 1], send_sem=ls_send.at[j, axis, idx],
            recv_sem=ls_recv.at[j, axis, idx], device_id=peer(neighbour(axis, 0, (1, -1, 2)[idx])),
            device_id_type=pl.DeviceIdType.MESH)

    def swap_copy(j):
        return pltpu.make_async_remote_copy(
            src_ref=cache_ref.at[:, 1 - core, j], dst_ref=sib_ref.at[j], send_sem=swap_send.at[j],
            recv_sem=swap_recv.at[j], device_id=peer(sibling), device_id_type=pl.DeviceIdType.MESH)

    def query_swap(j):
        return pltpu.make_async_remote_copy(
            src_ref=q_ref.at[:, 1 - core, j], dst_ref=q_sib.at[j], send_sem=qs_send.at[j],
            recv_sem=qs_recv.at[j], device_id=peer(sibling), device_id_type=pl.DeviceIdType.MESH)

    def query_own(j):
        return pltpu.make_async_copy(q_ref.at[:, core, j], q_own.at[j], q_sem.at[j])

    def page_copies(j, t):
        slot = lax.rem(t, DEPTH)
        return (pltpu.make_async_copy(cache_ref.at[t, core, j], page.at[slot, 0], page_sem.at[slot, 0]),
                pltpu.make_async_copy(sib_ref.at[j, t], page.at[slot, 1], page_sem.at[slot, 1]))

    def merge_queries(j):
        query_own(j).wait()
        query_swap(j).wait_recv()
        q_all[j, ypos, xpos] = q_own[j] + q_sib[j]

    def own_sends(j):
        for idx in (0, 1, 4, 9):
            for half in (0, 1):
                gather_copy(j, half, idx).start()

    def gather_events(j, events):
        for idx, sends in events:
            for half in (0, 1):
                gather_copy(j, half, idx, receive=True).wait_recv()
                for s in sends:
                    gather_copy(j, half, s).start()

    def first_pages(j):
        swap_copy(j).wait_recv()
        for t in range(DEPTH - 1):
            for c in page_copies(j, t):
                c.start()

    def attend(j, t):
        @pl.when(t + DEPTH - 1 < nt)
        def _():
            for c in page_copies(j, t + DEPTH - 1):
                c.start()

        slot = lax.rem(t, DEPTH)
        for c in page_copies(j, t):
            c.wait()
        q = q_all[j, :, :, t].reshape(heads, width)
        limit = len_ref[(t * 2 + core) * nj + j]
        outs, lses = [], []
        for p in (0, 1):
            owner = me if p == 0 else sibling
            s = jnp.dot(q, page[slot, p], preferred_element_type=jnp.float32) * (QK_DIM ** -0.5)
            position = owner * page_len + lax.broadcasted_iota(jnp.int32, (1, page_len), 1)
            s = jnp.where(position < limit, s, -1e30)
            m = jnp.max(s, axis=1, keepdims=True)
            w = jnp.exp(s - m)
            l = jnp.sum(w, axis=1, keepdims=True)
            pv = lax.dot_general(w.astype(jnp.bfloat16), page[slot, p, :latent], (((1,), (1,)), ((), ())),
                                 preferred_element_type=jnp.float32)
            outs.append((pv * (1.0 / l)).astype(jnp.bfloat16).astype(jnp.float32))
            lses.append(m + jnp.log(l))
        top = jnp.maximum(lses[0], lses[1])
        both = top + jnp.log(jnp.exp(lses[0] - top) + jnp.exp(lses[1] - top))
        part[j, t // side, lax.rem(t, side)] = jnp.exp(lses[0] - both) * outs[0] + jnp.exp(lses[1] - both) * outs[1]
        row = jnp.broadcast_to(both, (heads, 128)).T
        lse_x[j, 0, pl.ds(t, 1), :] = row[0:1]

    def attend_slice(j, n):
        per = nt // SLICES
        lax.fori_loop(n * per, (n + 1) * per, lambda t, _: (attend(j, t), 0)[1], 0)

    def combine(v):
        top = jnp.max(v, axis=0)
        return top + jnp.log(jnp.sum(jnp.exp(v - top[None]), axis=0))

    def lse_send(j, axis):
        for idx in range(3):
            lse_copy(j, axis, idx).start()

    def lse_turn(j):
        for idx in range(3):
            lse_copy(j, 0, idx).wait_recv()
        lse_y[j, 0] = combine(lse_x[j])
        lse_send(j, 1)

    def weigh(j):
        for idx in range(3):
            lse_copy(j, 1, idx).wait_recv()
        wgt[...] = jnp.exp(lse_x[j, 0] - combine(lse_y[j]))

        def body(t, _):
            w = jnp.broadcast_to(wgt[pl.ds(t, 1), :], (128, heads)).T
            yy, xx = t // side, lax.rem(t, side)
            for i in range(latent // 128):
                cols = pl.ds(i * 128, 128)
                part[j, yy, xx, :, cols] = part[j, yy, xx, :, cols] * w
            return 0

        lax.fori_loop(0, nt, body, 0)

    def reduce_start(r, axis):
        for idx in (0, 2, 1, 3):
            for half in (0, 1):
                reduce_copy(r, half, axis, idx).start()

    def reduce_turn(r, axis):
        for idx, dest, rng, nxt in ((0, 1, LOW, 4), (2, -1, HIGH, 5)):
            for half in (0, 1):
                reduce_copy(r, half, axis, idx).wait_recv()
                if axis == FIRST:
                    def body(i, _):
                        ref = first_part(r, half, dest, rng, i)
                        ref[...] = ref[...] + xbuf[r, half, idx, i]
                        return 0
                    lax.fori_loop(0, side, body, 0)
                else:
                    ref = second_part(r, half, dest, rng)
                    ref[...] = ref[...] + ybuf[r, half, idx]
                reduce_copy(r, half, axis, nxt).start()

    def reduce_end(r, axis):
        for rng, one, two in ((HIGH, 1, 5), (LOW, 3, 4)):
            for half in (0, 1):
                reduce_copy(r, half, axis, one).wait_recv()
                reduce_copy(r, half, axis, two).wait_recv()
                if axis == FIRST:
                    def body(i, _):
                        ref = first_part(r, half, 0, rng, i)
                        ref[...] = ref[...] + (xbuf[r, half, one, i] + xbuf[r, half, two, i])
                        return 0
                    lax.fori_loop(0, side, body, 0)
                else:
                    total = second_part(r, half, 0, rng)[...] + (ybuf[r, half, one] + ybuf[r, half, two])
                    out_ref[r, pl.ds(rows_of(half, rng), quarter_h)] = total.astype(out_ref.dtype)

    for j in range(nj):
        query_own(j).start()
    barrier = pltpu.get_barrier_semaphore()
    peers = [sibling] + [neighbour(axis, 0, step) for axis in (0, 1) for step in (1, -1, 2)]
    for dev in peers:
        pl.semaphore_signal(barrier, inc=1, device_id=peer(dev), device_id_type=pl.DeviceIdType.MESH)
    pl.semaphore_wait(barrier, len(peers))

    for j in range(nj):
        query_swap(j).start()
    for j in range(nj):
        swap_copy(j).start()
    merge_queries(0)
    own_sends(0)
    lax.fori_loop(1, nj, lambda j, _: (merge_queries(j), 0)[1], 0)

    def stage(k, _):
        def when(lag, fn, *args):
            pl.when((k >= lag) & (k < nj + lag))(lambda: fn(k - lag, *args))

        when(-1, own_sends)
        when(1, first_pages)
        when(0, gather_events, ((0, (2, 5, 10)), (1, (3, 6, 11))))
        when(1, attend_slice, 0)
        when(2, lse_turn)
        when(0, gather_events, ((2, (7, 12)), (3, (8, 13)), (4, (14,)), (9, ())))
        when(1, attend_slice, 1)
        when(0, gather_events, ((5, (15,)), (11, (16,)), (10, ()), (6, ())))
        when(4, reduce_turn, FIRST)
        when(5, reduce_turn, SECOND)
        when(3, weigh)
        when(3, reduce_start, FIRST)
        when(1, attend_slice, 2)
        when(0, gather_events, ((12, (17,)), (13, (18,)), (7, ()), (8, ())))
        when(1, attend_slice, 3)
        when(1, lse_send, 0)
        when(0, gather_events, ((14, ()), (15, ()), (16, ()), (17, ()), (18, ())))
        when(4, reduce_end, FIRST)
        when(4, reduce_start, SECOND)
        when(5, reduce_end, SECOND)
        return 0

    lax.fori_loop(0, nj + 5, stage, 0)

    def drain(j, _):
        swap_copy(j).wait_send()
        query_swap(j).wait_send()
        for half in (0, 1):
            for idx in range(len(GATHER)):
                gather_copy(j, half, idx).wait_send()
            for axis in (0, 1):
                for idx in range(len(REDUCE)):
                    reduce_copy(j, half, axis, idx).wait_send()
        for axis in (0, 1):
            for idx in range(3):
                lse_copy(j, axis, idx).wait_send()
        return 0

    lax.fori_loop(0, nj, drain, 0)


def solution(mesh):
    group_size = mesh.shape[AXIS]
    side = math.isqrt(group_size // 2)
    nt = side * side

    def local_step(q_blk, cache_blk, len_blk):
        batch_rows, own_heads, width = q_blk.shape
        page_len = cache_blk.shape[3]
        latent = width - ROPE_DIM
        nj = batch_rows // group_size
        hc = 2 * own_heads
        heads = hc * nt
        core = lax.rem(lax.axis_index(AXIS), 2)
        q = q_blk.reshape(nt, 2, nj, own_heads, width)
        zero = jnp.zeros_like(q)
        q = jnp.concatenate([jnp.where(core == 0, q, zero), jnp.where(core == 1, q, zero)], axis=3)
        cache = jnp.swapaxes(cache_blk.reshape(nt, 2, nj, page_len, width), 3, 4)
        any_space = pl.BlockSpec(memory_space=pl.ANY)
        dma = pltpu.SemaphoreType.DMA
        out, _ = pl.pallas_call(
            functools.partial(_kernel, side),
            out_shape=(jax.ShapeDtypeStruct((nj, heads, latent), jnp.bfloat16),
                       jax.ShapeDtypeStruct((nj, nt, width, page_len), jnp.bfloat16)),
            in_specs=[pl.BlockSpec(memory_space=pltpu.SMEM), any_space, any_space],
            out_specs=(pl.BlockSpec(memory_space=pltpu.VMEM), any_space),
            scratch_shapes=[
                pltpu.VMEM((nj, nt, hc, width), jnp.bfloat16),
                pltpu.VMEM((nj, nt, hc, width), jnp.bfloat16),
                pltpu.VMEM((nj, side, side, nt, hc, width), jnp.bfloat16),
                pltpu.VMEM((nj, side, side, heads, latent), jnp.float32),
                pltpu.VMEM((DEPTH, 2, width, page_len), jnp.bfloat16),
                pltpu.VMEM((nj, 2, len(REDUCE), side, heads // 4, latent), jnp.float32),
                pltpu.VMEM((nj, 2, len(REDUCE), heads // 4, latent), jnp.float32),
                pltpu.VMEM((nj, 4, nt, heads), jnp.float32),
                pltpu.VMEM((nj, 4, nt, heads), jnp.float32),
                pltpu.VMEM((nt, heads), jnp.float32),
                dma((nj,)), dma((DEPTH, 2)), dma((nj,)), dma((nj,)), dma((nj,)), dma((nj,)),
                dma((nj, 2, len(GATHER))), dma((nj, 2, len(GATHER))),
                dma((nj, 2, 2, len(REDUCE))), dma((nj, 2, 2, len(REDUCE))),
                dma((nj, 2, 3)), dma((nj, 2, 3)),
            ],
            compiler_params=pltpu.CompilerParams(collective_id=0, has_side_effects=True, vmem_limit_bytes=66_000_000),
        )(len_blk, q, cache)
        return out

    return jax.shard_map(local_step, mesh=mesh, in_specs=(P('dp', AXIS, None), P('dp', None, AXIS, None, None), P('dp')),
                         out_specs=P(('dp', AXIS), None, None), check_vma=False)
```

```python
import functools
import math

import jax
import jax.numpy as jnp
from jax import lax
from jax.experimental import pallas as pl
from jax.experimental.pallas import tpu as pltpu
from jax.sharding import PartitionSpec as P

ROPE_DIM = 64
QK_DIM = 192
AXIS = 'dcp'
DEPTH = 3
SLICES = 4

FIRST, SECOND = 0, 1
FULL, LOW, HIGH = 0, 1, 2
GATHER = (
    (FIRST, 1, (0, 0), FULL, 0),
    (FIRST, -1, (0, 0), FULL, 1),
    (FIRST, 1, (-1, 0), LOW, 2),
    (FIRST, -1, (1, 0), HIGH, 2),
    (SECOND, 1, (0, 0), FULL, 3),
    (SECOND, 1, (-1, 0), FULL, 4),
    (SECOND, 1, (1, 0), FULL, 7),
    (SECOND, 1, (2, 0), FULL, 7),
    (SECOND, -1, (0, 0), FULL, 7),
    (SECOND, -1, (-1, 0), FULL, 7),
    (SECOND, -1, (1, 0), FULL, 5),
    (SECOND, -1, (2, 0), FULL, 6),
    (SECOND, 1, (0, -1), FULL, 7),
    (SECOND, 1, (-1, -1), FULL, 7),
    (SECOND, -1, (1, 1), FULL, 7),
    (SECOND, -1, (2, 1), FULL, 7),
)
REDUCE = ((2, LOW, 1, 0), (1, HIGH, 1, 2), (2, HIGH, -1, 1), (-1, LOW, -1, 2), (1, LOW, 1, 2), (-1, HIGH, -1, 2))


def _kernel(side, len_ref, q_ref, cache_ref, out_ref, sib_ref, q_own, q_sib, q_all, part, page, xbuf, ybuf, lse_x, lse_y,
            wgt, q_sem, page_sem, swap_send, swap_recv, qs_send, qs_recv, ag_send, ag_recv, rs_send, rs_recv, ls_send,
            ls_recv):
    nj, nt, own_heads, width = q_own.shape
    heads, latent = part.shape[3:]
    page_len = page.shape[3]
    half_h, quarter_h = heads // 2, heads // 4
    tiles = q_all.shape[3]
    quarter_q, half_q = tiles // 4, tiles // 2
    columns = latent // 128

    me = lax.axis_index(AXIS)
    core = lax.rem(me, 2)
    xpos = lax.rem(me // 2, side)
    ypos = me // (2 * side)
    sibling = me + 1 - 2 * core

    def wrap(pos, step):
        return lax.rem(pos + (step + side), side)

    def neighbour(axis, half, step):
        if axis == half:
            return (ypos * side + wrap(xpos, step)) * 2 + core
        return (wrap(ypos, step) * side + xpos) * 2 + core

    def peer(dev):
        return {AXIS: dev}

    def remote(ref, dst, send_sem, recv_sem, dev):
        return pltpu.make_async_remote_copy(src_ref=ref, dst_ref=dst, send_sem=send_sem, recv_sem=recv_sem,
                                            device_id=peer(dev), device_id_type=pl.DeviceIdType.MESH)

    def gather_block(j, half, first, second, rng):
        if half == 0:
            yy, xx = wrap(ypos, second), wrap(xpos, first)
        else:
            yy, xx = wrap(ypos, first), wrap(xpos, second)
        start = half * half_q + (quarter_q if rng == HIGH else 0)
        return q_all.at[j, yy, xx, pl.ds(start, half_q if rng == FULL else quarter_q)]

    def gather_send(j, *indices):
        for idx in indices:
            for half in (0, 1):
                axis, step, (first, second), rng, sem = GATHER[idx]
                ref = gather_block(j, half, first, second, rng)
                remote(ref, ref, ag_send.at[j, 0 if rng == FULL else 1], ag_recv.at[j, half, sem],
                       neighbour(axis, half, step)).start()

    def wait_bytes(ref, sem):
        pltpu.make_async_copy(ref, ref, sem).wait()

    def gather_wait(j, half, sem):
        ref = q_all.at[j, 0] if sem == 7 else gather_block(j, half, 0, 0, FULL)
        wait_bytes(ref, ag_recv.at[j, half, sem])

    def rows_of(half, rng):
        return half * half_h + (quarter_h if rng == HIGH else 0)

    def first_part(r, half, step, rng, i=None):
        hs = pl.ds(rows_of(half, rng), quarter_h)
        second = slice(None) if i is None else i
        if half == 0:
            return part.at[r, second, wrap(xpos, step), hs]
        return part.at[r, wrap(ypos, step), second, hs]

    def second_part(r, half, step, rng):
        hs = pl.ds(rows_of(half, rng), quarter_h)
        if half == 0:
            return part.at[r, wrap(ypos, step), xpos, hs]
        return part.at[r, ypos, wrap(xpos, step), hs]

    def reduce_send(r, axis, *indices):
        for idx in indices:
            for half in (0, 1):
                dest, rng, step, sem = REDUCE[idx]
                src = (first_part if axis == FIRST else second_part)(r, half, dest, rng)
                dst = (xbuf if axis == FIRST else ybuf).at[r, half, idx]
                remote(src, dst, rs_send.at[r, axis], rs_recv.at[r, half, axis, sem], neighbour(axis, half, step)).start()

    def reduce_wait(r, axis, half, sem):
        buf = xbuf if axis == FIRST else ybuf
        wait_bytes(buf.at[r, half, pl.ds(0, 4)] if sem == 2 else buf.at[r, half, 0], rs_recv.at[r, half, axis, sem])

    def lse_buf(axis):
        return lse_x if axis == 0 else lse_y

    def lse_send(j, axis):
        buf = lse_buf(axis)
        for idx, step in enumerate((1, -1, 2)):
            remote(buf.at[j, 0], buf.at[j, idx + 1], ls_send.at[j, axis], ls_recv.at[j, axis], neighbour(axis, 0, step)).start()

    def lse_wait(j, axis):
        wait_bytes(lse_buf(axis).at[j, pl.ds(0, 3)], ls_recv.at[j, axis])

    def swap_copy(j):
        return remote(cache_ref.at[:, 1 - core, j], sib_ref.at[j], swap_send.at[j], swap_recv.at[j], sibling)

    def query_swap(j):
        return remote(q_ref.at[:, 1 - core, j], q_sib.at[j], qs_send.at[j], qs_recv.at[j], sibling)

    def query_own(j):
        return pltpu.make_async_copy(q_ref.at[:, core, j], q_own.at[j], q_sem.at[j])

    def load_pages(j, t):
        slot = lax.rem(t, DEPTH)
        for p, src in ((0, cache_ref.at[t, core, j]), (1, sib_ref.at[j, t])):
            pltpu.make_async_copy(src, page.at[slot, p, pl.ds(0, width)], page_sem.at[slot, p]).start()
            pltpu.make_async_copy(src.at[pl.ds(latent, ROPE_DIM)], page.at[slot, p, pl.ds(width, ROPE_DIM)],
                                  page_sem.at[slot, p]).start()

    def merge_queries(j):
        query_own(j).wait()
        query_swap(j).wait_recv()
        for t in range(nt):
            mine = q_own[j, t].astype(jnp.float32)
            other = q_sib[j, t].astype(jnp.float32)
            both = jnp.concatenate([jnp.where(core == 0, mine, other), jnp.where(core == 0, other, mine)], axis=0)
            base, sub = (t // 4) * quarter_q, t % 4
            for i in range(columns):
                q_all[j, ypos, xpos, base + sub * columns + i] = both[:, i * 128:(i + 1) * 128].astype(jnp.bfloat16)
            rope = both[:, latent:]
            if sub < 2:
                low = (low if sub else []) + [rope]
            else:
                q_all[j, ypos, xpos, base + 4 * columns + sub - 2] = jnp.concatenate([low[sub - 2], rope], axis=1).astype(
                    jnp.bfloat16)

    def gather_first(j):
        for sem, sends in ((0, (2, 5, 9)), (1, (3, 6, 10))):
            for half in (0, 1):
                gather_wait(j, half, sem)
            gather_send(j, *sends)

    def gather_turn(j):
        for half in (0, 1):
            gather_wait(j, half, 2)
        gather_send(j, 7, 11)

    def gather_second(j):
        for sem, send in ((3, 12), (5, 14), (4, 13), (6, 15)):
            for half in (0, 1):
                gather_wait(j, half, sem)
            gather_send(j, send)

    def gather_end(j):
        for half in (0, 1):
            gather_wait(j, half, 7)

    def first_pages(j):
        swap_copy(j).wait_recv()
        for t in range(DEPTH - 1):
            load_pages(j, t)

    def attend(j, t):
        @pl.when(t + DEPTH - 1 < nt)
        def _():
            load_pages(j, t + DEPTH - 1)

        slot = lax.rem(t, DEPTH)
        for p in (0, 1):
            wait_bytes(page.at[slot, p], page_sem.at[slot, p])
        base, sub = (t // 4) * quarter_q, lax.rem(t, 4)
        cols = [q_all[j, :, :, base + sub * columns + i].reshape(heads, 128) for i in range(columns)]
        rope = q_all[j, :, :, base + 4 * columns + lax.rem(sub, 2)].reshape(heads, 128)
        lane_half = lax.broadcasted_iota(jnp.int32, (heads, 128), 1) // ROPE_DIM
        cols.append(jnp.where(lane_half == sub // 2, rope, jnp.zeros_like(rope)))
        q = jnp.concatenate(cols, axis=1)
        limit = len_ref[(t * 2 + core) * nj + j]
        outs, lses = [], []
        for p in (0, 1):
            owner = me if p == 0 else sibling
            s = jnp.dot(q, page[slot, p], preferred_element_type=jnp.float32) * (QK_DIM ** -0.5)
            position = owner * page_len + lax.broadcasted_iota(jnp.int32, (1, page_len), 1)
            s = jnp.where(position < limit, s, -1e30)
            m = jnp.max(s, axis=1, keepdims=True)
            w = jnp.exp(s - m)
            l = jnp.sum(w, axis=1, keepdims=True)
            pv = lax.dot_general(w.astype(jnp.bfloat16), page[slot, p, :latent], (((1,), (1,)), ((), ())),
                                 preferred_element_type=jnp.float32)
            outs.append((pv * (1.0 / l)).astype(jnp.bfloat16).astype(jnp.float32))
            lses.append(m + jnp.log(l))
        top = jnp.maximum(lses[0], lses[1])
        both = top + jnp.log(jnp.exp(lses[0] - top) + jnp.exp(lses[1] - top))
        part[j, t // side, lax.rem(t, side)] = jnp.exp(lses[0] - both) * outs[0] + jnp.exp(lses[1] - both) * outs[1]
        row = jnp.broadcast_to(both, (heads, 128)).T
        lse_x[j, 0, pl.ds(t, 1), :] = row[0:1]

    def attend_slice(j, n):
        per = nt // SLICES
        lax.fori_loop(n * per, (n + 1) * per, lambda t, _: (attend(j, t), 0)[1], 0)

    def combine(v):
        top = jnp.max(v, axis=0)
        return top + jnp.log(jnp.sum(jnp.exp(v - top[None]), axis=0))

    def lse_turn(j):
        lse_wait(j, 0)
        lse_y[j, 0] = combine(lse_x[j])
        lse_send(j, 1)

    def weigh(j):
        lse_wait(j, 1)
        wgt[...] = jnp.exp(lse_x[j, 0] - combine(lse_y[j]))

        def body(t, _):
            w = jnp.broadcast_to(wgt[pl.ds(t, 1), :], (128, heads)).T
            yy, xx = t // side, lax.rem(t, side)
            for i in range(latent // 128):
                cols = pl.ds(i * 128, 128)
                part[j, yy, xx, :, cols] = part[j, yy, xx, :, cols] * w
            return 0

        lax.fori_loop(0, nt, body, 0)

    def reduce_start(r, axis):
        reduce_send(r, axis, 0, 2, 1, 3)

    def reduce_turn(r, axis):
        for idx, dest, rng, nxt, sem in ((0, 1, LOW, 4, 0), (2, -1, HIGH, 5, 1)):
            for half in (0, 1):
                reduce_wait(r, axis, half, sem)
                if axis == FIRST:
                    def body(i, _):
                        ref = first_part(r, half, dest, rng, i)
                        ref[...] = ref[...] + xbuf[r, half, idx, i]
                        return 0
                    lax.fori_loop(0, side, body, 0)
                else:
                    ref = second_part(r, half, dest, rng)
                    ref[...] = ref[...] + ybuf[r, half, idx]
            reduce_send(r, axis, nxt)

    def reduce_end(r, axis):
        for half in (0, 1):
            reduce_wait(r, axis, half, 2)
            for rng, one, two in ((HIGH, 1, 5), (LOW, 3, 4)):
                if axis == FIRST:
                    def body(i, _):
                        ref = first_part(r, half, 0, rng, i)
                        ref[...] = ref[...] + (xbuf[r, half, one, i] + xbuf[r, half, two, i])
                        return 0
                    lax.fori_loop(0, side, body, 0)
                else:
                    total = second_part(r, half, 0, rng)[...] + (ybuf[r, half, one] + ybuf[r, half, two])
                    out_ref[r, pl.ds(rows_of(half, rng), quarter_h)] = total.astype(out_ref.dtype)

    for j in range(nj):
        query_own(j).start()
    barrier = pltpu.get_barrier_semaphore()
    peers = [sibling] + [neighbour(axis, 0, step) for axis in (0, 1) for step in (1, -1, 2)]
    for dev in peers:
        pl.semaphore_signal(barrier, inc=1, device_id=peer(dev), device_id_type=pl.DeviceIdType.MESH)
    pl.semaphore_wait(barrier, len(peers))

    for j in range(nj):
        query_swap(j).start()
    for j in range(nj):
        swap_copy(j).start()
    with jax.named_scope('merge0'):
        merge_queries(0)
    gather_send(0, 0, 1, 4, 8)
    with jax.named_scope('merges'):
        lax.fori_loop(1, nj, lambda j, _: (merge_queries(j), 0)[1], 0)

    def stage(k, _):
        def when(lag, fn, *args):
            def run():
                with jax.named_scope(fn.__name__ + '_'.join(str(a) for a in args)):
                    fn(k - 1 - lag, *args)
            pl.when((k > lag) & (k <= nj + lag))(run)

        when(0, gather_second)
        when(1, first_pages)
        when(-2, gather_send, 0, 1)
        when(-1, gather_first)
        when(-2, gather_send, 4, 8)
        when(4, reduce_turn, FIRST)
        when(5, reduce_turn, SECOND)
        when(3, weigh)
        when(3, reduce_start, FIRST)
        when(1, attend_slice, 0)
        when(2, lse_turn)
        when(1, attend_slice, 1)
        when(-1, gather_turn)
        when(1, attend_slice, 2)
        when(1, attend_slice, 3)
        when(1, lse_send, 0)
        when(0, gather_end)
        when(4, reduce_end, FIRST)
        when(4, reduce_start, SECOND)
        when(5, reduce_end, SECOND)
        return 0

    lax.fori_loop(0, nj + 6, stage, 0)

    def drain(j, _):
        swap_copy(j).wait_send()
        query_swap(j).wait_send()
        wait_bytes(q_all.at[j, :, :, pl.ds(0, 14 * tiles // 16)], ag_send.at[j, 0])
        wait_bytes(q_all.at[j, 0, 0], ag_send.at[j, 1])
        wait_bytes(xbuf.at[j], rs_send.at[j, 0])
        wait_bytes(ybuf.at[j], rs_send.at[j, 1])
        for axis in (0, 1):
            wait_bytes(lse_buf(axis).at[j, pl.ds(0, 3)], ls_send.at[j, axis])
        return 0

    with jax.named_scope('drain'):
        lax.fori_loop(0, nj, drain, 0)


def solution(mesh):
    group_size = mesh.shape[AXIS]
    side = math.isqrt(group_size // 2)
    nt = side * side

    def local_step(q_blk, cache_blk, len_blk):
        batch_rows, own_heads, width = q_blk.shape
        page_len = cache_blk.shape[3]
        latent = width - ROPE_DIM
        nj = batch_rows // group_size
        heads = 2 * own_heads * nt
        tiles = nt * (latent // 128) + nt // 2
        q = q_blk.reshape(nt, 2, nj, own_heads, width)
        cache = jnp.swapaxes(cache_blk.reshape(nt, 2, nj, page_len, width), 3, 4)
        any_space = pl.BlockSpec(memory_space=pl.ANY)
        dma = pltpu.SemaphoreType.DMA
        out, _ = pl.pallas_call(
            functools.partial(_kernel, side),
            out_shape=(jax.ShapeDtypeStruct((nj, heads, latent), jnp.bfloat16),
                       jax.ShapeDtypeStruct((nj, nt, width, page_len), jnp.bfloat16)),
            in_specs=[pl.BlockSpec(memory_space=pltpu.SMEM), any_space, any_space],
            out_specs=(pl.BlockSpec(memory_space=pltpu.VMEM), any_space),
            scratch_shapes=[
                pltpu.VMEM((nj, nt, own_heads, width), jnp.bfloat16),
                pltpu.VMEM((nj, nt, own_heads, width), jnp.bfloat16),
                pltpu.VMEM((nj, side, side, tiles, 2 * own_heads, 128), jnp.bfloat16),
                pltpu.VMEM((nj, side, side, heads, latent), jnp.float32),
                pltpu.VMEM((DEPTH, 2, width + ROPE_DIM, page_len), jnp.bfloat16),
                pltpu.VMEM((nj, 2, len(REDUCE), side, heads // 4, latent), jnp.float32),
                pltpu.VMEM((nj, 2, len(REDUCE), heads // 4, latent), jnp.float32),
                pltpu.VMEM((nj, 4, nt, heads), jnp.float32),
                pltpu.VMEM((nj, 4, nt, heads), jnp.float32),
                pltpu.VMEM((nt, heads), jnp.float32),
                dma((nj,)), dma((DEPTH, 2)), dma((nj,)), dma((nj,)), dma((nj,)), dma((nj,)),
                dma((nj, 2)), dma((nj, 2, 8)), dma((nj, 2)), dma((nj, 2, 2, 3)), dma((nj, 2)), dma((nj, 2)),
            ],
            compiler_params=pltpu.CompilerParams(collective_id=0, has_side_effects=True, vmem_limit_bytes=66_000_000),
        )(len_blk, q, cache)
        return out

    return jax.shard_map(local_step, mesh=mesh, in_specs=(P('dp', AXIS, None), P('dp', None, AXIS, None, None), P('dp')),
                         out_specs=P(('dp', AXIS), None, None), check_vma=False)
```

```python
import functools
import math

import jax
import jax.numpy as jnp
from jax import lax
from jax.experimental import pallas as pl
from jax.experimental.pallas import tpu as pltpu
from jax.sharding import PartitionSpec as P

ROPE_DIM = 64
QK_DIM = 192
AXIS = 'dcp'
DEPTH = 3
SLICES = 4

FIRST, SECOND = 0, 1
FULL, LOW, HIGH = 0, 1, 2
GATHER = (
    (FIRST, 1, (0, 0), FULL, 0),
    (FIRST, -1, (0, 0), FULL, 1),
    (FIRST, 1, (-1, 0), LOW, 2),
    (FIRST, -1, (1, 0), HIGH, 2),
    (SECOND, 1, (0, 0), FULL, 3),
    (SECOND, 1, (-1, 0), FULL, 4),
    (SECOND, 1, (1, 0), FULL, 7),
    (SECOND, 1, (2, 0), FULL, 7),
    (SECOND, -1, (0, 0), FULL, 7),
    (SECOND, -1, (-1, 0), FULL, 7),
    (SECOND, -1, (1, 0), FULL, 5),
    (SECOND, -1, (2, 0), FULL, 6),
    (SECOND, 1, (0, -1), FULL, 7),
    (SECOND, 1, (-1, -1), FULL, 7),
    (SECOND, -1, (1, 1), FULL, 7),
    (SECOND, -1, (2, 1), FULL, 7),
)
REDUCE = ((2, LOW, 1, 0), (1, HIGH, 1, 2), (2, HIGH, -1, 1), (-1, LOW, -1, 2), (1, LOW, 1, 2), (-1, HIGH, -1, 2))


def _kernel(side, len_ref, q_ref, cache_ref, out_ref, sib_ref, q_sib, q_all, part, page, xbuf, ybuf, lse_x, lse_y,
            wgt, page_sem, swap_send, swap_recv, qs_send, qs_recv, ag_send, ag_recv, rs_send, rs_recv, ls_send,
            ls_recv):
    nt, nj, own_heads, width = q_sib.shape
    heads, latent = part.shape[3:]
    page_len = page.shape[3]
    half_h, quarter_h = heads // 2, heads // 4
    tiles = q_all.shape[3]
    quarter_q, half_q = tiles // 4, tiles // 2
    columns = latent // 128

    me = lax.axis_index(AXIS)
    core = lax.rem(me, 2)
    xpos = lax.rem(me // 2, side)
    ypos = me // (2 * side)
    sibling = me + 1 - 2 * core

    def wrap(pos, step):
        return lax.rem(pos + (step + side), side)

    def neighbour(axis, half, step):
        if axis == half:
            return (ypos * side + wrap(xpos, step)) * 2 + core
        return (wrap(ypos, step) * side + xpos) * 2 + core

    def peer(dev):
        return {AXIS: dev}

    def remote(ref, dst, send_sem, recv_sem, dev):
        return pltpu.make_async_remote_copy(src_ref=ref, dst_ref=dst, send_sem=send_sem, recv_sem=recv_sem,
                                            device_id=peer(dev), device_id_type=pl.DeviceIdType.MESH)

    def gather_block(j, half, first, second, rng):
        if half == 0:
            yy, xx = wrap(ypos, second), wrap(xpos, first)
        else:
            yy, xx = wrap(ypos, first), wrap(xpos, second)
        start = half * half_q + (quarter_q if rng == HIGH else 0)
        return q_all.at[j, yy, xx, pl.ds(start, half_q if rng == FULL else quarter_q)]

    def gather_send(j, *indices):
        for idx in indices:
            for half in (0, 1):
                axis, step, (first, second), rng, sem = GATHER[idx]
                ref = gather_block(j, half, first, second, rng)
                remote(ref, ref, ag_send.at[j, 0 if rng == FULL else 1], ag_recv.at[j, half, sem],
                       neighbour(axis, half, step)).start()

    def wait_bytes(ref, sem):
        pltpu.make_async_copy(ref, ref, sem).wait()

    def gather_wait(j, half, sem):
        ref = q_all.at[j, 0] if sem == 7 else gather_block(j, half, 0, 0, FULL)
        wait_bytes(ref, ag_recv.at[j, half, sem])

    def rows_of(half, rng):
        return half * half_h + (quarter_h if rng == HIGH else 0)

    def first_part(r, half, step, rng, i=None):
        hs = pl.ds(rows_of(half, rng), quarter_h)
        second = slice(None) if i is None else i
        if half == 0:
            return part.at[r, second, wrap(xpos, step), hs]
        return part.at[r, wrap(ypos, step), second, hs]

    def second_part(r, half, step, rng):
        hs = pl.ds(rows_of(half, rng), quarter_h)
        if half == 0:
            return part.at[r, wrap(ypos, step), xpos, hs]
        return part.at[r, ypos, wrap(xpos, step), hs]

    def reduce_send(r, axis, *indices):
        for idx in indices:
            for half in (0, 1):
                dest, rng, step, sem = REDUCE[idx]
                src = (first_part if axis == FIRST else second_part)(r, half, dest, rng)
                dst = (xbuf if axis == FIRST else ybuf).at[r, half, idx]
                remote(src, dst, rs_send.at[r, axis], rs_recv.at[r, half, axis, sem], neighbour(axis, half, step)).start()

    def reduce_wait(r, axis, half, sem):
        buf = xbuf if axis == FIRST else ybuf
        wait_bytes(buf.at[r, half, pl.ds(0, 4)] if sem == 2 else buf.at[r, half, 0], rs_recv.at[r, half, axis, sem])

    def lse_buf(axis):
        return lse_x if axis == 0 else lse_y

    def lse_send(j, axis):
        buf = lse_buf(axis)
        for idx, step in enumerate((1, -1, 2)):
            remote(buf.at[j, 0], buf.at[j, idx + 1], ls_send.at[j, axis], ls_recv.at[j, axis], neighbour(axis, 0, step)).start()

    def lse_wait(j, axis):
        wait_bytes(lse_buf(axis).at[j, pl.ds(0, 3)], ls_recv.at[j, axis])

    def swap_copy(j):
        return remote(cache_ref.at[:, 1 - core, j], sib_ref.at[j], swap_send.at[j], swap_recv.at[j], sibling)

    def query_swap():
        return remote(q_ref.at[:, 1 - core], q_sib, qs_send, qs_recv, sibling)

    def load_pages(j, t):
        slot = lax.rem(t, DEPTH)
        for p, src in ((0, cache_ref.at[t, core, j]), (1, sib_ref.at[j, t])):
            pltpu.make_async_copy(src, page.at[slot, p, pl.ds(0, width)], page_sem.at[slot, p]).start()
            pltpu.make_async_copy(src.at[pl.ds(latent, ROPE_DIM)], page.at[slot, p, pl.ds(width, ROPE_DIM)],
                                  page_sem.at[slot, p]).start()

    def merge_queries(j):
        for t in range(nt):
            mine = q_ref[t, core, j].astype(jnp.float32)
            other = q_sib[t, j].astype(jnp.float32)
            both = jnp.concatenate([jnp.where(core == 0, mine, other), jnp.where(core == 0, other, mine)], axis=0)
            base, sub = (t // 4) * quarter_q, t % 4
            for i in range(columns):
                q_all[j, ypos, xpos, base + sub * columns + i] = both[:, i * 128:(i + 1) * 128].astype(jnp.bfloat16)
            rope = both[:, latent:]
            if sub < 2:
                low = (low if sub else []) + [rope]
            else:
                q_all[j, ypos, xpos, base + 4 * columns + sub - 2] = jnp.concatenate([low[sub - 2], rope], axis=1).astype(
                    jnp.bfloat16)

    def gather_first(j):
        for sem, sends in ((0, (2, 5, 9)), (1, (3, 6, 10))):
            for half in (0, 1):
                gather_wait(j, half, sem)
            gather_send(j, *sends)

    def gather_turn(j):
        for half in (0, 1):
            gather_wait(j, half, 2)
        gather_send(j, 7, 11)

    def gather_second(j, sem, send):
        for half in (0, 1):
            gather_wait(j, half, sem)
        gather_send(j, send)

    def gather_end(j):
        for half in (0, 1):
            gather_wait(j, half, 7)

    def first_pages(j):
        swap_copy(j).wait_recv()
        for t in range(DEPTH - 1):
            load_pages(j, t)

    def attend(j, t):
        @pl.when(t + DEPTH - 1 < nt)
        def _():
            load_pages(j, t + DEPTH - 1)

        slot = lax.rem(t, DEPTH)
        for p in (0, 1):
            wait_bytes(page.at[slot, p], page_sem.at[slot, p])
        base, sub = (t // 4) * quarter_q, lax.rem(t, 4)
        cols = [q_all[j, :, :, base + sub * columns + i].reshape(heads, 128) for i in range(columns)]
        rope = q_all[j, :, :, base + 4 * columns + lax.rem(sub, 2)].reshape(heads, 128)
        lane_half = lax.broadcasted_iota(jnp.int32, (heads, 128), 1) // ROPE_DIM
        cols.append(jnp.where(lane_half == sub // 2, rope, jnp.zeros_like(rope)))
        q = jnp.concatenate(cols, axis=1)
        limit = len_ref[(t * 2 + core) * nj + j]
        outs, lses = [], []
        for p in (0, 1):
            owner = me if p == 0 else sibling
            s = jnp.dot(q, page[slot, p], preferred_element_type=jnp.float32) * (QK_DIM ** -0.5)
            position = owner * page_len + lax.broadcasted_iota(jnp.int32, (1, page_len), 1)
            s = jnp.where(position < limit, s, -1e30)
            m = jnp.max(s, axis=1, keepdims=True)
            w = jnp.exp(s - m)
            l = jnp.sum(w, axis=1, keepdims=True)
            pv = lax.dot_general(w.astype(jnp.bfloat16), page[slot, p, :latent], (((1,), (1,)), ((), ())),
                                 preferred_element_type=jnp.float32)
            outs.append((pv * (1.0 / l)).astype(jnp.bfloat16).astype(jnp.float32))
            lses.append(m + jnp.log(l))
        top = jnp.maximum(lses[0], lses[1])
        both = top + jnp.log(jnp.exp(lses[0] - top) + jnp.exp(lses[1] - top))
        part[j, t // side, lax.rem(t, side)] = jnp.exp(lses[0] - both) * outs[0] + jnp.exp(lses[1] - both) * outs[1]
        row = jnp.broadcast_to(both, (heads, 128)).T
        lse_x[j, 0, pl.ds(t, 1), :] = row[0:1]

    def attend_slice(j, n):
        per = nt // SLICES
        lax.fori_loop(n * per, (n + 1) * per, lambda t, _: (attend(j, t), 0)[1], 0)

    def combine(v):
        top = jnp.max(v, axis=0)
        return top + jnp.log(jnp.sum(jnp.exp(v - top[None]), axis=0))

    def lse_turn(j):
        lse_wait(j, 0)
        lse_y[j, 0] = combine(lse_x[j])
        lse_send(j, 1)

    def weigh(j):
        lse_wait(j, 1)
        wgt[...] = jnp.exp(lse_x[j, 0] - combine(lse_y[j]))

        def body(t, _):
            w = jnp.broadcast_to(wgt[pl.ds(t, 1), :], (128, heads)).T
            yy, xx = t // side, lax.rem(t, side)
            for i in range(latent // 128):
                cols = pl.ds(i * 128, 128)
                part[j, yy, xx, :, cols] = part[j, yy, xx, :, cols] * w
            return 0

        lax.fori_loop(0, nt, body, 0)

    def reduce_start(r, axis):
        reduce_send(r, axis, 0, 2, 1, 3)

    def reduce_turn(r, axis):
        for idx, dest, rng, nxt, sem in ((0, 1, LOW, 4, 0), (2, -1, HIGH, 5, 1)):
            for half in (0, 1):
                reduce_wait(r, axis, half, sem)
                if axis == FIRST:
                    def body(i, _):
                        ref = first_part(r, half, dest, rng, i)
                        ref[...] = ref[...] + xbuf[r, half, idx, i]
                        return 0
                    lax.fori_loop(0, side, body, 0)
                else:
                    ref = second_part(r, half, dest, rng)
                    ref[...] = ref[...] + ybuf[r, half, idx]
            reduce_send(r, axis, nxt)

    def reduce_end(r, axis):
        for half in (0, 1):
            reduce_wait(r, axis, half, 2)
            for rng, one, two in ((HIGH, 1, 5), (LOW, 3, 4)):
                if axis == FIRST:
                    def body(i, _):
                        ref = first_part(r, half, 0, rng, i)
                        ref[...] = ref[...] + (xbuf[r, half, one, i] + xbuf[r, half, two, i])
                        return 0
                    lax.fori_loop(0, side, body, 0)
                else:
                    total = second_part(r, half, 0, rng)[...] + (ybuf[r, half, one] + ybuf[r, half, two])
                    out_ref[r, pl.ds(rows_of(half, rng), quarter_h)] = total.astype(out_ref.dtype)

    barrier = pltpu.get_barrier_semaphore()
    peers = [sibling] + [neighbour(axis, 0, step) for axis in (0, 1) for step in (1, -1, 2)]
    for dev in peers:
        pl.semaphore_signal(barrier, inc=1, device_id=peer(dev), device_id_type=pl.DeviceIdType.MESH)
    with jax.named_scope('barrier'):
        pl.semaphore_wait(barrier, len(peers))

    query_swap().start()
    for j in range(nj):
        swap_copy(j).start()
    with jax.named_scope('merge0'):
        query_swap().wait_recv()
        merge_queries(0)
    gather_send(0, 0, 1, 4, 8)
    with jax.named_scope('merges'):
        lax.fori_loop(1, nj, lambda j, _: (merge_queries(j), 0)[1], 0)
    gather_send(1, 0, 1)
    with jax.named_scope('chunk0'):
        gather_first(0)
        gather_second(0, 3, 12)
        gather_second(0, 5, 14)
        gather_turn(0)
        gather_second(0, 4, 13)
        gather_send(1, 4, 8)
    with jax.named_scope('chunk1'):
        gather_first(1)
        gather_second(0, 6, 15)
        gather_send(2, 0, 1)
        gather_end(0)

    def stage(k, _):
        def when(lag, fn, *args):
            def run():
                with jax.named_scope(fn.__name__ + '_'.join(str(a) for a in args)):
                    fn(k - lag, *args)
            pl.when((k >= lag) & (k < nj + lag))(run)

        when(0, first_pages)
        when(-1, gather_turn)
        when(-1, gather_second, 3, 12)
        when(-1, gather_second, 5, 14)
        when(-1, gather_second, 4, 13)
        when(3, reduce_turn, FIRST)
        when(4, reduce_turn, SECOND)
        when(0, attend_slice, 0)
        when(1, lse_turn)
        when(2, weigh)
        when(2, reduce_start, FIRST)
        when(-2, gather_first)
        when(-2, gather_send, 4, 8)
        when(0, attend_slice, 1)
        when(-1, gather_second, 6, 15)
        when(-3, gather_send, 0, 1)
        when(0, attend_slice, 2)
        when(0, attend_slice, 3)
        when(0, lse_send, 0)
        when(-1, gather_end)
        when(3, reduce_end, FIRST)
        when(3, reduce_start, SECOND)
        when(4, reduce_end, SECOND)
        return 0

    lax.fori_loop(0, nj + 4, stage, 0)

    def drain(j, _):
        swap_copy(j).wait_send()
        wait_bytes(q_all.at[j, :, :, pl.ds(0, 14 * tiles // 16)], ag_send.at[j, 0])
        wait_bytes(q_all.at[j, 0, 0], ag_send.at[j, 1])
        wait_bytes(xbuf.at[j], rs_send.at[j, 0])
        wait_bytes(ybuf.at[j], rs_send.at[j, 1])
        for axis in (0, 1):
            wait_bytes(lse_buf(axis).at[j, pl.ds(0, 3)], ls_send.at[j, axis])
        return 0

    with jax.named_scope('drain'):
        query_swap().wait_send()
        lax.fori_loop(0, nj, drain, 0)


def solution(mesh):
    group_size = mesh.shape[AXIS]
    side = math.isqrt(group_size // 2)
    nt = side * side

    def local_step(q_blk, cache_blk, len_blk):
        batch_rows, own_heads, width = q_blk.shape
        page_len = cache_blk.shape[3]
        latent = width - ROPE_DIM
        nj = batch_rows // group_size
        heads = 2 * own_heads * nt
        tiles = nt * (latent // 128) + nt // 2
        q = q_blk.reshape(nt, 2, nj, own_heads, width)
        cache = jnp.swapaxes(cache_blk.reshape(nt, 2, nj, page_len, width), 3, 4)
        any_space = pl.BlockSpec(memory_space=pl.ANY)
        dma = pltpu.SemaphoreType.DMA
        out, _ = pl.pallas_call(
            functools.partial(_kernel, side),
            out_shape=(jax.ShapeDtypeStruct((nj, heads, latent), jnp.bfloat16),
                       jax.ShapeDtypeStruct((nj, nt, width, page_len), jnp.bfloat16)),
            in_specs=[pl.BlockSpec(memory_space=pltpu.SMEM), pl.BlockSpec(memory_space=pltpu.VMEM), any_space],
            out_specs=(pl.BlockSpec(memory_space=pltpu.VMEM), any_space),
            scratch_shapes=[
                pltpu.VMEM((nt, nj, own_heads, width), jnp.bfloat16),
                pltpu.VMEM((nj, side, side, tiles, 2 * own_heads, 128), jnp.bfloat16),
                pltpu.VMEM((nj, side, side, heads, latent), jnp.float32),
                pltpu.VMEM((DEPTH, 2, width + ROPE_DIM, page_len), jnp.bfloat16),
                pltpu.VMEM((nj, 2, len(REDUCE), side, heads // 4, latent), jnp.float32),
                pltpu.VMEM((nj, 2, len(REDUCE), heads // 4, latent), jnp.float32),
                pltpu.VMEM((nj, 4, nt, heads), jnp.float32),
                pltpu.VMEM((nj, 4, nt, heads), jnp.float32),
                pltpu.VMEM((nt, heads), jnp.float32),
                dma((DEPTH, 2)), dma((nj,)), dma((nj,)), dma(()), dma(()),
                dma((nj, 2)), dma((nj, 2, 8)), dma((nj, 2)), dma((nj, 2, 2, 3)), dma((nj, 2)), dma((nj, 2)),
            ],
            compiler_params=pltpu.CompilerParams(collective_id=0, has_side_effects=True, vmem_limit_bytes=54_000_000),
        )(len_blk, q, cache)
        return out

    return jax.shard_map(local_step, mesh=mesh, in_specs=(P('dp', AXIS, None), P('dp', None, AXIS, None, None), P('dp')),
                         out_specs=P(('dp', AXIS), None, None), check_vma=False)
```

```python
import functools
import math

import jax
import jax.numpy as jnp
from jax import lax
from jax.experimental import pallas as pl
from jax.experimental.pallas import tpu as pltpu
from jax.sharding import PartitionSpec as P

ROPE_DIM = 64
QK_DIM = 192
AXIS = 'dcp'
DEPTH = 3
SLICES = 4

FIRST, SECOND = 0, 1
FULL, LOW, HIGH = 0, 1, 2
GATHER = (
    (FIRST, 1, (0, 0), FULL, 0),
    (FIRST, -1, (0, 0), FULL, 1),
    (FIRST, 1, (-1, 0), LOW, 2),
    (FIRST, -1, (1, 0), HIGH, 2),
    (SECOND, 1, (0, 0), FULL, 3),
    (SECOND, 1, (-1, 0), FULL, 4),
    (SECOND, 1, (1, 0), FULL, 7),
    (SECOND, 1, (2, 0), FULL, 7),
    (SECOND, -1, (0, 0), FULL, 7),
    (SECOND, -1, (-1, 0), FULL, 7),
    (SECOND, -1, (1, 0), FULL, 5),
    (SECOND, -1, (2, 0), FULL, 6),
    (SECOND, 1, (0, -1), FULL, 7),
    (SECOND, 1, (-1, -1), FULL, 7),
    (SECOND, -1, (1, 1), FULL, 7),
    (SECOND, -1, (2, 1), FULL, 7),
)
REDUCE = ((2, LOW, 1, 0), (1, HIGH, 1, 2), (2, HIGH, -1, 1), (-1, LOW, -1, 2), (1, LOW, 1, 2), (-1, HIGH, -1, 2))


def _kernel(side, len_ref, q_ref, cache_ref, out_ref, sib_ref, q_sib, q_all, part, page, xbuf, ybuf, lse_x, lse_y,
            wgt, page_sem, swap_send, swap_recv, qs_send, qs_recv, ag_send, ag_recv, rs_send, rs_recv, ls_send,
            ls_recv):
    nt, nj, own_heads, width = q_sib.shape
    heads, latent = part.shape[3:]
    page_len = page.shape[3]
    half_h, quarter_h = heads // 2, heads // 4
    tiles = q_all.shape[3]
    quarter_q, half_q = tiles // 4, tiles // 2
    columns = latent // 128

    me = lax.axis_index(AXIS)
    core = lax.rem(me, 2)
    xpos = lax.rem(me // 2, side)
    ypos = me // (2 * side)
    sibling = me + 1 - 2 * core

    def wrap(pos, step):
        return lax.rem(pos + (step + side), side)

    def neighbour(axis, half, step):
        if axis == half:
            return (ypos * side + wrap(xpos, step)) * 2 + core
        return (wrap(ypos, step) * side + xpos) * 2 + core

    def peer(dev):
        return {AXIS: dev}

    def remote(ref, dst, send_sem, recv_sem, dev):
        return pltpu.make_async_remote_copy(src_ref=ref, dst_ref=dst, send_sem=send_sem, recv_sem=recv_sem,
                                            device_id=peer(dev), device_id_type=pl.DeviceIdType.MESH)

    def gather_block(j, half, first, second, rng):
        if half == 0:
            yy, xx = wrap(ypos, second), wrap(xpos, first)
        else:
            yy, xx = wrap(ypos, first), wrap(xpos, second)
        start = half * half_q + (quarter_q if rng == HIGH else 0)
        return q_all.at[j, yy, xx, pl.ds(start, half_q if rng == FULL else quarter_q)]

    def gather_send(j, *indices):
        for idx in indices:
            for half in (0, 1):
                axis, step, (first, second), rng, sem = GATHER[idx]
                ref = gather_block(j, half, first, second, rng)
                remote(ref, ref, ag_send.at[j, 0 if rng == FULL else 1], ag_recv.at[j, half, sem],
                       neighbour(axis, half, step)).start()

    def wait_bytes(ref, sem):
        pltpu.make_async_copy(ref, ref, sem).wait()

    def gather_wait(j, half, sem):
        ref = q_all.at[j, 0] if sem == 7 else gather_block(j, half, 0, 0, FULL)
        wait_bytes(ref, ag_recv.at[j, half, sem])

    def rows_of(half, rng):
        return half * half_h + (quarter_h if rng == HIGH else 0)

    def first_part(r, half, step, rng, i=None):
        hs = pl.ds(rows_of(half, rng), quarter_h)
        second = slice(None) if i is None else i
        if half == 0:
            return part.at[r, second, wrap(xpos, step), hs]
        return part.at[r, wrap(ypos, step), second, hs]

    def second_part(r, half, step, rng):
        hs = pl.ds(rows_of(half, rng), quarter_h)
        if half == 0:
            return part.at[r, wrap(ypos, step), xpos, hs]
        return part.at[r, ypos, wrap(xpos, step), hs]

    def reduce_send(r, axis, *indices):
        for idx in indices:
            for half in (0, 1):
                dest, rng, step, sem = REDUCE[idx]
                src = (first_part if axis == FIRST else second_part)(r, half, dest, rng)
                dst = (xbuf if axis == FIRST else ybuf).at[r, half, idx]
                remote(src, dst, rs_send.at[r, axis], rs_recv.at[r, half, axis, sem], neighbour(axis, half, step)).start()

    def reduce_wait(r, axis, half, sem):
        buf = xbuf if axis == FIRST else ybuf
        wait_bytes(buf.at[r, half, pl.ds(0, 4)] if sem == 2 else buf.at[r, half, 0], rs_recv.at[r, half, axis, sem])

    def lse_buf(axis):
        return lse_x if axis == 0 else lse_y

    def lse_send(j, axis):
        buf = lse_buf(axis)
        for idx, step in enumerate((1, -1, 2)):
            remote(buf.at[j, 0], buf.at[j, idx + 1], ls_send.at[j, axis], ls_recv.at[j, axis], neighbour(axis, 0, step)).start()

    def lse_wait(j, axis):
        wait_bytes(lse_buf(axis).at[j, pl.ds(0, 3)], ls_recv.at[j, axis])

    def swap_piece(j, n):
        ts = pl.ds(n * (nt // SLICES), nt // SLICES)
        remote(cache_ref.at[ts, 1 - core, j], sib_ref.at[j, ts], swap_send.at[j], swap_recv.at[j], sibling).start()

    def query_swap():
        return remote(q_ref.at[:, 1 - core], q_sib, qs_send, qs_recv, sibling)

    def load_pages(j, t):
        slot = lax.rem(t, DEPTH)
        for p, src in ((0, cache_ref.at[t, core, j]), (1, sib_ref.at[j, t])):
            pltpu.make_async_copy(src, page.at[slot, p, pl.ds(0, width)], page_sem.at[slot, p]).start()
            pltpu.make_async_copy(src.at[pl.ds(latent, ROPE_DIM)], page.at[slot, p, pl.ds(width, ROPE_DIM)],
                                  page_sem.at[slot, p]).start()

    def merge_queries(j):
        for t in range(nt):
            mine = q_ref[t, core, j].astype(jnp.float32)
            other = q_sib[t, j].astype(jnp.float32)
            both = jnp.concatenate([jnp.where(core == 0, mine, other), jnp.where(core == 0, other, mine)], axis=0)
            base, sub = (t // 4) * quarter_q, t % 4
            for i in range(columns):
                q_all[j, ypos, xpos, base + sub * columns + i] = both[:, i * 128:(i + 1) * 128].astype(jnp.bfloat16)
            rope = both[:, latent:]
            if sub < 2:
                low = (low if sub else []) + [rope]
            else:
                q_all[j, ypos, xpos, base + 4 * columns + sub - 2] = jnp.concatenate([low[sub - 2], rope], axis=1).astype(
                    jnp.bfloat16)

    def gather_first(j):
        for sem, sends in ((0, (2, 5, 9)), (1, (3, 6, 10))):
            for half in (0, 1):
                gather_wait(j, half, sem)
            gather_send(j, *sends)

    def gather_turn(j):
        for half in (0, 1):
            gather_wait(j, half, 2)
        gather_send(j, 7, 11)

    def gather_second(j, sem, send):
        for half in (0, 1):
            gather_wait(j, half, sem)
        gather_send(j, send)

    def gather_end(j):
        for half in (0, 1):
            gather_wait(j, half, 7)

    def first_pages(j):
        wait_bytes(sib_ref.at[j], swap_recv.at[j])
        for t in range(DEPTH - 1):
            load_pages(j, t)

    def attend(j, t):
        @pl.when(t + DEPTH - 1 < nt)
        def _():
            load_pages(j, t + DEPTH - 1)

        slot = lax.rem(t, DEPTH)
        for p in (0, 1):
            wait_bytes(page.at[slot, p], page_sem.at[slot, p])
        base, sub = (t // 4) * quarter_q, lax.rem(t, 4)
        cols = [q_all[j, :, :, base + sub * columns + i].reshape(heads, 128) for i in range(columns)]
        rope = q_all[j, :, :, base + 4 * columns + lax.rem(sub, 2)].reshape(heads, 128)
        lane_half = lax.broadcasted_iota(jnp.int32, (heads, 128), 1) // ROPE_DIM
        cols.append(jnp.where(lane_half == sub // 2, rope, jnp.zeros_like(rope)))
        q = jnp.concatenate(cols, axis=1)
        limit = len_ref[(t * 2 + core) * nj + j]
        outs, lses = [], []
        for p in (0, 1):
            owner = me if p == 0 else sibling
            s = jnp.dot(q, page[slot, p], preferred_element_type=jnp.float32) * (QK_DIM ** -0.5)
            position = owner * page_len + lax.broadcasted_iota(jnp.int32, (1, page_len), 1)
            s = jnp.where(position < limit, s, -1e30)
            m = jnp.max(s, axis=1, keepdims=True)
            w = jnp.exp(s - m)
            l = jnp.sum(w, axis=1, keepdims=True)
            pv = lax.dot_general(w.astype(jnp.bfloat16), page[slot, p, :latent], (((1,), (1,)), ((), ())),
                                 preferred_element_type=jnp.float32)
            outs.append((pv * (1.0 / l)).astype(jnp.bfloat16).astype(jnp.float32))
            lses.append(m + jnp.log(l))
        top = jnp.maximum(lses[0], lses[1])
        both = top + jnp.log(jnp.exp(lses[0] - top) + jnp.exp(lses[1] - top))
        part[j, t // side, lax.rem(t, side)] = jnp.exp(lses[0] - both) * outs[0] + jnp.exp(lses[1] - both) * outs[1]
        row = jnp.broadcast_to(both, (heads, 128)).T
        lse_x[j, 0, pl.ds(t, 1), :] = row[0:1]

    def attend_slice(j, n):
        per = nt // SLICES
        lax.fori_loop(n * per, (n + 1) * per, lambda t, _: (attend(j, t), 0)[1], 0)

    def combine(v):
        top = jnp.max(v, axis=0)
        return top + jnp.log(jnp.sum(jnp.exp(v - top[None]), axis=0))

    def lse_turn(j):
        lse_wait(j, 0)
        lse_y[j, 0] = combine(lse_x[j])
        lse_send(j, 1)

    def weigh(j):
        lse_wait(j, 1)
        wgt[...] = jnp.exp(lse_x[j, 0] - combine(lse_y[j]))

        def body(t, _):
            w = jnp.broadcast_to(wgt[pl.ds(t, 1), :], (128, heads)).T
            yy, xx = t // side, lax.rem(t, side)
            for i in range(latent // 128):
                cols = pl.ds(i * 128, 128)
                part[j, yy, xx, :, cols] = part[j, yy, xx, :, cols] * w
            return 0

        lax.fori_loop(0, nt, body, 0)

    def reduce_start(r, axis):
        reduce_send(r, axis, 0, 2, 1, 3)

    def reduce_turn(r, axis):
        for idx, dest, rng, nxt, sem in ((0, 1, LOW, 4, 0), (2, -1, HIGH, 5, 1)):
            for half in (0, 1):
                reduce_wait(r, axis, half, sem)
                if axis == FIRST:
                    def body(i, _):
                        ref = first_part(r, half, dest, rng, i)
                        ref[...] = ref[...] + xbuf[r, half, idx, i]
                        return 0
                    lax.fori_loop(0, side, body, 0)
                else:
                    ref = second_part(r, half, dest, rng)
                    ref[...] = ref[...] + ybuf[r, half, idx]
            reduce_send(r, axis, nxt)

    def reduce_end(r, axis):
        for half in (0, 1):
            reduce_wait(r, axis, half, 2)
            for rng, one, two in ((HIGH, 1, 5), (LOW, 3, 4)):
                if axis == FIRST:
                    def body(i, _):
                        ref = first_part(r, half, 0, rng, i)
                        ref[...] = ref[...] + (xbuf[r, half, one, i] + xbuf[r, half, two, i])
                        return 0
                    lax.fori_loop(0, side, body, 0)
                else:
                    total = second_part(r, half, 0, rng)[...] + (ybuf[r, half, one] + ybuf[r, half, two])
                    out_ref[r, pl.ds(rows_of(half, rng), quarter_h)] = total.astype(out_ref.dtype)

    barrier = pltpu.get_barrier_semaphore()
    peers = [sibling] + [neighbour(axis, 0, step) for axis in (0, 1) for step in (1, -1, 2)]
    for dev in peers:
        pl.semaphore_signal(barrier, inc=1, device_id=peer(dev), device_id_type=pl.DeviceIdType.MESH)
    with jax.named_scope('barrier'):
        pl.semaphore_wait(barrier, len(peers))

    query_swap().start()
    with jax.named_scope('merge0'):
        query_swap().wait_recv()
        merge_queries(0)
    gather_send(0, 0, 1, 4, 8)
    swap_piece(0, 0)
    swap_piece(0, 1)
    with jax.named_scope('merges'):
        lax.fori_loop(1, nj, lambda j, _: (merge_queries(j), 0)[1], 0)
    gather_send(1, 0, 1)
    with jax.named_scope('chunk0'):
        gather_first(0)
        swap_piece(0, 2)
        gather_second(0, 3, 12)
        gather_second(0, 5, 14)
        swap_piece(0, 3)
        gather_turn(0)
        gather_second(0, 4, 13)
        gather_send(1, 4, 8)
    with jax.named_scope('chunk1'):
        gather_first(1)
        swap_piece(1, 0)
        gather_second(0, 6, 15)
        gather_send(2, 0, 1)
        swap_piece(1, 1)
        gather_end(0)

    def stage(k, _):
        def when(lag, fn, *args):
            def run():
                with jax.named_scope(fn.__name__ + '_'.join(str(a) for a in args)):
                    fn(k - lag, *args)
            pl.when((k >= lag) & (k < nj + lag))(run)

        when(0, first_pages)
        when(-1, gather_turn)
        when(-1, gather_second, 3, 12)
        when(-1, gather_second, 5, 14)
        when(-1, gather_second, 4, 13)
        when(3, reduce_turn, FIRST)
        when(4, reduce_turn, SECOND)
        when(-1, swap_piece, 2)
        when(0, attend_slice, 0)
        when(1, lse_turn)
        when(2, weigh)
        when(2, reduce_start, FIRST)
        when(-2, gather_first)
        when(-2, gather_send, 4, 8)
        when(-1, swap_piece, 3)
        when(0, attend_slice, 1)
        when(-1, gather_second, 6, 15)
        when(-3, gather_send, 0, 1)
        when(-2, swap_piece, 0)
        when(0, attend_slice, 2)
        when(-2, swap_piece, 1)
        when(0, attend_slice, 3)
        when(0, lse_send, 0)
        when(-1, gather_end)
        when(3, reduce_end, FIRST)
        when(3, reduce_start, SECOND)
        when(4, reduce_end, SECOND)
        return 0

    lax.fori_loop(0, nj + 4, stage, 0)

    def drain(j, _):
        wait_bytes(sib_ref.at[j], swap_send.at[j])
        wait_bytes(q_all.at[j, :, :, pl.ds(0, 14 * tiles // 16)], ag_send.at[j, 0])
        wait_bytes(q_all.at[j, 0, 0], ag_send.at[j, 1])
        wait_bytes(xbuf.at[j], rs_send.at[j, 0])
        wait_bytes(ybuf.at[j], rs_send.at[j, 1])
        for axis in (0, 1):
            wait_bytes(lse_buf(axis).at[j, pl.ds(0, 3)], ls_send.at[j, axis])
        return 0

    with jax.named_scope('drain'):
        query_swap().wait_send()
        lax.fori_loop(0, nj, drain, 0)


def solution(mesh):
    group_size = mesh.shape[AXIS]
    side = math.isqrt(group_size // 2)
    nt = side * side

    def local_step(q_blk, cache_blk, len_blk):
        batch_rows, own_heads, width = q_blk.shape
        page_len = cache_blk.shape[3]
        latent = width - ROPE_DIM
        nj = batch_rows // group_size
        heads = 2 * own_heads * nt
        tiles = nt * (latent // 128) + nt // 2
        q = q_blk.reshape(nt, 2, nj, own_heads, width)
        cache = jnp.swapaxes(cache_blk.reshape(nt, 2, nj, page_len, width), 3, 4)
        any_space = pl.BlockSpec(memory_space=pl.ANY)
        dma = pltpu.SemaphoreType.DMA
        out, _ = pl.pallas_call(
            functools.partial(_kernel, side),
            out_shape=(jax.ShapeDtypeStruct((nj, heads, latent), jnp.bfloat16),
                       jax.ShapeDtypeStruct((nj, nt, width, page_len), jnp.bfloat16)),
            in_specs=[pl.BlockSpec(memory_space=pltpu.SMEM), pl.BlockSpec(memory_space=pltpu.VMEM), any_space],
            out_specs=(pl.BlockSpec(memory_space=pltpu.VMEM), any_space),
            scratch_shapes=[
                pltpu.VMEM((nt, nj, own_heads, width), jnp.bfloat16),
                pltpu.VMEM((nj, side, side, tiles, 2 * own_heads, 128), jnp.bfloat16),
                pltpu.VMEM((nj, side, side, heads, latent), jnp.float32),
                pltpu.VMEM((DEPTH, 2, width + ROPE_DIM, page_len), jnp.bfloat16),
                pltpu.VMEM((nj, 2, len(REDUCE), side, heads // 4, latent), jnp.float32),
                pltpu.VMEM((nj, 2, len(REDUCE), heads // 4, latent), jnp.float32),
                pltpu.VMEM((nj, 4, nt, heads), jnp.float32),
                pltpu.VMEM((nj, 4, nt, heads), jnp.float32),
                pltpu.VMEM((nt, heads), jnp.float32),
                dma((DEPTH, 2)), dma((nj,)), dma((nj,)), dma(()), dma(()),
                dma((nj, 2)), dma((nj, 2, 8)), dma((nj, 2)), dma((nj, 2, 2, 3)), dma((nj, 2)), dma((nj, 2)),
            ],
            compiler_params=pltpu.CompilerParams(collective_id=0, has_side_effects=True, vmem_limit_bytes=54_000_000),
        )(len_blk, q, cache)
        return out

    return jax.shard_map(local_step, mesh=mesh, in_specs=(P('dp', AXIS, None), P('dp', None, AXIS, None, None), P('dp')),
                         out_specs=P(('dp', AXIS), None, None), check_vma=False)
```

```python
import functools
import math

import jax
import jax.numpy as jnp
from jax import lax
from jax.experimental import pallas as pl
from jax.experimental.pallas import tpu as pltpu
from jax.sharding import PartitionSpec as P

ROPE_DIM = 64
QK_DIM = 192
AXIS = 'dcp'
DEPTH = 3
SLICES = 4

FIRST, SECOND = 0, 1
FULL, LOW, HIGH = 0, 1, 2
GATHER = (
    (FIRST, 1, (0, 0), FULL, 0),
    (FIRST, -1, (0, 0), FULL, 1),
    (FIRST, 1, (-1, 0), LOW, 2),
    (FIRST, -1, (1, 0), HIGH, 2),
    (SECOND, 1, (0, 0), FULL, 3),
    (SECOND, 1, (-1, 0), FULL, 4),
    (SECOND, 1, (1, 0), FULL, 7),
    (SECOND, 1, (2, 0), FULL, 7),
    (SECOND, -1, (0, 0), FULL, 7),
    (SECOND, -1, (-1, 0), FULL, 7),
    (SECOND, -1, (1, 0), FULL, 5),
    (SECOND, -1, (2, 0), FULL, 6),
    (SECOND, 1, (0, -1), FULL, 7),
    (SECOND, 1, (-1, -1), FULL, 7),
    (SECOND, -1, (1, 1), FULL, 7),
    (SECOND, -1, (2, 1), FULL, 7),
)
REDUCE = ((2, LOW, 1, 0), (1, HIGH, 1, 2), (2, HIGH, -1, 1), (-1, LOW, -1, 2), (1, LOW, 1, 2), (-1, HIGH, -1, 2))


def _kernel(side, len_ref, q_ref, cache_ref, out_ref, sib_ref, q_sib, q_all, part, page, xbuf, ybuf, lse_x, lse_y,
            wgt, page_sem, swap_send, swap_recv, qs_send, qs_recv, ag_send, ag_recv, rs_send, rs_recv, ls_send,
            ls_recv):
    nt, nj, own_heads, width = q_sib.shape
    heads, latent = part.shape[3:]
    page_len = page.shape[3]
    half_h, quarter_h = heads // 2, heads // 4
    tiles = q_all.shape[3]
    quarter_q, half_q = tiles // 4, tiles // 2
    columns = latent // 128

    me = lax.axis_index(AXIS)
    core = lax.rem(me, 2)
    xpos = lax.rem(me // 2, side)
    ypos = me // (2 * side)
    sibling = me + 1 - 2 * core

    def wrap(pos, step):
        return lax.rem(pos + (step + side), side)

    def neighbour(axis, half, step):
        if axis == half:
            return (ypos * side + wrap(xpos, step)) * 2 + core
        return (wrap(ypos, step) * side + xpos) * 2 + core

    def peer(dev):
        return {AXIS: dev}

    def remote(ref, dst, send_sem, recv_sem, dev):
        return pltpu.make_async_remote_copy(src_ref=ref, dst_ref=dst, send_sem=send_sem, recv_sem=recv_sem,
                                            device_id=peer(dev), device_id_type=pl.DeviceIdType.MESH)

    def gather_block(j, half, first, second, rng):
        if half == 0:
            yy, xx = wrap(ypos, second), wrap(xpos, first)
        else:
            yy, xx = wrap(ypos, first), wrap(xpos, second)
        start = half * half_q + (quarter_q if rng == HIGH else 0)
        return q_all.at[j, yy, xx, pl.ds(start, half_q if rng == FULL else quarter_q)]

    def gather_send(j, *indices):
        for idx in indices:
            for half in (0, 1):
                axis, step, (first, second), rng, sem = GATHER[idx]
                ref = gather_block(j, half, first, second, rng)
                remote(ref, ref, ag_send.at[j, 0 if rng == FULL else 1], ag_recv.at[j, half, sem],
                       neighbour(axis, half, step)).start()

    def wait_bytes(ref, sem):
        pltpu.make_async_copy(ref, ref, sem).wait()

    def gather_wait(j, half, sem):
        ref = q_all.at[j, 0] if sem == 7 else gather_block(j, half, 0, 0, FULL)
        wait_bytes(ref, ag_recv.at[j, half, sem])

    def rows_of(half, rng):
        return half * half_h + (quarter_h if rng == HIGH else 0)

    def first_part(r, half, step, rng, i=None):
        hs = pl.ds(rows_of(half, rng), quarter_h)
        second = slice(None) if i is None else i
        if half == 0:
            return part.at[r, second, wrap(xpos, step), hs]
        return part.at[r, wrap(ypos, step), second, hs]

    def second_part(r, half, step, rng):
        hs = pl.ds(rows_of(half, rng), quarter_h)
        if half == 0:
            return part.at[r, wrap(ypos, step), xpos, hs]
        return part.at[r, ypos, wrap(xpos, step), hs]

    def reduce_send(r, axis, *indices):
        for idx in indices:
            for half in (0, 1):
                dest, rng, step, sem = REDUCE[idx]
                src = (first_part if axis == FIRST else second_part)(r, half, dest, rng)
                dst = (xbuf if axis == FIRST else ybuf).at[r, half, idx]
                remote(src, dst, rs_send.at[r, axis], rs_recv.at[r, half, axis, sem], neighbour(axis, half, step)).start()

    def reduce_wait(r, axis, half, sem):
        buf = xbuf if axis == FIRST else ybuf
        wait_bytes(buf.at[r, half, pl.ds(0, 4)] if sem == 2 else buf.at[r, half, 0], rs_recv.at[r, half, axis, sem])

    def lse_buf(axis):
        return lse_x if axis == 0 else lse_y

    def lse_send(j, axis):
        buf = lse_buf(axis)
        for idx, step in enumerate((1, -1, 2)):
            remote(buf.at[j, 0], buf.at[j, idx + 1], ls_send.at[j, axis], ls_recv.at[j, axis], neighbour(axis, 0, step)).start()

    def lse_wait(j, axis):
        wait_bytes(lse_buf(axis).at[j, pl.ds(0, 3)], ls_recv.at[j, axis])

    def swap_piece(j, n):
        ts = pl.ds(n * (nt // SLICES), nt // SLICES)
        remote(cache_ref.at[ts, 1 - core, j], sib_ref.at[j, ts], swap_send.at[j], swap_recv.at[j], sibling).start()

    def query_swap():
        return remote(q_ref.at[:, 1 - core], q_sib, qs_send, qs_recv, sibling)

    def load_pages(j, t):
        slot = lax.rem(t, DEPTH)
        for p, src in ((0, cache_ref.at[t, core, j]), (1, sib_ref.at[j, t])):
            pltpu.make_async_copy(src, page.at[slot, p, pl.ds(0, width)], page_sem.at[slot, p]).start()
            pltpu.make_async_copy(src.at[pl.ds(latent, ROPE_DIM)], page.at[slot, p, pl.ds(width, ROPE_DIM)],
                                  page_sem.at[slot, p]).start()

    def merge_queries(j):
        for t in range(nt):
            mine = q_ref[t, core, j].astype(jnp.float32)
            other = q_sib[t, j].astype(jnp.float32)
            both = jnp.concatenate([jnp.where(core == 0, mine, other), jnp.where(core == 0, other, mine)], axis=0)
            base, sub = (t // 4) * quarter_q, t % 4
            for i in range(columns):
                q_all[j, ypos, xpos, base + sub * columns + i] = both[:, i * 128:(i + 1) * 128].astype(jnp.bfloat16)
            rope = both[:, latent:]
            if sub < 2:
                low = (low if sub else []) + [rope]
            else:
                q_all[j, ypos, xpos, base + 4 * columns + sub - 2] = jnp.concatenate([low[sub - 2], rope], axis=1).astype(
                    jnp.bfloat16)

    def gather_first(j):
        for sem, sends in ((0, (2, 5, 9)), (1, (3, 6, 10))):
            for half in (0, 1):
                gather_wait(j, half, sem)
            gather_send(j, *sends)

    def gather_turn(j):
        for half in (0, 1):
            gather_wait(j, half, 2)
        gather_send(j, 7, 11)

    def gather_second(j, sem, send):
        for half in (0, 1):
            gather_wait(j, half, sem)
        gather_send(j, send)

    def gather_end(j):
        for half in (0, 1):
            gather_wait(j, half, 7)

    def first_pages(j):
        wait_bytes(sib_ref.at[j], swap_recv.at[j])
        for t in range(DEPTH - 1):
            load_pages(j, t)

    def attend(j, t):
        @pl.when(t + DEPTH - 1 < nt)
        def _():
            load_pages(j, t + DEPTH - 1)

        slot = lax.rem(t, DEPTH)
        for p in (0, 1):
            wait_bytes(page.at[slot, p], page_sem.at[slot, p])
        base, sub = (t // 4) * quarter_q, lax.rem(t, 4)
        cols = [q_all[j, :, :, base + sub * columns + i].reshape(heads, 128) for i in range(columns)]
        rope = q_all[j, :, :, base + 4 * columns + lax.rem(sub, 2)].reshape(heads, 128)
        lane_half = lax.broadcasted_iota(jnp.int32, (heads, 128), 1) // ROPE_DIM
        cols.append(jnp.where(lane_half == sub // 2, rope, jnp.zeros_like(rope)))
        q = jnp.concatenate(cols, axis=1)
        limit = len_ref[(t * 2 + core) * nj + j]
        outs, lses = [], []
        for p in (0, 1):
            owner = me if p == 0 else sibling
            s = jnp.dot(q, page[slot, p], preferred_element_type=jnp.float32) * (QK_DIM ** -0.5)
            position = owner * page_len + lax.broadcasted_iota(jnp.int32, (1, page_len), 1)
            s = jnp.where(position < limit, s, -1e30)
            m = jnp.max(s, axis=1, keepdims=True)
            w = jnp.exp(s - m)
            l = jnp.sum(w, axis=1, keepdims=True)
            pv = lax.dot_general(w.astype(jnp.bfloat16), page[slot, p, :latent], (((1,), (1,)), ((), ())),
                                 preferred_element_type=jnp.float32)
            outs.append((pv * (1.0 / l)).astype(jnp.bfloat16).astype(jnp.float32))
            lses.append(m + jnp.log(l))
        top = jnp.maximum(lses[0], lses[1])
        both = top + jnp.log(jnp.exp(lses[0] - top) + jnp.exp(lses[1] - top))
        part[j, t // side, lax.rem(t, side)] = jnp.exp(lses[0] - both) * outs[0] + jnp.exp(lses[1] - both) * outs[1]
        row = jnp.broadcast_to(both, (heads, 128)).T
        lse_x[j, 0, pl.ds(t, 1), :] = row[0:1]

    def attend_slice(j, n):
        per = nt // SLICES
        lax.fori_loop(n * per, (n + 1) * per, lambda t, _: (attend(j, t), 0)[1], 0)

    def combine(v):
        top = jnp.max(v, axis=0)
        return top + jnp.log(jnp.sum(jnp.exp(v - top[None]), axis=0))

    def lse_turn(j):
        lse_wait(j, 0)
        lse_y[j, 0] = combine(lse_x[j])
        lse_send(j, 1)

    def weigh(j):
        lse_wait(j, 1)
        wgt[...] = jnp.exp(lse_x[j, 0] - combine(lse_y[j]))

        def body(t, _):
            w = jnp.broadcast_to(wgt[pl.ds(t, 1), :], (128, heads)).T
            yy, xx = t // side, lax.rem(t, side)
            for i in range(latent // 128):
                cols = pl.ds(i * 128, 128)
                part[j, yy, xx, :, cols] = part[j, yy, xx, :, cols] * w
            return 0

        lax.fori_loop(0, nt, body, 0)

    def reduce_start(r, axis):
        reduce_send(r, axis, 0, 2, 1, 3)

    def reduce_turn(r, axis):
        for idx, dest, rng, nxt, sem in ((0, 1, LOW, 4, 0), (2, -1, HIGH, 5, 1)):
            for half in (0, 1):
                reduce_wait(r, axis, half, sem)
                if axis == FIRST:
                    def body(i, _):
                        ref = first_part(r, half, dest, rng, i)
                        ref[...] = ref[...] + xbuf[r, half, idx, i]
                        return 0
                    lax.fori_loop(0, side, body, 0)
                else:
                    ref = second_part(r, half, dest, rng)
                    ref[...] = ref[...] + ybuf[r, half, idx]
            reduce_send(r, axis, nxt)

    def reduce_end(r, axis):
        for half in (0, 1):
            reduce_wait(r, axis, half, 2)
            for rng, one, two in ((HIGH, 1, 5), (LOW, 3, 4)):
                if axis == FIRST:
                    def body(i, _):
                        ref = first_part(r, half, 0, rng, i)
                        ref[...] = ref[...] + (xbuf[r, half, one, i] + xbuf[r, half, two, i])
                        return 0
                    lax.fori_loop(0, side, body, 0)
                else:
                    total = second_part(r, half, 0, rng)[...] + (ybuf[r, half, one] + ybuf[r, half, two])
                    out_ref[r, pl.ds(rows_of(half, rng), quarter_h)] = total.astype(out_ref.dtype)

    barrier = pltpu.get_barrier_semaphore()
    peers = [sibling] + [neighbour(axis, 0, step) for axis in (0, 1) for step in (1, -1, 2)]
    for dev in peers:
        pl.semaphore_signal(barrier, inc=1, device_id=peer(dev), device_id_type=pl.DeviceIdType.MESH)
    with jax.named_scope('barrier'):
        pl.semaphore_wait(barrier, len(peers))

    query_swap().start()
    with jax.named_scope('merge0'):
        query_swap().wait_recv()
        merge_queries(0)
    gather_send(0, 0, 1, 4, 8)
    swap_piece(0, 0)
    swap_piece(0, 1)
    with jax.named_scope('merges'):
        lax.fori_loop(1, nj, lambda j, _: (merge_queries(j), 0)[1], 0)
    with jax.named_scope('chunk0'):
        gather_first(0)
        swap_piece(0, 2)
        gather_second(0, 3, 12)
        gather_turn(0)
        swap_piece(0, 3)
        gather_second(0, 4, 13)
        gather_second(0, 5, 14)
        gather_send(1, 0, 1)
        gather_second(0, 6, 15)
    with jax.named_scope('chunk1'):
        swap_piece(1, 0)
        gather_send(1, 4, 8)
        gather_first(1)
        gather_send(2, 0, 1)
        swap_piece(1, 1)
        gather_end(0)

    def stage(k, _):
        def when(lag, fn, *args):
            def run():
                with jax.named_scope(fn.__name__ + '_'.join(str(a) for a in args)):
                    fn(k - lag, *args)
            pl.when((k >= lag) & (k < nj + lag))(run)

        def gather_middle(first):
            @pl.when((k == 0) == first)
            def _():
                when(-1, gather_turn)
                when(-1, gather_second, 3, 12)
                when(-1, gather_second, 5, 14)
                when(-1, gather_second, 4, 13)

        when(0, first_pages)
        gather_middle(False)
        when(-1, swap_piece, 2)
        when(0, attend_slice, 0)
        when(1, lse_turn)
        gather_middle(True)
        when(-2, gather_first)
        when(-2, gather_send, 4, 8)
        when(-1, swap_piece, 3)
        when(0, attend_slice, 1)
        when(-1, gather_second, 6, 15)
        when(-3, gather_send, 0, 1)
        when(-2, swap_piece, 0)
        when(0, attend_slice, 2)
        when(2, reduce_turn, FIRST)
        when(3, reduce_turn, SECOND)
        when(1, weigh)
        when(1, reduce_start, FIRST)
        when(-2, swap_piece, 1)
        when(0, attend_slice, 3)
        when(0, lse_send, 0)
        when(-1, gather_end)
        when(2, reduce_end, FIRST)
        when(2, reduce_start, SECOND)
        when(3, reduce_end, SECOND)
        return 0

    lax.fori_loop(0, nj + 3, stage, 0)

    def drain(j, _):
        wait_bytes(sib_ref.at[j], swap_send.at[j])
        wait_bytes(q_all.at[j, :, :, pl.ds(0, 14 * tiles // 16)], ag_send.at[j, 0])
        wait_bytes(q_all.at[j, 0, 0], ag_send.at[j, 1])
        wait_bytes(xbuf.at[j], rs_send.at[j, 0])
        wait_bytes(ybuf.at[j], rs_send.at[j, 1])
        for axis in (0, 1):
            wait_bytes(lse_buf(axis).at[j, pl.ds(0, 3)], ls_send.at[j, axis])
        return 0

    with jax.named_scope('drain'):
        query_swap().wait_send()
        lax.fori_loop(0, nj, drain, 0)


def solution(mesh):
    group_size = mesh.shape[AXIS]
    side = math.isqrt(group_size // 2)
    nt = side * side

    def local_step(q_blk, cache_blk, len_blk):
        batch_rows, own_heads, width = q_blk.shape
        page_len = cache_blk.shape[3]
        latent = width - ROPE_DIM
        nj = batch_rows // group_size
        heads = 2 * own_heads * nt
        tiles = nt * (latent // 128) + nt // 2
        q = q_blk.reshape(nt, 2, nj, own_heads, width)
        cache = jnp.swapaxes(cache_blk.reshape(nt, 2, nj, page_len, width), 3, 4)
        any_space = pl.BlockSpec(memory_space=pl.ANY)
        dma = pltpu.SemaphoreType.DMA
        out, _ = pl.pallas_call(
            functools.partial(_kernel, side),
            out_shape=(jax.ShapeDtypeStruct((nj, heads, latent), jnp.bfloat16),
                       jax.ShapeDtypeStruct((nj, nt, width, page_len), jnp.bfloat16)),
            in_specs=[pl.BlockSpec(memory_space=pltpu.SMEM), pl.BlockSpec(memory_space=pltpu.VMEM), any_space],
            out_specs=(pl.BlockSpec(memory_space=pltpu.VMEM), any_space),
            scratch_shapes=[
                pltpu.VMEM((nt, nj, own_heads, width), jnp.bfloat16),
                pltpu.VMEM((nj, side, side, tiles, 2 * own_heads, 128), jnp.bfloat16),
                pltpu.VMEM((nj, side, side, heads, latent), jnp.float32),
                pltpu.VMEM((DEPTH, 2, width + ROPE_DIM, page_len), jnp.bfloat16),
                pltpu.VMEM((nj, 2, len(REDUCE), side, heads // 4, latent), jnp.float32),
                pltpu.VMEM((nj, 2, len(REDUCE), heads // 4, latent), jnp.float32),
                pltpu.VMEM((nj, 4, nt, heads), jnp.float32),
                pltpu.VMEM((nj, 4, nt, heads), jnp.float32),
                pltpu.VMEM((nt, heads), jnp.float32),
                dma((DEPTH, 2)), dma((nj,)), dma((nj,)), dma(()), dma(()),
                dma((nj, 2)), dma((nj, 2, 8)), dma((nj, 2)), dma((nj, 2, 2, 3)), dma((nj, 2)), dma((nj, 2)),
            ],
            compiler_params=pltpu.CompilerParams(collective_id=0, has_side_effects=True, vmem_limit_bytes=54_000_000),
        )(len_blk, q, cache)
        return out

    return jax.shard_map(local_step, mesh=mesh, in_specs=(P('dp', AXIS, None), P('dp', None, AXIS, None, None), P('dp')),
                         out_specs=P(('dp', AXIS), None, None), check_vma=False)
```

```python
import functools
import math

import jax
import jax.numpy as jnp
from jax import lax
from jax.experimental import pallas as pl
from jax.experimental.pallas import tpu as pltpu
from jax.sharding import PartitionSpec as P

ROPE_DIM = 64
QK_DIM = 192
AXIS = 'dcp'
DEPTH = 3
SLICES = 4

FIRST, SECOND = 0, 1
FULL, LOW, HIGH = 0, 1, 2
GATHER = (
    (FIRST, 1, (0, 0), FULL, 0),
    (FIRST, -1, (0, 0), FULL, 1),
    (FIRST, 1, (-1, 0), LOW, 2),
    (FIRST, -1, (1, 0), HIGH, 2),
    (SECOND, 1, (0, 0), FULL, 3),
    (SECOND, 1, (-1, 0), FULL, 4),
    (SECOND, 1, (1, 0), FULL, 7),
    (SECOND, 1, (2, 0), FULL, 7),
    (SECOND, -1, (0, 0), FULL, 7),
    (SECOND, -1, (-1, 0), FULL, 7),
    (SECOND, -1, (1, 0), FULL, 5),
    (SECOND, -1, (2, 0), FULL, 6),
    (SECOND, 1, (0, -1), FULL, 7),
    (SECOND, 1, (-1, -1), FULL, 7),
    (SECOND, -1, (1, 1), FULL, 7),
    (SECOND, -1, (2, 1), FULL, 7),
)
REDUCE = ((2, LOW, 1, 0), (1, HIGH, 1, 2), (2, HIGH, -1, 1), (-1, LOW, -1, 2), (1, LOW, 1, 2), (-1, HIGH, -1, 2))


def _kernel(side, len_ref, q_ref, cache_ref, out_ref, sib_ref, q_sib, q_all, part, page, xbuf, ybuf, lse_x, lse_y,
            wgt, page_sem, swap_send, swap_recv, qs_send, qs_recv, ag_send, ag_recv, rs_send, rs_recv, ls_send,
            ls_recv):
    nt, nj, own_heads, width = q_sib.shape
    heads, latent = part.shape[3:]
    page_len = page.shape[3]
    half_h, quarter_h = heads // 2, heads // 4
    tiles = q_all.shape[3]
    quarter_q, half_q = tiles // 4, tiles // 2
    columns = latent // 128

    me = lax.axis_index(AXIS)
    core = lax.rem(me, 2)
    xpos = lax.rem(me // 2, side)
    ypos = me // (2 * side)
    sibling = me + 1 - 2 * core

    def wrap(pos, step):
        return lax.rem(pos + (step + side), side)

    def neighbour(axis, half, step):
        if axis == half:
            return (ypos * side + wrap(xpos, step)) * 2 + core
        return (wrap(ypos, step) * side + xpos) * 2 + core

    def peer(dev):
        return {AXIS: dev}

    def remote(ref, dst, send_sem, recv_sem, dev):
        return pltpu.make_async_remote_copy(src_ref=ref, dst_ref=dst, send_sem=send_sem, recv_sem=recv_sem,
                                            device_id=peer(dev), device_id_type=pl.DeviceIdType.MESH)

    def gather_block(j, half, first, second, rng):
        if half == 0:
            yy, xx = wrap(ypos, second), wrap(xpos, first)
        else:
            yy, xx = wrap(ypos, first), wrap(xpos, second)
        start = half * half_q + (quarter_q if rng == HIGH else 0)
        return q_all.at[j, yy, xx, pl.ds(start, half_q if rng == FULL else quarter_q)]

    def gather_send(j, *indices):
        for idx in indices:
            for half in (0, 1):
                axis, step, (first, second), rng, sem = GATHER[idx]
                ref = gather_block(j, half, first, second, rng)
                remote(ref, ref, ag_send.at[j, 0 if rng == FULL else 1], ag_recv.at[j, half, sem],
                       neighbour(axis, half, step)).start()

    def wait_bytes(ref, sem):
        pltpu.make_async_copy(ref, ref, sem).wait()

    def gather_wait(j, half, sem):
        ref = q_all.at[j, 0] if sem == 7 else gather_block(j, half, 0, 0, FULL)
        wait_bytes(ref, ag_recv.at[j, half, sem])

    def rows_of(half, rng):
        return half * half_h + (quarter_h if rng == HIGH else 0)

    def first_part(r, half, step, rng, i=None):
        hs = pl.ds(rows_of(half, rng), quarter_h)
        second = slice(None) if i is None else i
        if half == 0:
            return part.at[r, second, wrap(xpos, step), hs]
        return part.at[r, wrap(ypos, step), second, hs]

    def second_part(r, half, step, rng):
        hs = pl.ds(rows_of(half, rng), quarter_h)
        if half == 0:
            return part.at[r, wrap(ypos, step), xpos, hs]
        return part.at[r, ypos, wrap(xpos, step), hs]

    def reduce_send(r, axis, *indices):
        for idx in indices:
            for half in (0, 1):
                dest, rng, step, sem = REDUCE[idx]
                src = (first_part if axis == FIRST else second_part)(r, half, dest, rng)
                dst = (xbuf if axis == FIRST else ybuf).at[r, half, idx]
                remote(src, dst, rs_send.at[r, axis], rs_recv.at[r, half, axis, sem], neighbour(axis, half, step)).start()

    def reduce_wait(r, axis, half, sem):
        buf = xbuf if axis == FIRST else ybuf
        wait_bytes(buf.at[r, half, pl.ds(0, 4)] if sem == 2 else buf.at[r, half, 0], rs_recv.at[r, half, axis, sem])

    def lse_buf(axis):
        return lse_x if axis == 0 else lse_y

    def lse_send(j, axis):
        buf = lse_buf(axis)
        for idx, step in enumerate((1, -1, 2)):
            remote(buf.at[j, 0], buf.at[j, idx + 1], ls_send.at[j, axis], ls_recv.at[j, axis], neighbour(axis, 0, step)).start()

    def lse_wait(j, axis):
        wait_bytes(lse_buf(axis).at[j, pl.ds(0, 3)], ls_recv.at[j, axis])

    def swap_piece(j, n):
        ts = pl.ds(n * (nt // SLICES), nt // SLICES)
        remote(cache_ref.at[ts, 1 - core, j], sib_ref.at[j, ts], swap_send.at[j], swap_recv.at[j], sibling).start()

    def query_swap():
        return remote(q_ref.at[:, 1 - core], q_sib, qs_send, qs_recv, sibling)

    def load_pages(n):
        slot, j, t = lax.rem(n, DEPTH), n // nt, lax.rem(n, nt)
        for p, src in ((0, cache_ref.at[t, core, j]), (1, sib_ref.at[j, t])):
            pltpu.make_async_copy(src, page.at[slot, p, pl.ds(0, width)], page_sem.at[slot, p]).start()
            pltpu.make_async_copy(src.at[pl.ds(latent, ROPE_DIM)], page.at[slot, p, pl.ds(width, ROPE_DIM)],
                                  page_sem.at[slot, p]).start()

    def merge_queries(j):
        for t in range(nt):
            mine = q_ref[t, core, j].astype(jnp.float32)
            other = q_sib[t, j].astype(jnp.float32)
            both = jnp.concatenate([jnp.where(core == 0, mine, other), jnp.where(core == 0, other, mine)], axis=0)
            base, sub = (t // 4) * quarter_q, t % 4
            for i in range(columns):
                q_all[j, ypos, xpos, base + sub * columns + i] = both[:, i * 128:(i + 1) * 128].astype(jnp.bfloat16)
            rope = both[:, latent:]
            if sub < 2:
                low = (low if sub else []) + [rope]
            else:
                q_all[j, ypos, xpos, base + 4 * columns + sub - 2] = jnp.concatenate([low[sub - 2], rope], axis=1).astype(
                    jnp.bfloat16)

    def gather_first(j):
        for sem, sends in ((0, (2, 5, 9)), (1, (3, 6, 10))):
            for half in (0, 1):
                gather_wait(j, half, sem)
            gather_send(j, *sends)

    def gather_turn(j):
        for half in (0, 1):
            gather_wait(j, half, 2)
        gather_send(j, 7, 11)

    def gather_second(j, sem, send):
        for half in (0, 1):
            gather_wait(j, half, sem)
        gather_send(j, send)

    def gather_end(j):
        for half in (0, 1):
            gather_wait(j, half, 7)

    def swap_wait(j):
        wait_bytes(sib_ref.at[j], swap_recv.at[j])

    def attend(n):
        @pl.when(n + DEPTH - 1 < nj * nt)
        def _():
            load_pages(n + DEPTH - 1)

        slot, j, t = lax.rem(n, DEPTH), n // nt, lax.rem(n, nt)
        for p in (0, 1):
            wait_bytes(page.at[slot, p], page_sem.at[slot, p])
        base, sub = (t // 4) * quarter_q, lax.rem(t, 4)
        cols = [q_all[j, :, :, base + sub * columns + i].reshape(heads, 128) for i in range(columns)]
        rope = q_all[j, :, :, base + 4 * columns + lax.rem(sub, 2)].reshape(heads, 128)
        lane_half = lax.broadcasted_iota(jnp.int32, (heads, 128), 1) // ROPE_DIM
        cols.append(jnp.where(lane_half == sub // 2, rope, jnp.zeros_like(rope)))
        q = jnp.concatenate(cols, axis=1)
        limit = len_ref[(t * 2 + core) * nj + j]
        outs, lses = [], []
        for p in (0, 1):
            owner = me if p == 0 else sibling
            s = jnp.dot(q, page[slot, p], preferred_element_type=jnp.float32) * (QK_DIM ** -0.5)
            position = owner * page_len + lax.broadcasted_iota(jnp.int32, (1, page_len), 1)
            s = jnp.where(position < limit, s, -1e30)
            m = jnp.max(s, axis=1, keepdims=True)
            w = jnp.exp(s - m)
            l = jnp.sum(w, axis=1, keepdims=True)
            pv = lax.dot_general(w.astype(jnp.bfloat16), page[slot, p, :latent], (((1,), (1,)), ((), ())),
                                 preferred_element_type=jnp.float32)
            outs.append((pv * (1.0 / l)).astype(jnp.bfloat16).astype(jnp.float32))
            lses.append(m + jnp.log(l))
        top = jnp.maximum(lses[0], lses[1])
        both = top + jnp.log(jnp.exp(lses[0] - top) + jnp.exp(lses[1] - top))
        part[j, t // side, lax.rem(t, side)] = jnp.exp(lses[0] - both) * outs[0] + jnp.exp(lses[1] - both) * outs[1]
        row = jnp.broadcast_to(both, (heads, 128)).T
        lse_x[j, 0, pl.ds(t, 1), :] = row[0:1]

    def combine(v):
        top = jnp.max(v, axis=0)
        return top + jnp.log(jnp.sum(jnp.exp(v - top[None]), axis=0))

    def lse_turn(j):
        lse_wait(j, 0)
        lse_y[j, 0] = combine(lse_x[j])
        lse_send(j, 1)

    def weigh(j):
        lse_wait(j, 1)
        wgt[...] = jnp.exp(lse_x[j, 0] - combine(lse_y[j]))

        def body(t, _):
            w = jnp.broadcast_to(wgt[pl.ds(t, 1), :], (128, heads)).T
            yy, xx = t // side, lax.rem(t, side)
            for i in range(latent // 128):
                cols = pl.ds(i * 128, 128)
                part[j, yy, xx, :, cols] = part[j, yy, xx, :, cols] * w
            return 0

        lax.fori_loop(0, nt, body, 0)

    def reduce_turn(r, axis):
        for idx, dest, rng, nxt, sem in ((0, 1, LOW, 4, 0), (2, -1, HIGH, 5, 1)):
            for half in (0, 1):
                reduce_wait(r, axis, half, sem)
                if axis == FIRST:
                    def body(i, _):
                        ref = first_part(r, half, dest, rng, i)
                        ref[...] = ref[...] + xbuf[r, half, idx, i]
                        return 0
                    lax.fori_loop(0, side, body, 0)
                else:
                    ref = second_part(r, half, dest, rng)
                    ref[...] = ref[...] + ybuf[r, half, idx]
            reduce_send(r, axis, nxt)

    def reduce_end(r, axis):
        for half in (0, 1):
            reduce_wait(r, axis, half, 2)
            for rng, one, two in ((HIGH, 1, 5), (LOW, 3, 4)):
                if axis == FIRST:
                    def body(i, _):
                        ref = first_part(r, half, 0, rng, i)
                        ref[...] = ref[...] + (xbuf[r, half, one, i] + xbuf[r, half, two, i])
                        return 0
                    lax.fori_loop(0, side, body, 0)
                else:
                    total = second_part(r, half, 0, rng)[...] + (ybuf[r, half, one] + ybuf[r, half, two])
                    out_ref[r, pl.ds(rows_of(half, rng), quarter_h)] = total.astype(out_ref.dtype)

    barrier = pltpu.get_barrier_semaphore()
    peers = [sibling] + [neighbour(axis, 0, step) for axis in (0, 1) for step in (1, -1, 2)]
    for dev in peers:
        pl.semaphore_signal(barrier, inc=1, device_id=peer(dev), device_id_type=pl.DeviceIdType.MESH)
    with jax.named_scope('barrier'):
        pl.semaphore_wait(barrier, len(peers))

    query_swap().start()
    with jax.named_scope('merge0'):
        query_swap().wait_recv()
        merge_queries(0)
    gather_send(0, 0, 1, 4, 8)
    swap_piece(0, 0)
    swap_piece(0, 1)
    with jax.named_scope('merges'):
        lax.fori_loop(1, nj, lambda j, _: (merge_queries(j), 0)[1], 0)
    with jax.named_scope('chunk0'):
        gather_first(0)
        swap_piece(0, 2)
        gather_second(0, 3, 12)
        gather_turn(0)
        swap_piece(0, 3)
        gather_second(0, 4, 13)
        gather_second(0, 5, 14)
        gather_send(1, 0, 1)
        gather_second(0, 6, 15)
    with jax.named_scope('chunk1'):
        swap_piece(1, 0)
        gather_first(1)
        gather_send(1, 4, 8)
        gather_send(2, 0, 1)
        swap_piece(1, 1)
        swap_wait(0)
        for n in range(DEPTH - 1):
            load_pages(n)
        gather_end(0)

    def run(*steps):
        for fn, *args in steps:
            with jax.named_scope(fn.__name__ + '_' + '_'.join(str(a) for a in args)):
                fn(*args)

    def middle(j):
        run((gather_turn, j), (gather_second, j, 3, 12), (gather_second, j, 5, 14), (gather_second, j, 4, 13))

    slots = {
        0: ((swap_piece, 1, 2),),
        1: ((middle, 1), (gather_first, 2), (gather_send, 2, 4, 8), (swap_piece, 1, 3)),
        2: ((gather_second, 1, 6, 15), (gather_send, 3, 0, 1), (swap_piece, 2, 0)),
        3: ((swap_wait, 1), (swap_piece, 2, 1)),
        4: ((lse_send, 0, 0), (gather_end, 1), (middle, 2), (swap_piece, 2, 2)),
        5: ((gather_first, 3), (gather_send, 3, 4, 8), (swap_piece, 2, 3)),
        6: ((lse_turn, 0), (gather_second, 2, 6, 15), (swap_piece, 3, 0)),
        7: ((swap_wait, 2), (swap_piece, 3, 1)),
        8: ((lse_send, 1, 0), (gather_end, 2), (middle, 3), (swap_piece, 3, 2)),
        9: ((swap_piece, 3, 3), (weigh, 0), (reduce_send, 0, FIRST, 0, 2)),
        10: ((lse_turn, 1), (gather_second, 3, 6, 15)),
        11: ((reduce_send, 0, FIRST, 1, 3), (swap_wait, 3)),
        12: ((lse_send, 2, 0), (gather_end, 3)),
        13: ((reduce_turn, 0, FIRST),),
        14: ((lse_turn, 2), (weigh, 1), (reduce_send, 1, FIRST, 0, 2)),
    }

    def slot_body(n, _):
        for at, steps in slots.items():
            pl.when(n == at)(functools.partial(run, *steps))
        with jax.named_scope('attend'):
            lax.fori_loop(n * (nt // SLICES), (n + 1) * (nt // SLICES), lambda i, _: (attend(i), 0)[1], 0)
        return 0

    lax.fori_loop(0, nj * SLICES, slot_body, 0)

    early, late = (0, 2, 1, 3), (1, 3)
    run((lse_send, 3, 0), (reduce_send, 1, FIRST, *late), (reduce_end, 0, FIRST), (reduce_send, 0, SECOND, *early))
    run((reduce_turn, 1, FIRST), (lse_turn, 3), (reduce_turn, 0, SECOND), (weigh, 2), (reduce_send, 2, FIRST, *early),
        (reduce_end, 1, FIRST), (reduce_send, 1, SECOND, *early), (reduce_end, 0, SECOND))
    run((reduce_turn, 2, FIRST), (reduce_turn, 1, SECOND), (weigh, 3), (reduce_send, 3, FIRST, *early),
        (reduce_end, 2, FIRST), (reduce_send, 2, SECOND, *early), (reduce_end, 1, SECOND))
    run((reduce_turn, 3, FIRST), (reduce_turn, 2, SECOND), (reduce_end, 3, FIRST), (reduce_send, 3, SECOND, *early),
        (reduce_end, 2, SECOND))
    run((reduce_turn, 3, SECOND), (reduce_end, 3, SECOND))

    def drain(j, _):
        wait_bytes(sib_ref.at[j], swap_send.at[j])
        wait_bytes(q_all.at[j, :, :, pl.ds(0, 14 * tiles // 16)], ag_send.at[j, 0])
        wait_bytes(q_all.at[j, 0, 0], ag_send.at[j, 1])
        wait_bytes(xbuf.at[j], rs_send.at[j, 0])
        wait_bytes(ybuf.at[j], rs_send.at[j, 1])
        for axis in (0, 1):
            wait_bytes(lse_buf(axis).at[j, pl.ds(0, 3)], ls_send.at[j, axis])
        return 0

    with jax.named_scope('drain'):
        query_swap().wait_send()
        lax.fori_loop(0, nj, drain, 0)


def solution(mesh):
    group_size = mesh.shape[AXIS]
    side = math.isqrt(group_size // 2)
    nt = side * side

    def local_step(q_blk, cache_blk, len_blk):
        batch_rows, own_heads, width = q_blk.shape
        page_len = cache_blk.shape[3]
        latent = width - ROPE_DIM
        nj = batch_rows // group_size
        heads = 2 * own_heads * nt
        tiles = nt * (latent // 128) + nt // 2
        q = q_blk.reshape(nt, 2, nj, own_heads, width)
        cache = jnp.swapaxes(cache_blk.reshape(nt, 2, nj, page_len, width), 3, 4)
        any_space = pl.BlockSpec(memory_space=pl.ANY)
        dma = pltpu.SemaphoreType.DMA
        out, _ = pl.pallas_call(
            functools.partial(_kernel, side),
            out_shape=(jax.ShapeDtypeStruct((nj, heads, latent), jnp.bfloat16),
                       jax.ShapeDtypeStruct((nj, nt, width, page_len), jnp.bfloat16)),
            in_specs=[pl.BlockSpec(memory_space=pltpu.SMEM), pl.BlockSpec(memory_space=pltpu.VMEM), any_space],
            out_specs=(pl.BlockSpec(memory_space=pltpu.VMEM), any_space),
            scratch_shapes=[
                pltpu.VMEM((nt, nj, own_heads, width), jnp.bfloat16),
                pltpu.VMEM((nj, side, side, tiles, 2 * own_heads, 128), jnp.bfloat16),
                pltpu.VMEM((nj, side, side, heads, latent), jnp.float32),
                pltpu.VMEM((DEPTH, 2, width + ROPE_DIM, page_len), jnp.bfloat16),
                pltpu.VMEM((nj, 2, len(REDUCE), side, heads // 4, latent), jnp.float32),
                pltpu.VMEM((nj, 2, len(REDUCE), heads // 4, latent), jnp.float32),
                pltpu.VMEM((nj, 4, nt, heads), jnp.float32),
                pltpu.VMEM((nj, 4, nt, heads), jnp.float32),
                pltpu.VMEM((nt, heads), jnp.float32),
                dma((DEPTH, 2)), dma((nj,)), dma((nj,)), dma(()), dma(()),
                dma((nj, 2)), dma((nj, 2, 8)), dma((nj, 2)), dma((nj, 2, 2, 3)), dma((nj, 2)), dma((nj, 2)),
            ],
            compiler_params=pltpu.CompilerParams(collective_id=0, has_side_effects=True, vmem_limit_bytes=54_000_000),
        )(len_blk, q, cache)
        return out

    return jax.shard_map(local_step, mesh=mesh, in_specs=(P('dp', AXIS, None), P('dp', None, AXIS, None, None), P('dp')),
                         out_specs=P(('dp', AXIS), None, None), check_vma=False)
```

```python
import functools
import math

import jax
import jax.numpy as jnp
from jax import lax
from jax.experimental import pallas as pl
from jax.experimental.pallas import tpu as pltpu
from jax.sharding import PartitionSpec as P

ROPE_DIM = 64
QK_DIM = 192
AXIS = 'dcp'
DEPTH = 3
SLICES = 4

FIRST, SECOND = 0, 1
FULL, LOW, HIGH = 0, 1, 2
GATHER = (
    (FIRST, 1, (0, 0), FULL, 0),
    (FIRST, -1, (0, 0), FULL, 1),
    (FIRST, 1, (-1, 0), LOW, 2),
    (FIRST, -1, (1, 0), HIGH, 2),
    (SECOND, 1, (0, 0), FULL, 3),
    (SECOND, 1, (-1, 0), FULL, 4),
    (SECOND, 1, (1, 0), FULL, 7),
    (SECOND, 1, (2, 0), FULL, 7),
    (SECOND, -1, (0, 0), FULL, 7),
    (SECOND, -1, (-1, 0), FULL, 7),
    (SECOND, -1, (1, 0), FULL, 5),
    (SECOND, -1, (2, 0), FULL, 6),
    (SECOND, 1, (0, -1), FULL, 7),
    (SECOND, 1, (-1, -1), FULL, 7),
    (SECOND, -1, (1, 1), FULL, 7),
    (SECOND, -1, (2, 1), FULL, 7),
)
REDUCE = ((2, LOW, 1, 0), (1, HIGH, 1, 2), (2, HIGH, -1, 1), (-1, LOW, -1, 2), (1, LOW, 1, 2), (-1, HIGH, -1, 2))


def _kernel(side, len_ref, q_ref, cache_ref, out_ref, sib_ref, q_sib, q_all, part, page, xbuf, ybuf, lse_x, lse_y,
            wgt, page_sem, swap_send, swap_recv, qs_send, qs_recv, ag_send, ag_recv, rs_send, rs_recv, ls_send,
            ls_recv):
    nt, nj, own_heads, width = q_sib.shape
    heads, latent = part.shape[3:]
    page_len = page.shape[3]
    half_h, quarter_h = heads // 2, heads // 4
    tiles = q_all.shape[3]
    quarter_q, half_q = tiles // 4, tiles // 2
    columns = latent // 128

    me = lax.axis_index(AXIS)
    core = lax.rem(me, 2)
    xpos = lax.rem(me // 2, side)
    ypos = me // (2 * side)
    sibling = me + 1 - 2 * core

    def wrap(pos, step):
        return lax.rem(pos + (step + side), side)

    def neighbour(axis, half, step):
        if axis == half:
            return (ypos * side + wrap(xpos, step)) * 2 + core
        return (wrap(ypos, step) * side + xpos) * 2 + core

    def peer(dev):
        return {AXIS: dev}

    def remote(ref, dst, send_sem, recv_sem, dev):
        return pltpu.make_async_remote_copy(src_ref=ref, dst_ref=dst, send_sem=send_sem, recv_sem=recv_sem,
                                            device_id=peer(dev), device_id_type=pl.DeviceIdType.MESH)

    def gather_block(j, half, first, second, rng):
        if half == 0:
            yy, xx = wrap(ypos, second), wrap(xpos, first)
        else:
            yy, xx = wrap(ypos, first), wrap(xpos, second)
        start = half * half_q + (quarter_q if rng == HIGH else 0)
        return q_all.at[j, yy, xx, pl.ds(start, half_q if rng == FULL else quarter_q)]

    def gather_send(j, *indices):
        for idx in indices:
            for half in (0, 1):
                axis, step, (first, second), rng, sem = GATHER[idx]
                ref = gather_block(j, half, first, second, rng)
                remote(ref, ref, ag_send.at[j, 0 if rng == FULL else 1], ag_recv.at[j, half, sem],
                       neighbour(axis, half, step)).start()

    def wait_bytes(ref, sem):
        pltpu.make_async_copy(ref, ref, sem).wait()

    def gather_wait(j, half, sem):
        ref = q_all.at[j, 0] if sem == 7 else gather_block(j, half, 0, 0, FULL)
        wait_bytes(ref, ag_recv.at[j, half, sem])

    def rows_of(half, rng):
        return half * half_h + (quarter_h if rng == HIGH else 0)

    def first_part(r, half, step, rng, i=None):
        hs = pl.ds(rows_of(half, rng), quarter_h)
        second = slice(None) if i is None else i
        if half == 0:
            return part.at[r, second, wrap(xpos, step), hs]
        return part.at[r, wrap(ypos, step), second, hs]

    def second_part(r, half, step, rng):
        hs = pl.ds(rows_of(half, rng), quarter_h)
        if half == 0:
            return part.at[r, wrap(ypos, step), xpos, hs]
        return part.at[r, ypos, wrap(xpos, step), hs]

    def reduce_send(r, axis, *indices):
        for idx in indices:
            for half in (0, 1):
                dest, rng, step, sem = REDUCE[idx]
                src = (first_part if axis == FIRST else second_part)(r, half, dest, rng)
                dst = (xbuf if axis == FIRST else ybuf).at[r, half, idx]
                remote(src, dst, rs_send.at[r, axis], rs_recv.at[r, half, axis, sem], neighbour(axis, half, step)).start()

    def reduce_wait(r, axis, half, sem):
        buf = xbuf if axis == FIRST else ybuf
        wait_bytes(buf.at[r, half, pl.ds(0, 4)] if sem == 2 else buf.at[r, half, 0], rs_recv.at[r, half, axis, sem])

    def lse_buf(axis):
        return lse_x if axis == 0 else lse_y

    def lse_send(j, axis):
        buf = lse_buf(axis)
        for idx, step in enumerate((1, -1, 2)):
            remote(buf.at[j, 0], buf.at[j, idx + 1], ls_send.at[j, axis], ls_recv.at[j, axis], neighbour(axis, 0, step)).start()

    def lse_wait(j, axis):
        wait_bytes(lse_buf(axis).at[j, pl.ds(0, 3)], ls_recv.at[j, axis])

    def swap_piece(j, n):
        ts = pl.ds(n * (nt // SLICES), nt // SLICES)
        remote(cache_ref.at[ts, 1 - core, j], sib_ref.at[j, ts], swap_send.at[j], swap_recv.at[j], sibling).start()

    def query_swap():
        return remote(q_ref.at[:, 1 - core], q_sib, qs_send, qs_recv, sibling)

    def load_pages(n):
        slot, j, t = lax.rem(n, DEPTH), n // nt, lax.rem(n, nt)
        for p, src in ((0, cache_ref.at[t, core, j]), (1, sib_ref.at[j, t])):
            pltpu.make_async_copy(src, page.at[slot, p, pl.ds(0, width)], page_sem.at[slot, p]).start()
            pltpu.make_async_copy(src.at[pl.ds(latent, ROPE_DIM)], page.at[slot, p, pl.ds(width, ROPE_DIM)],
                                  page_sem.at[slot, p]).start()

    def merge_queries(j):
        for t in range(nt):
            mine = q_ref[t, core, j].astype(jnp.float32)
            other = q_sib[t, j].astype(jnp.float32)
            both = jnp.concatenate([jnp.where(core == 0, mine, other), jnp.where(core == 0, other, mine)], axis=0)
            base, sub = (t // 4) * quarter_q, t % 4
            for i in range(columns):
                q_all[j, ypos, xpos, base + sub * columns + i] = both[:, i * 128:(i + 1) * 128].astype(jnp.bfloat16)
            rope = both[:, latent:]
            if sub < 2:
                low = (low if sub else []) + [rope]
            else:
                q_all[j, ypos, xpos, base + 4 * columns + sub - 2] = jnp.concatenate([low[sub - 2], rope], axis=1).astype(
                    jnp.bfloat16)

    def gather_first(j):
        for sem, sends in ((0, (2, 5, 9)), (1, (3, 6, 10))):
            for half in (0, 1):
                gather_wait(j, half, sem)
            gather_send(j, *sends)

    def gather_turn(j):
        for half in (0, 1):
            gather_wait(j, half, 2)
        gather_send(j, 7, 11)

    def gather_second(j, sem, send):
        for half in (0, 1):
            gather_wait(j, half, sem)
        gather_send(j, send)

    def gather_end(j):
        for half in (0, 1):
            gather_wait(j, half, 7)

    def swap_wait(j):
        wait_bytes(sib_ref.at[j], swap_recv.at[j])

    def attend(n):
        @pl.when(n + DEPTH - 1 < nj * nt)
        def _():
            load_pages(n + DEPTH - 1)

        slot, j, t = lax.rem(n, DEPTH), n // nt, lax.rem(n, nt)
        for p in (0, 1):
            wait_bytes(page.at[slot, p], page_sem.at[slot, p])
        base, sub = (t // 4) * quarter_q, lax.rem(t, 4)
        cols = [q_all[j, :, :, base + sub * columns + i].reshape(heads, 128) for i in range(columns)]
        rope = q_all[j, :, :, base + 4 * columns + lax.rem(sub, 2)].reshape(heads, 128)
        lane_half = lax.broadcasted_iota(jnp.int32, (heads, 128), 1) // ROPE_DIM
        cols.append(jnp.where(lane_half == sub // 2, rope, jnp.zeros_like(rope)))
        q = jnp.concatenate(cols, axis=1)
        limit = len_ref[(t * 2 + core) * nj + j]
        outs, lses = [], []
        for p in (0, 1):
            owner = me if p == 0 else sibling
            s = jnp.dot(q, page[slot, p], preferred_element_type=jnp.float32) * (QK_DIM ** -0.5)
            position = owner * page_len + lax.broadcasted_iota(jnp.int32, (1, page_len), 1)
            s = jnp.where(position < limit, s, -1e30)
            m = jnp.max(s, axis=1, keepdims=True)
            w = jnp.exp(s - m)
            l = jnp.sum(w, axis=1, keepdims=True)
            pv = lax.dot_general(w.astype(jnp.bfloat16), page[slot, p, :latent], (((1,), (1,)), ((), ())),
                                 preferred_element_type=jnp.float32)
            outs.append((pv * (1.0 / l)).astype(jnp.bfloat16).astype(jnp.float32))
            lses.append(m + jnp.log(l))
        top = jnp.maximum(lses[0], lses[1])
        both = top + jnp.log(jnp.exp(lses[0] - top) + jnp.exp(lses[1] - top))
        part[j, t // side, lax.rem(t, side)] = jnp.exp(lses[0] - both) * outs[0] + jnp.exp(lses[1] - both) * outs[1]
        row = jnp.broadcast_to(both, (heads, 128)).T
        lse_x[j, 0, pl.ds(t, 1), :] = row[0:1]

    def combine(v):
        top = jnp.max(v, axis=0)
        return top + jnp.log(jnp.sum(jnp.exp(v - top[None]), axis=0))

    def lse_turn(j):
        lse_wait(j, 0)
        lse_y[j, 0] = combine(lse_x[j])
        lse_send(j, 1)

    def weigh(j):
        lse_wait(j, 1)
        wgt[...] = jnp.exp(lse_x[j, 0] - combine(lse_y[j]))

        def body(t, _):
            w = jnp.broadcast_to(wgt[pl.ds(t, 1), :], (128, heads)).T
            yy, xx = t // side, lax.rem(t, side)
            for i in range(latent // 128):
                cols = pl.ds(i * 128, 128)
                part[j, yy, xx, :, cols] = part[j, yy, xx, :, cols] * w
            return 0

        lax.fori_loop(0, nt, body, 0)

    def reduce_turn(r, axis):
        for idx, dest, rng, nxt, sem in ((0, 1, LOW, 4, 0), (2, -1, HIGH, 5, 1)):
            for half in (0, 1):
                reduce_wait(r, axis, half, sem)
                if axis == FIRST:
                    def body(i, _):
                        ref = first_part(r, half, dest, rng, i)
                        ref[...] = ref[...] + xbuf[r, half, idx, i]
                        return 0
                    lax.fori_loop(0, side, body, 0)
                else:
                    ref = second_part(r, half, dest, rng)
                    ref[...] = ref[...] + ybuf[r, half, idx]
            reduce_send(r, axis, nxt)

    def reduce_end(r, axis):
        for half in (0, 1):
            reduce_wait(r, axis, half, 2)
            for rng, one, two in ((HIGH, 1, 5), (LOW, 3, 4)):
                if axis == FIRST:
                    def body(i, _):
                        ref = first_part(r, half, 0, rng, i)
                        ref[...] = ref[...] + (xbuf[r, half, one, i] + xbuf[r, half, two, i])
                        return 0
                    lax.fori_loop(0, side, body, 0)
                else:
                    total = second_part(r, half, 0, rng)[...] + (ybuf[r, half, one] + ybuf[r, half, two])
                    out_ref[r, pl.ds(rows_of(half, rng), quarter_h)] = total.astype(out_ref.dtype)

    barrier = pltpu.get_barrier_semaphore()
    peers = [sibling] + [neighbour(axis, 0, step) for axis in (0, 1) for step in (1, -1, 2)]
    for dev in peers:
        pl.semaphore_signal(barrier, inc=1, device_id=peer(dev), device_id_type=pl.DeviceIdType.MESH)
    with jax.named_scope('barrier'):
        pl.semaphore_wait(barrier, len(peers))

    query_swap().start()
    with jax.named_scope('merge0'):
        query_swap().wait_recv()
        merge_queries(0)
    gather_send(0, 0, 1, 4, 8)
    swap_piece(0, 0)
    swap_piece(0, 1)
    with jax.named_scope('merges'):
        lax.fori_loop(1, nj, lambda j, _: (merge_queries(j), 0)[1], 0)
    with jax.named_scope('chunk0'):
        gather_first(0)
        swap_piece(0, 2)
        gather_second(0, 3, 12)
        gather_turn(0)
        gather_send(1, 0, 1)
        swap_piece(0, 3)
        gather_second(0, 4, 13)
        gather_second(0, 5, 14)
        gather_second(0, 6, 15)
    with jax.named_scope('chunk1'):
        swap_piece(1, 0)
        gather_first(1)
        gather_send(1, 4, 8)
        gather_send(2, 0, 1)
        swap_piece(1, 1)
        swap_wait(0)
        for n in range(DEPTH - 1):
            load_pages(n)
        gather_end(0)

    def run(*steps):
        for fn, *args in steps:
            with jax.named_scope(fn.__name__ + '_' + '_'.join(str(a) for a in args)):
                fn(*args)

    def middle(j):
        run((gather_turn, j), (gather_second, j, 4, 13), (gather_second, j, 5, 14), (gather_second, j, 3, 12))

    slots = {
        0: ((swap_piece, 1, 2),),
        1: ((middle, 1), (swap_piece, 1, 3)),
        2: ((swap_piece, 2, 0),),
        3: ((gather_second, 1, 6, 15), (gather_first, 2), (gather_send, 2, 4, 8), (gather_send, 3, 0, 1), (swap_wait, 1),
            (swap_piece, 2, 1)),
        4: ((lse_send, 0, 0), (gather_end, 1), (swap_piece, 2, 2)),
        5: ((lse_turn, 0), (swap_piece, 2, 3)),
        6: ((middle, 2), (swap_piece, 3, 0)),
        7: ((gather_second, 2, 6, 15), (gather_first, 3), (gather_send, 3, 4, 8), (weigh, 0), (swap_wait, 2), (swap_piece, 3, 1)),
        8: ((lse_send, 1, 0), (gather_end, 2), (reduce_send, 0, FIRST, 0, 2), (swap_piece, 3, 2)),
        9: ((middle, 3), (swap_piece, 3, 3)),
        10: ((lse_turn, 1),),
        11: ((gather_second, 3, 6, 15), (reduce_send, 0, FIRST, 1, 3), (swap_wait, 3)),
        12: ((lse_send, 2, 0), (reduce_turn, 0, FIRST), (gather_end, 3)),
        13: ((weigh, 1), (reduce_send, 1, FIRST, 0, 2)),
        15: ((lse_turn, 2), (reduce_send, 1, FIRST, 1, 3)),
    }

    def slot_body(n, _):
        for at, steps in slots.items():
            pl.when(n == at)(functools.partial(run, *steps))
        with jax.named_scope('attend'):
            lax.fori_loop(n * (nt // SLICES), (n + 1) * (nt // SLICES), lambda i, _: (attend(i), 0)[1], 0)
        return 0

    lax.fori_loop(0, nj * SLICES, slot_body, 0)

    early = (0, 2, 1, 3)
    run((lse_send, 3, 0), (reduce_end, 0, FIRST), (reduce_send, 0, SECOND, *early))
    run((reduce_turn, 1, FIRST), (lse_turn, 3), (reduce_turn, 0, SECOND), (weigh, 2), (reduce_send, 2, FIRST, *early),
        (reduce_end, 1, FIRST), (reduce_send, 1, SECOND, *early), (reduce_end, 0, SECOND))
    run((reduce_turn, 2, FIRST), (reduce_turn, 1, SECOND), (weigh, 3), (reduce_send, 3, FIRST, *early),
        (reduce_end, 2, FIRST), (reduce_send, 2, SECOND, *early), (reduce_end, 1, SECOND))
    run((reduce_turn, 3, FIRST), (reduce_turn, 2, SECOND), (reduce_end, 3, FIRST), (reduce_send, 3, SECOND, *early),
        (reduce_end, 2, SECOND))
    run((reduce_turn, 3, SECOND), (reduce_end, 3, SECOND))

    def drain(j, _):
        wait_bytes(sib_ref.at[j], swap_send.at[j])
        wait_bytes(q_all.at[j, :, :, pl.ds(0, 14 * tiles // 16)], ag_send.at[j, 0])
        wait_bytes(q_all.at[j, 0, 0], ag_send.at[j, 1])
        wait_bytes(xbuf.at[j], rs_send.at[j, 0])
        wait_bytes(ybuf.at[j], rs_send.at[j, 1])
        for axis in (0, 1):
            wait_bytes(lse_buf(axis).at[j, pl.ds(0, 3)], ls_send.at[j, axis])
        return 0

    with jax.named_scope('drain'):
        query_swap().wait_send()
        lax.fori_loop(0, nj, drain, 0)


def solution(mesh):
    group_size = mesh.shape[AXIS]
    side = math.isqrt(group_size // 2)
    nt = side * side

    def local_step(q_blk, cache_blk, len_blk):
        batch_rows, own_heads, width = q_blk.shape
        page_len = cache_blk.shape[3]
        latent = width - ROPE_DIM
        nj = batch_rows // group_size
        heads = 2 * own_heads * nt
        tiles = nt * (latent // 128) + nt // 2
        q = q_blk.reshape(nt, 2, nj, own_heads, width)
        cache = jnp.swapaxes(cache_blk.reshape(nt, 2, nj, page_len, width), 3, 4)
        any_space = pl.BlockSpec(memory_space=pl.ANY)
        dma = pltpu.SemaphoreType.DMA
        out, _ = pl.pallas_call(
            functools.partial(_kernel, side),
            out_shape=(jax.ShapeDtypeStruct((nj, heads, latent), jnp.bfloat16),
                       jax.ShapeDtypeStruct((nj, nt, width, page_len), jnp.bfloat16)),
            in_specs=[pl.BlockSpec(memory_space=pltpu.SMEM), pl.BlockSpec(memory_space=pltpu.VMEM), any_space],
            out_specs=(pl.BlockSpec(memory_space=pltpu.VMEM), any_space),
            scratch_shapes=[
                pltpu.VMEM((nt, nj, own_heads, width), jnp.bfloat16),
                pltpu.VMEM((nj, side, side, tiles, 2 * own_heads, 128), jnp.bfloat16),
                pltpu.VMEM((nj, side, side, heads, latent), jnp.float32),
                pltpu.VMEM((DEPTH, 2, width + ROPE_DIM, page_len), jnp.bfloat16),
                pltpu.VMEM((nj, 2, len(REDUCE), side, heads // 4, latent), jnp.float32),
                pltpu.VMEM((nj, 2, len(REDUCE), heads // 4, latent), jnp.float32),
                pltpu.VMEM((nj, 4, nt, heads), jnp.float32),
                pltpu.VMEM((nj, 4, nt, heads), jnp.float32),
                pltpu.VMEM((nt, heads), jnp.float32),
                dma((DEPTH, 2)), dma((nj,)), dma((nj,)), dma(()), dma(()),
                dma((nj, 2)), dma((nj, 2, 8)), dma((nj, 2)), dma((nj, 2, 2, 3)), dma((nj, 2)), dma((nj, 2)),
            ],
            compiler_params=pltpu.CompilerParams(collective_id=0, has_side_effects=True, vmem_limit_bytes=54_000_000),
        )(len_blk, q, cache)
        return out

    return jax.shard_map(local_step, mesh=mesh, in_specs=(P('dp', AXIS, None), P('dp', None, AXIS, None, None), P('dp')),
                         out_specs=P(('dp', AXIS), None, None), check_vma=False)
```

```python
import functools
import math

import jax
import jax.numpy as jnp
from jax import lax
from jax.experimental import pallas as pl
from jax.experimental.pallas import tpu as pltpu
from jax.sharding import PartitionSpec as P

ROPE_DIM = 64
QK_DIM = 192
AXIS = 'dcp'
DEPTH = 3
SLICES = 4

FIRST, SECOND = 0, 1
FULL, LOW, HIGH = 0, 1, 2
GATHER = (
    (FIRST, 1, (0, 0), FULL, 0),
    (FIRST, -1, (0, 0), FULL, 1),
    (FIRST, 1, (-1, 0), LOW, 2),
    (FIRST, -1, (1, 0), HIGH, 2),
    (SECOND, 1, (0, 0), FULL, 3),
    (SECOND, 1, (-1, 0), FULL, 4),
    (SECOND, 1, (1, 0), FULL, 7),
    (SECOND, 1, (2, 0), FULL, 7),
    (SECOND, -1, (0, 0), FULL, 7),
    (SECOND, -1, (-1, 0), FULL, 7),
    (SECOND, -1, (1, 0), FULL, 5),
    (SECOND, -1, (2, 0), FULL, 6),
    (SECOND, 1, (0, -1), FULL, 7),
    (SECOND, 1, (-1, -1), FULL, 7),
    (SECOND, -1, (1, 1), FULL, 7),
    (SECOND, -1, (2, 1), FULL, 7),
)
REDUCE = ((2, LOW, 1, 0), (1, HIGH, 1, 2), (2, HIGH, -1, 1), (-1, LOW, -1, 2), (1, LOW, 1, 2), (-1, HIGH, -1, 2))


def _kernel(side, len_ref, q_ref, cache_ref, out_ref, sib_ref, q_sib, q_all, part, page, xbuf, ybuf, lse_x, lse_y,
            wgt, page_sem, swap_send, swap_recv, qs_send, qs_recv, ag_send, ag_recv, rs_send, rs_recv, ls_send,
            ls_recv):
    nt, nj, own_heads, width = q_sib.shape
    heads, latent = part.shape[3:]
    page_len = page.shape[3]
    half_h, quarter_h = heads // 2, heads // 4
    tiles = q_all.shape[3]
    quarter_q, half_q = tiles // 4, tiles // 2
    columns = latent // 128

    me = lax.axis_index(AXIS)
    core = lax.rem(me, 2)
    xpos = lax.rem(me // 2, side)
    ypos = me // (2 * side)
    sibling = me + 1 - 2 * core

    def wrap(pos, step):
        return lax.rem(pos + (step + side), side)

    def neighbour(axis, half, step):
        if axis == half:
            return (ypos * side + wrap(xpos, step)) * 2 + core
        return (wrap(ypos, step) * side + xpos) * 2 + core

    def peer(dev):
        return {AXIS: dev}

    def remote(ref, dst, send_sem, recv_sem, dev):
        return pltpu.make_async_remote_copy(src_ref=ref, dst_ref=dst, send_sem=send_sem, recv_sem=recv_sem,
                                            device_id=peer(dev), device_id_type=pl.DeviceIdType.MESH)

    def gather_block(j, half, first, second, rng):
        if half == 0:
            yy, xx = wrap(ypos, second), wrap(xpos, first)
        else:
            yy, xx = wrap(ypos, first), wrap(xpos, second)
        start = half * half_q + (quarter_q if rng == HIGH else 0)
        return q_all.at[j, yy, xx, pl.ds(start, half_q if rng == FULL else quarter_q)]

    def gather_send(j, *indices):
        for idx in indices:
            for half in (0, 1):
                axis, step, (first, second), rng, sem = GATHER[idx]
                ref = gather_block(j, half, first, second, rng)
                remote(ref, ref, ag_send.at[j, 0 if rng == FULL else 1], ag_recv.at[j, half, sem],
                       neighbour(axis, half, step)).start()

    def wait_bytes(ref, sem):
        pltpu.make_async_copy(ref, ref, sem).wait()

    def gather_wait(j, half, sem):
        ref = q_all.at[j, 0] if sem == 7 else gather_block(j, half, 0, 0, FULL)
        wait_bytes(ref, ag_recv.at[j, half, sem])

    def rows_of(half, rng):
        return half * half_h + (quarter_h if rng == HIGH else 0)

    def first_part(r, half, step, rng, i=None):
        hs = pl.ds(rows_of(half, rng), quarter_h)
        second = slice(None) if i is None else i
        if half == 0:
            return part.at[r, second, wrap(xpos, step), hs]
        return part.at[r, wrap(ypos, step), second, hs]

    def second_part(r, half, step, rng):
        hs = pl.ds(rows_of(half, rng), quarter_h)
        if half == 0:
            return part.at[r, wrap(ypos, step), xpos, hs]
        return part.at[r, ypos, wrap(xpos, step), hs]

    def reduce_send(r, axis, *indices):
        for idx in indices:
            for half in (0, 1):
                dest, rng, step, sem = REDUCE[idx]
                src = (first_part if axis == FIRST else second_part)(r, half, dest, rng)
                dst = (xbuf if axis == FIRST else ybuf).at[r, half, idx]
                remote(src, dst, rs_send.at[r, axis], rs_recv.at[r, half, axis, sem], neighbour(axis, half, step)).start()

    def reduce_wait(r, axis, half, sem):
        buf = xbuf if axis == FIRST else ybuf
        wait_bytes(buf.at[r, half, pl.ds(0, 4)] if sem == 2 else buf.at[r, half, 0], rs_recv.at[r, half, axis, sem])

    def lse_buf(axis):
        return lse_x if axis == 0 else lse_y

    def lse_send(j, axis):
        buf = lse_buf(axis)
        for idx, step in enumerate((1, -1, 2)):
            remote(buf.at[j, 0], buf.at[j, idx + 1], ls_send.at[j, axis], ls_recv.at[j, axis], neighbour(axis, 0, step)).start()

    def lse_wait(j, axis):
        wait_bytes(lse_buf(axis).at[j, pl.ds(0, 3)], ls_recv.at[j, axis])

    def swap_piece(j, n):
        ts = pl.ds(n * (nt // SLICES), nt // SLICES)
        remote(cache_ref.at[ts, 1 - core, j], sib_ref.at[j, ts], swap_send.at[j], swap_recv.at[j], sibling).start()

    def query_swap():
        return remote(q_ref.at[:, 1 - core], q_sib, qs_send, qs_recv, sibling)

    def load_pages(n):
        slot, j, t = lax.rem(n, DEPTH), n // nt, lax.rem(n, nt)
        for p, src in ((0, cache_ref.at[t, core, j]), (1, sib_ref.at[j, t])):
            pltpu.make_async_copy(src, page.at[slot, p, pl.ds(0, width)], page_sem.at[slot, p]).start()
            pltpu.make_async_copy(src.at[pl.ds(latent, ROPE_DIM)], page.at[slot, p, pl.ds(width, ROPE_DIM)],
                                  page_sem.at[slot, p]).start()

    def merge_queries(j):
        for t in range(nt):
            mine = q_ref[t, core, j].astype(jnp.float32)
            other = q_sib[t, j].astype(jnp.float32)
            both = jnp.concatenate([jnp.where(core == 0, mine, other), jnp.where(core == 0, other, mine)], axis=0)
            base, sub = (t // 4) * quarter_q, t % 4
            for i in range(columns):
                q_all[j, ypos, xpos, base + sub * columns + i] = both[:, i * 128:(i + 1) * 128].astype(jnp.bfloat16)
            rope = both[:, latent:]
            if sub < 2:
                low = (low if sub else []) + [rope]
            else:
                q_all[j, ypos, xpos, base + 4 * columns + sub - 2] = jnp.concatenate([low[sub - 2], rope], axis=1).astype(
                    jnp.bfloat16)

    def gather_first(j):
        for sem, sends in ((0, (2, 5, 9)), (1, (3, 6, 10))):
            for half in (0, 1):
                gather_wait(j, half, sem)
            gather_send(j, *sends)

    def gather_turn(j):
        for half in (0, 1):
            gather_wait(j, half, 2)
        gather_send(j, 7, 11)

    def gather_second(j, sem, send):
        for half in (0, 1):
            gather_wait(j, half, sem)
        gather_send(j, send)

    def gather_end(j):
        for half in (0, 1):
            gather_wait(j, half, 7)

    def swap_wait(j):
        wait_bytes(sib_ref.at[j], swap_recv.at[j])

    def attend(n):
        @pl.when(n + DEPTH - 1 < nj * nt)
        def _():
            load_pages(n + DEPTH - 1)

        slot, j, t = lax.rem(n, DEPTH), n // nt, lax.rem(n, nt)
        for p in (0, 1):
            wait_bytes(page.at[slot, p], page_sem.at[slot, p])
        base, sub = (t // 4) * quarter_q, lax.rem(t, 4)
        cols = [q_all[j, :, :, base + sub * columns + i].reshape(heads, 128) for i in range(columns)]
        rope = q_all[j, :, :, base + 4 * columns + lax.rem(sub, 2)].reshape(heads, 128)
        lane_half = lax.broadcasted_iota(jnp.int32, (heads, 128), 1) // ROPE_DIM
        cols.append(jnp.where(lane_half == sub // 2, rope, jnp.zeros_like(rope)))
        q = jnp.concatenate(cols, axis=1)
        limit = len_ref[(t * 2 + core) * nj + j]
        outs, lses = [], []
        for p in (0, 1):
            owner = me if p == 0 else sibling
            s = jnp.dot(q, page[slot, p], preferred_element_type=jnp.float32) * (QK_DIM ** -0.5)
            position = owner * page_len + lax.broadcasted_iota(jnp.int32, (1, page_len), 1)
            s = jnp.where(position < limit, s, -1e30)
            m = jnp.max(s, axis=1, keepdims=True)
            w = jnp.exp(s - m)
            l = jnp.sum(w, axis=1, keepdims=True)
            pv = lax.dot_general(w.astype(jnp.bfloat16), page[slot, p, :latent], (((1,), (1,)), ((), ())),
                                 preferred_element_type=jnp.float32)
            outs.append((pv * (1.0 / l)).astype(jnp.bfloat16).astype(jnp.float32))
            lses.append(m + jnp.log(l))
        top = jnp.maximum(lses[0], lses[1])
        both = top + jnp.log(jnp.exp(lses[0] - top) + jnp.exp(lses[1] - top))
        part[j, t // side, lax.rem(t, side)] = jnp.exp(lses[0] - both) * outs[0] + jnp.exp(lses[1] - both) * outs[1]
        row = jnp.broadcast_to(both, (heads, 128)).T
        lse_x[j, 0, pl.ds(t, 1), :] = row[0:1]

    def combine(v):
        top = jnp.max(v, axis=0)
        return top + jnp.log(jnp.sum(jnp.exp(v - top[None]), axis=0))

    def lse_turn(j):
        lse_wait(j, 0)
        lse_y[j, 0] = combine(lse_x[j])
        lse_send(j, 1)

    def weigh(j):
        lse_wait(j, 1)
        wgt[...] = jnp.exp(lse_x[j, 0] - combine(lse_y[j]))

        def body(t, _):
            w = jnp.broadcast_to(wgt[pl.ds(t, 1), :], (128, heads)).T
            yy, xx = t // side, lax.rem(t, side)
            for i in range(latent // 128):
                cols = pl.ds(i * 128, 128)
                part[j, yy, xx, :, cols] = part[j, yy, xx, :, cols] * w
            return 0

        lax.fori_loop(0, nt, body, 0)

    def reduce_turn(r, axis):
        for idx, dest, rng, nxt, sem in ((0, 1, LOW, 4, 0), (2, -1, HIGH, 5, 1)):
            for half in (0, 1):
                reduce_wait(r, axis, half, sem)
                if axis == FIRST:
                    def body(i, _):
                        ref = first_part(r, half, dest, rng, i)
                        ref[...] = ref[...] + xbuf[r, half, idx, i]
                        return 0
                    lax.fori_loop(0, side, body, 0)
                else:
                    ref = second_part(r, half, dest, rng)
                    ref[...] = ref[...] + ybuf[r, half, idx]
            reduce_send(r, axis, nxt)

    def reduce_end(r, axis):
        for half in (0, 1):
            reduce_wait(r, axis, half, 2)
            for rng, one, two in ((HIGH, 1, 5), (LOW, 3, 4)):
                if axis == FIRST:
                    def body(i, _):
                        ref = first_part(r, half, 0, rng, i)
                        ref[...] = ref[...] + (xbuf[r, half, one, i] + xbuf[r, half, two, i])
                        return 0
                    lax.fori_loop(0, side, body, 0)
                else:
                    total = second_part(r, half, 0, rng)[...] + (ybuf[r, half, one] + ybuf[r, half, two])
                    out_ref[r, pl.ds(rows_of(half, rng), quarter_h)] = total.astype(out_ref.dtype)

    barrier = pltpu.get_barrier_semaphore()
    peers = [sibling] + [neighbour(axis, 0, step) for axis in (0, 1) for step in (1, -1, 2)]
    for dev in peers:
        pl.semaphore_signal(barrier, inc=1, device_id=peer(dev), device_id_type=pl.DeviceIdType.MESH)
    with jax.named_scope('barrier'):
        pl.semaphore_wait(barrier, len(peers))

    query_swap().start()
    with jax.named_scope('merge0'):
        query_swap().wait_recv()
        merge_queries(0)
    gather_send(0, 0, 1, 4, 8)
    swap_piece(0, 0)
    swap_piece(0, 1)
    with jax.named_scope('merges'):
        lax.fori_loop(1, nj, lambda j, _: (merge_queries(j), 0)[1], 0)
    with jax.named_scope('chunk0'):
        gather_first(0)
        swap_piece(0, 2)
        gather_second(0, 3, 12)
        gather_turn(0)
        gather_send(1, 0, 1)
        swap_piece(0, 3)
        gather_second(0, 4, 13)
        gather_second(0, 5, 14)
        gather_second(0, 6, 15)
    with jax.named_scope('chunk1'):
        swap_piece(1, 0)
        gather_first(1)
        gather_send(1, 4, 8)
        gather_send(2, 0, 1)
        swap_piece(1, 1)
        swap_wait(0)
        for n in range(DEPTH - 1):
            load_pages(n)
        gather_end(0)

    def run(*steps):
        for fn, *args in steps:
            with jax.named_scope(fn.__name__ + '_' + '_'.join(str(a) for a in args)):
                fn(*args)

    def middle(j):
        run((gather_turn, j), (gather_second, j, 4, 13), (gather_second, j, 5, 14), (gather_second, j, 3, 12))

    slots = {
        0: ((swap_piece, 1, 2),),
        1: ((gather_send, 2, 4, 8), (gather_send, 3, 0, 1), (swap_piece, 1, 3)),
        2: ((gather_turn, 1), (gather_second, 1, 4, 13), (gather_second, 1, 5, 14), (swap_piece, 2, 0)),
        3: ((gather_second, 1, 3, 12), (gather_first, 2), (swap_wait, 1), (swap_piece, 2, 1)),
        4: ((lse_send, 0, 0), (gather_second, 1, 6, 15), (gather_second, 2, 3, 12), (gather_send, 3, 4, 8), (lse_turn, 0),
            (gather_turn, 2), (gather_end, 1), (gather_second, 2, 4, 13), (gather_second, 2, 5, 14), (gather_first, 3),
            (swap_piece, 2, 2)),
        5: ((gather_second, 2, 6, 15), (swap_piece, 2, 3)),
        6: ((gather_turn, 3), (gather_second, 3, 3, 12), (weigh, 0), (swap_piece, 3, 0)),
        7: ((gather_second, 3, 4, 13), (gather_second, 3, 5, 14), (swap_wait, 2), (swap_piece, 3, 1)),
        8: ((lse_send, 1, 0), (gather_second, 3, 6, 15), (reduce_send, 0, FIRST, 0, 2), (gather_end, 2), (swap_piece, 3, 2)),
        9: ((swap_piece, 3, 3),),
        10: ((lse_turn, 1), (reduce_send, 0, FIRST, 1, 3)),
        11: ((swap_wait, 3),),
        12: ((lse_send, 2, 0), (reduce_turn, 0, FIRST), (gather_end, 3)),
        14: ((lse_turn, 2), (weigh, 1), (reduce_send, 1, FIRST, 0, 2)),
        15: ((reduce_send, 1, FIRST, 1, 3),),
    }

    def slot_body(n, _):
        for at, steps in slots.items():
            pl.when(n == at)(functools.partial(run, *steps))
        with jax.named_scope('attend'):
            lax.fori_loop(n * (nt // SLICES), (n + 1) * (nt // SLICES), lambda i, _: (attend(i), 0)[1], 0)
        return 0

    lax.fori_loop(0, nj * SLICES, slot_body, 0)

    early = (0, 2, 1, 3)
    run((lse_send, 3, 0), (reduce_end, 0, FIRST), (reduce_send, 0, SECOND, *early))
    run((reduce_turn, 1, FIRST), (reduce_turn, 0, SECOND), (lse_turn, 3), (weigh, 2), (reduce_send, 2, FIRST, *early),
        (reduce_end, 1, FIRST), (reduce_send, 1, SECOND, *early), (reduce_end, 0, SECOND))
    run((reduce_turn, 2, FIRST), (reduce_turn, 1, SECOND), (weigh, 3), (reduce_send, 3, FIRST, *early),
        (reduce_end, 2, FIRST), (reduce_send, 2, SECOND, *early), (reduce_end, 1, SECOND))
    run((reduce_turn, 3, FIRST), (reduce_turn, 2, SECOND), (reduce_end, 3, FIRST), (reduce_send, 3, SECOND, *early),
        (reduce_end, 2, SECOND))
    run((reduce_turn, 3, SECOND), (reduce_end, 3, SECOND))

    def drain(j, _):
        wait_bytes(sib_ref.at[j], swap_send.at[j])
        wait_bytes(q_all.at[j, :, :, pl.ds(0, 14 * tiles // 16)], ag_send.at[j, 0])
        wait_bytes(q_all.at[j, 0, 0], ag_send.at[j, 1])
        wait_bytes(xbuf.at[j], rs_send.at[j, 0])
        wait_bytes(ybuf.at[j], rs_send.at[j, 1])
        for axis in (0, 1):
            wait_bytes(lse_buf(axis).at[j, pl.ds(0, 3)], ls_send.at[j, axis])
        return 0

    with jax.named_scope('drain'):
        query_swap().wait_send()
        lax.fori_loop(0, nj, drain, 0)


def solution(mesh):
    group_size = mesh.shape[AXIS]
    side = math.isqrt(group_size // 2)
    nt = side * side

    def local_step(q_blk, cache_blk, len_blk):
        batch_rows, own_heads, width = q_blk.shape
        page_len = cache_blk.shape[3]
        latent = width - ROPE_DIM
        nj = batch_rows // group_size
        heads = 2 * own_heads * nt
        tiles = nt * (latent // 128) + nt // 2
        q = q_blk.reshape(nt, 2, nj, own_heads, width)
        cache = jnp.swapaxes(cache_blk.reshape(nt, 2, nj, page_len, width), 3, 4)
        any_space = pl.BlockSpec(memory_space=pl.ANY)
        dma = pltpu.SemaphoreType.DMA
        out, _ = pl.pallas_call(
            functools.partial(_kernel, side),
            out_shape=(jax.ShapeDtypeStruct((nj, heads, latent), jnp.bfloat16),
                       jax.ShapeDtypeStruct((nj, nt, width, page_len), jnp.bfloat16)),
            in_specs=[pl.BlockSpec(memory_space=pltpu.SMEM), pl.BlockSpec(memory_space=pltpu.VMEM), any_space],
            out_specs=(pl.BlockSpec(memory_space=pltpu.VMEM), any_space),
            scratch_shapes=[
                pltpu.VMEM((nt, nj, own_heads, width), jnp.bfloat16),
                pltpu.VMEM((nj, side, side, tiles, 2 * own_heads, 128), jnp.bfloat16),
                pltpu.VMEM((nj, side, side, heads, latent), jnp.float32),
                pltpu.VMEM((DEPTH, 2, width + ROPE_DIM, page_len), jnp.bfloat16),
                pltpu.VMEM((nj, 2, len(REDUCE), side, heads // 4, latent), jnp.float32),
                pltpu.VMEM((nj, 2, len(REDUCE), heads // 4, latent), jnp.float32),
                pltpu.VMEM((nj, 4, nt, heads), jnp.float32),
                pltpu.VMEM((nj, 4, nt, heads), jnp.float32),
                pltpu.VMEM((nt, heads), jnp.float32),
                dma((DEPTH, 2)), dma((nj,)), dma((nj,)), dma(()), dma(()),
                dma((nj, 2)), dma((nj, 2, 8)), dma((nj, 2)), dma((nj, 2, 2, 3)), dma((nj, 2)), dma((nj, 2)),
            ],
            compiler_params=pltpu.CompilerParams(collective_id=0, has_side_effects=True, vmem_limit_bytes=54_000_000),
        )(len_blk, q, cache)
        return out

    return jax.shard_map(local_step, mesh=mesh, in_specs=(P('dp', AXIS, None), P('dp', None, AXIS, None, None), P('dp')),
                         out_specs=P(('dp', AXIS), None, None), check_vma=False)
```

```python
import functools
import math

import jax
import jax.numpy as jnp
from jax import lax
from jax.experimental import pallas as pl
from jax.experimental.pallas import tpu as pltpu
from jax.sharding import PartitionSpec as P

ROPE_DIM = 64
QK_DIM = 192
AXIS = 'dcp'
DEPTH = 3
SLICES = 4

FIRST, SECOND = 0, 1
FULL, LOW, HIGH = 0, 1, 2
GATHER = (
    (FIRST, 1, (0, 0), FULL, 0),
    (FIRST, -1, (0, 0), FULL, 1),
    (FIRST, 1, (-1, 0), LOW, 2),
    (FIRST, -1, (1, 0), HIGH, 2),
    (SECOND, 1, (0, 0), FULL, 3),
    (SECOND, 1, (-1, 0), FULL, 4),
    (SECOND, 1, (1, 0), FULL, 7),
    (SECOND, 1, (2, 0), FULL, 7),
    (SECOND, -1, (0, 0), FULL, 7),
    (SECOND, -1, (-1, 0), FULL, 7),
    (SECOND, -1, (1, 0), FULL, 5),
    (SECOND, -1, (2, 0), FULL, 6),
    (SECOND, 1, (0, -1), FULL, 7),
    (SECOND, 1, (-1, -1), FULL, 7),
    (SECOND, -1, (1, 1), FULL, 7),
    (SECOND, -1, (2, 1), FULL, 7),
)
REDUCE = ((2, LOW, 1, 0), (1, HIGH, 1, 2), (2, HIGH, -1, 1), (-1, LOW, -1, 2), (1, LOW, 1, 2), (-1, HIGH, -1, 2))


def _kernel(side, len_ref, q_ref, cache_ref, out_ref, sib_ref, q_sib, q_all, part, page, xbuf, ybuf, lse_x, lse_y,
            wgt, page_sem, swap_send, swap_recv, qs_send, qs_recv, ag_send, ag_recv, rs_send, rs_recv, last_recv, ls_send,
            ls_recv):
    nt, nj, own_heads, width = q_sib.shape
    heads, latent = part.shape[3:]
    page_len = page.shape[3]
    half_h, quarter_h = heads // 2, heads // 4
    tiles = q_all.shape[3]
    quarter_q, half_q = tiles // 4, tiles // 2
    columns = latent // 128

    me = lax.axis_index(AXIS)
    core = lax.rem(me, 2)
    xpos = lax.rem(me // 2, side)
    ypos = me // (2 * side)
    sibling = me + 1 - 2 * core

    def wrap(pos, step):
        return lax.rem(pos + (step + side), side)

    def neighbour(axis, half, step):
        if axis == half:
            return (ypos * side + wrap(xpos, step)) * 2 + core
        return (wrap(ypos, step) * side + xpos) * 2 + core

    def peer(dev):
        return {AXIS: dev}

    def remote(ref, dst, send_sem, recv_sem, dev):
        return pltpu.make_async_remote_copy(src_ref=ref, dst_ref=dst, send_sem=send_sem, recv_sem=recv_sem,
                                            device_id=peer(dev), device_id_type=pl.DeviceIdType.MESH)

    def gather_block(j, half, first, second, rng):
        if half == 0:
            yy, xx = wrap(ypos, second), wrap(xpos, first)
        else:
            yy, xx = wrap(ypos, first), wrap(xpos, second)
        start = half * half_q + (quarter_q if rng == HIGH else 0)
        return q_all.at[j, yy, xx, pl.ds(start, half_q if rng == FULL else quarter_q)]

    def gather_send(j, *indices):
        for idx in indices:
            for half in (0, 1):
                axis, step, (first, second), rng, sem = GATHER[idx]
                ref = gather_block(j, half, first, second, rng)
                remote(ref, ref, ag_send.at[j, 0 if rng == FULL else 1], ag_recv.at[j, half, sem],
                       neighbour(axis, half, step)).start()

    def wait_bytes(ref, sem):
        pltpu.make_async_copy(ref, ref, sem).wait()

    def gather_wait(j, half, sem):
        ref = q_all.at[j, 0] if sem == 7 else gather_block(j, half, 0, 0, FULL)
        wait_bytes(ref, ag_recv.at[j, half, sem])

    def rows_of(half, rng):
        return half * half_h + (quarter_h if rng == HIGH else 0)

    def first_part(r, half, step, rng, i=None):
        hs = pl.ds(rows_of(half, rng), quarter_h)
        second = slice(None) if i is None else i
        if half == 0:
            return part.at[r, second, wrap(xpos, step), hs]
        return part.at[r, wrap(ypos, step), second, hs]

    def second_part(r, half, step, rng):
        hs = pl.ds(rows_of(half, rng), quarter_h)
        if half == 0:
            return part.at[r, wrap(ypos, step), xpos, hs]
        return part.at[r, ypos, wrap(xpos, step), hs]

    def reduce_send(r, axis, *indices):
        for idx in indices:
            for half in (0, 1):
                dest, rng, step, sem = REDUCE[idx]
                src = (first_part if axis == FIRST else second_part)(r, half, dest, rng)
                dst = (xbuf if axis == FIRST else ybuf).at[r, half, idx]
                remote(src, dst, rs_send.at[r, axis], rs_recv.at[r, half, axis, sem], neighbour(axis, half, step)).start()

    def reduce_wait(r, axis, half, sem):
        buf = xbuf if axis == FIRST else ybuf
        wait_bytes(buf.at[r, half, pl.ds(0, 4)] if sem == 2 else buf.at[r, half, 0], rs_recv.at[r, half, axis, sem])

    def lse_buf(axis):
        return lse_x if axis == 0 else lse_y

    def lse_send(j, axis):
        buf = lse_buf(axis)
        for idx, step in enumerate((1, -1, 2)):
            remote(buf.at[j, 0], buf.at[j, idx + 1], ls_send.at[j, axis], ls_recv.at[j, axis], neighbour(axis, 0, step)).start()

    def lse_wait(j, axis):
        wait_bytes(lse_buf(axis).at[j, pl.ds(0, 3)], ls_recv.at[j, axis])

    def swap_piece(j, n):
        ts = pl.ds(n * (nt // SLICES), nt // SLICES)
        remote(cache_ref.at[ts, 1 - core, j], sib_ref.at[j, ts], swap_send.at[j], swap_recv.at[j], sibling).start()

    def query_swap():
        return remote(q_ref.at[:, 1 - core], q_sib, qs_send, qs_recv, sibling)

    def load_pages(n):
        slot, j, t = lax.rem(n, DEPTH), n // nt, lax.rem(n, nt)
        for p, src in ((0, cache_ref.at[t, core, j]), (1, sib_ref.at[j, t])):
            pltpu.make_async_copy(src, page.at[slot, p, pl.ds(0, width)], page_sem.at[slot, p]).start()
            pltpu.make_async_copy(src.at[pl.ds(latent, ROPE_DIM)], page.at[slot, p, pl.ds(width, ROPE_DIM)],
                                  page_sem.at[slot, p]).start()

    def merge_queries(j):
        for t in range(nt):
            mine = q_ref[t, core, j].astype(jnp.float32)
            other = q_sib[t, j].astype(jnp.float32)
            both = jnp.concatenate([jnp.where(core == 0, mine, other), jnp.where(core == 0, other, mine)], axis=0)
            base, sub = (t // 4) * quarter_q, t % 4
            for i in range(columns):
                q_all[j, ypos, xpos, base + sub * columns + i] = both[:, i * 128:(i + 1) * 128].astype(jnp.bfloat16)
            rope = both[:, latent:]
            if sub < 2:
                low = (low if sub else []) + [rope]
            else:
                q_all[j, ypos, xpos, base + 4 * columns + sub - 2] = jnp.concatenate([low[sub - 2], rope], axis=1).astype(
                    jnp.bfloat16)

    def gather_first(j):
        for sem, sends in ((0, (2, 5, 9)), (1, (3, 6, 10))):
            for half in (0, 1):
                gather_wait(j, half, sem)
            gather_send(j, *sends)

    def gather_turn(j):
        for half in (0, 1):
            gather_wait(j, half, 2)
        gather_send(j, 7, 11)

    def gather_second(j, sem, send):
        for half in (0, 1):
            gather_wait(j, half, sem)
        gather_send(j, send)

    def gather_end(j):
        for half in (0, 1):
            gather_wait(j, half, 7)

    def swap_wait(j):
        wait_bytes(sib_ref.at[j], swap_recv.at[j])

    def attend(n):
        @pl.when(n + DEPTH - 1 < nj * nt)
        def _():
            load_pages(n + DEPTH - 1)

        slot, j, t = lax.rem(n, DEPTH), n // nt, lax.rem(n, nt)
        for p in (0, 1):
            wait_bytes(page.at[slot, p], page_sem.at[slot, p])
        base, sub = (t // 4) * quarter_q, lax.rem(t, 4)
        cols = [q_all[j, :, :, base + sub * columns + i].reshape(heads, 128) for i in range(columns)]
        rope = q_all[j, :, :, base + 4 * columns + lax.rem(sub, 2)].reshape(heads, 128)
        lane_half = lax.broadcasted_iota(jnp.int32, (heads, 128), 1) // ROPE_DIM
        cols.append(jnp.where(lane_half == sub // 2, rope, jnp.zeros_like(rope)))
        q = jnp.concatenate(cols, axis=1)
        limit = len_ref[(t * 2 + core) * nj + j]
        outs, lses = [], []
        for p in (0, 1):
            owner = me if p == 0 else sibling
            s = jnp.dot(q, page[slot, p], preferred_element_type=jnp.float32) * (QK_DIM ** -0.5)
            position = owner * page_len + lax.broadcasted_iota(jnp.int32, (1, page_len), 1)
            s = jnp.where(position < limit, s, -1e30)
            m = jnp.max(s, axis=1, keepdims=True)
            w = jnp.exp(s - m)
            l = jnp.sum(w, axis=1, keepdims=True)
            pv = lax.dot_general(w.astype(jnp.bfloat16), page[slot, p, :latent], (((1,), (1,)), ((), ())),
                                 preferred_element_type=jnp.float32)
            outs.append((pv * (1.0 / l)).astype(jnp.bfloat16).astype(jnp.float32))
            lses.append(m + jnp.log(l))
        top = jnp.maximum(lses[0], lses[1])
        both = top + jnp.log(jnp.exp(lses[0] - top) + jnp.exp(lses[1] - top))
        part[j, t // side, lax.rem(t, side)] = jnp.exp(lses[0] - both) * outs[0] + jnp.exp(lses[1] - both) * outs[1]
        row = jnp.broadcast_to(both, (heads, 128)).T
        lse_x[j, 0, pl.ds(t, 1), :] = row[0:1]

    def combine(v):
        top = jnp.max(v, axis=0)
        return top + jnp.log(jnp.sum(jnp.exp(v - top[None]), axis=0))

    def lse_turn(j):
        lse_wait(j, 0)
        lse_y[j, 0] = combine(lse_x[j])
        lse_send(j, 1)

    def weigh(j):
        lse_wait(j, 1)
        wgt[...] = jnp.exp(lse_x[j, 0] - combine(lse_y[j]))

        def body(t, _):
            w = jnp.broadcast_to(wgt[pl.ds(t, 1), :], (128, heads)).T
            yy, xx = t // side, lax.rem(t, side)
            for i in range(latent // 128):
                cols = pl.ds(i * 128, 128)
                part[j, yy, xx, :, cols] = part[j, yy, xx, :, cols] * w
            return 0

        lax.fori_loop(0, nt, body, 0)

    def reduce_turn(r, axis):
        for idx, dest, rng, nxt, sem in ((0, 1, LOW, 4, 0), (2, -1, HIGH, 5, 1)):
            for half in (0, 1):
                reduce_wait(r, axis, half, sem)
                if axis == FIRST:
                    def body(i, _):
                        ref = first_part(r, half, dest, rng, i)
                        ref[...] = ref[...] + xbuf[r, half, idx, i]
                        return 0
                    lax.fori_loop(0, side, body, 0)
                else:
                    ref = second_part(r, half, dest, rng)
                    ref[...] = ref[...] + ybuf[r, half, idx]
            reduce_send(r, axis, nxt)

    def reduce_end(r, axis):
        for half in (0, 1):
            reduce_wait(r, axis, half, 2)
            for rng, one, two in ((HIGH, 1, 5), (LOW, 3, 4)):
                if axis == FIRST:
                    def body(i, _):
                        ref = first_part(r, half, 0, rng, i)
                        ref[...] = ref[...] + (xbuf[r, half, one, i] + xbuf[r, half, two, i])
                        return 0
                    lax.fori_loop(0, side, body, 0)
                else:
                    total = second_part(r, half, 0, rng)[...] + (ybuf[r, half, one] + ybuf[r, half, two])
                    out_ref[r, pl.ds(rows_of(half, rng), quarter_h)] = total.astype(out_ref.dtype)

    PIECES = ((2,), (1, -1), (0,))

    def row_of(half, step):
        return wrap(ypos if half == 0 else xpos, step)

    def last_turn(r):
        for half in (0, 1):
            for sem in (0, 1):
                reduce_wait(r, FIRST, half, sem)
        for n, piece in enumerate(PIECES):
            for step in piece:
                for lane, (idx, dest, rng, nxt) in enumerate(((0, 1, LOW, 4), (2, -1, HIGH, 5))):
                    for half in (0, 1):
                        i = row_of(half, step)
                        ref = first_part(r, half, dest, rng, i)
                        ref[...] = ref[...] + xbuf[r, half, idx, i]
                        remote(ref, xbuf.at[r, half, nxt, i], rs_send.at[r, FIRST], last_recv.at[half, lane, n],
                               neighbour(FIRST, half, REDUCE[nxt][2])).start()

    def last_piece(r, n):
        for half in (0, 1):
            if n == 0:
                wait_bytes(xbuf.at[r, half, pl.ds(0, 2)], rs_recv.at[r, half, FIRST, 2])
            for lane in (0, 1):
                wait_bytes(xbuf.at[r, half, 0, pl.ds(0, len(PIECES[n]))], last_recv.at[half, lane, n])
            for step in PIECES[n]:
                i = row_of(half, step)
                for rng, one, two in ((HIGH, 1, 5), (LOW, 3, 4)):
                    ref = first_part(r, half, 0, rng, i)
                    ref[...] = ref[...] + (xbuf[r, half, one, i] + xbuf[r, half, two, i])
        if n < 2:
            reduce_send(r, SECOND, *((0, 2), (1, 3))[n])

    barrier = pltpu.get_barrier_semaphore()
    peers = [sibling] + [neighbour(axis, 0, step) for axis in (0, 1) for step in (1, -1, 2)]
    for dev in peers:
        pl.semaphore_signal(barrier, inc=1, device_id=peer(dev), device_id_type=pl.DeviceIdType.MESH)
    with jax.named_scope('barrier'):
        pl.semaphore_wait(barrier, len(peers))

    query_swap().start()
    with jax.named_scope('merge0'):
        query_swap().wait_recv()
        merge_queries(0)
    gather_send(0, 0, 1, 4, 8)
    swap_piece(0, 0)
    swap_piece(0, 1)
    with jax.named_scope('merges'):
        lax.fori_loop(1, nj, lambda j, _: (merge_queries(j), 0)[1], 0)
    with jax.named_scope('chunk0'):
        gather_first(0)
        swap_piece(0, 2)
        gather_second(0, 3, 12)
        gather_turn(0)
        gather_send(1, 0, 1)
        swap_piece(0, 3)
        gather_second(0, 4, 13)
        gather_second(0, 5, 14)
        gather_second(0, 6, 15)
    with jax.named_scope('chunk1'):
        swap_piece(1, 0)
        gather_first(1)
        gather_send(1, 4, 8)
        gather_send(2, 0, 1)
        swap_piece(1, 1)
        swap_wait(0)
        for n in range(DEPTH - 1):
            load_pages(n)
        gather_end(0)

    def run(*steps):
        for fn, *args in steps:
            with jax.named_scope(fn.__name__ + '_' + '_'.join(str(a) for a in args)):
                fn(*args)

    def middle(j):
        run((gather_turn, j), (gather_second, j, 4, 13), (gather_second, j, 5, 14), (gather_second, j, 3, 12))

    slots = {
        0: ((swap_piece, 1, 2),),
        1: ((gather_send, 2, 4, 8), (gather_send, 3, 0, 1), (swap_piece, 1, 3)),
        2: ((gather_turn, 1), (gather_second, 1, 4, 13), (gather_second, 1, 5, 14), (swap_piece, 2, 0)),
        3: ((gather_second, 1, 3, 12), (gather_first, 2), (swap_wait, 1), (swap_piece, 2, 1)),
        4: ((lse_send, 0, 0), (gather_second, 1, 6, 15), (gather_second, 2, 3, 12), (gather_send, 3, 4, 8), (lse_turn, 0),
            (gather_turn, 2), (gather_end, 1), (gather_second, 2, 4, 13), (gather_second, 2, 5, 14), (gather_first, 3),
            (swap_piece, 2, 2)),
        5: ((gather_second, 2, 6, 15), (swap_piece, 2, 3)),
        6: ((gather_turn, 3), (gather_second, 3, 3, 12), (weigh, 0), (swap_piece, 3, 0)),
        7: ((gather_second, 3, 4, 13), (gather_second, 3, 5, 14), (swap_wait, 2), (swap_piece, 3, 1)),
        8: ((lse_send, 1, 0), (gather_second, 3, 6, 15), (reduce_send, 0, FIRST, 0, 2), (gather_end, 2), (swap_piece, 3, 2)),
        9: ((swap_piece, 3, 3),),
        10: ((lse_turn, 1), (reduce_send, 0, FIRST, 1, 3)),
        11: ((swap_wait, 3),),
        12: ((lse_send, 2, 0), (reduce_turn, 0, FIRST), (gather_end, 3)),
        13: ((weigh, 1), (reduce_send, 1, FIRST, 0, 2)),
        14: ((lse_turn, 2),),
        15: ((reduce_send, 1, FIRST, 1, 3),),
    }

    def slot_body(n, _):
        for at, steps in slots.items():
            pl.when(n == at)(functools.partial(run, *steps))
        with jax.named_scope('attend'):
            lax.fori_loop(n * (nt // SLICES), (n + 1) * (nt // SLICES), lambda i, _: (attend(i), 0)[1], 0)
        return 0

    lax.fori_loop(0, nj * SLICES, slot_body, 0)

    early = (0, 2, 1, 3)
    run((lse_send, 3, 0), (reduce_end, 0, FIRST), (reduce_send, 0, SECOND, *early))
    run((reduce_turn, 1, FIRST), (reduce_turn, 0, SECOND), (lse_turn, 3), (weigh, 2), (reduce_send, 2, FIRST, *early),
        (reduce_end, 1, FIRST), (reduce_send, 1, SECOND, *early), (reduce_end, 0, SECOND))
    run((reduce_turn, 2, FIRST), (reduce_turn, 1, SECOND), (weigh, 3), (reduce_send, 3, FIRST, *early),
        (reduce_end, 2, FIRST), (reduce_send, 2, SECOND, *early), (reduce_end, 1, SECOND))
    run((last_turn, 3), (reduce_turn, 2, SECOND), (last_piece, 3, 0), (last_piece, 3, 1), (last_piece, 3, 2))
    run((reduce_turn, 3, SECOND), (reduce_end, 2, SECOND), (reduce_end, 3, SECOND))

    def drain(j, _):
        wait_bytes(sib_ref.at[j], swap_send.at[j])
        wait_bytes(q_all.at[j, :, :, pl.ds(0, 14 * tiles // 16)], ag_send.at[j, 0])
        wait_bytes(q_all.at[j, 0, 0], ag_send.at[j, 1])
        wait_bytes(xbuf.at[j], rs_send.at[j, 0])
        wait_bytes(ybuf.at[j], rs_send.at[j, 1])
        for axis in (0, 1):
            wait_bytes(lse_buf(axis).at[j, pl.ds(0, 3)], ls_send.at[j, axis])
        return 0

    with jax.named_scope('drain'):
        query_swap().wait_send()
        lax.fori_loop(0, nj, drain, 0)


def solution(mesh):
    group_size = mesh.shape[AXIS]
    side = math.isqrt(group_size // 2)
    nt = side * side

    def local_step(q_blk, cache_blk, len_blk):
        batch_rows, own_heads, width = q_blk.shape
        page_len = cache_blk.shape[3]
        latent = width - ROPE_DIM
        nj = batch_rows // group_size
        heads = 2 * own_heads * nt
        tiles = nt * (latent // 128) + nt // 2
        q = q_blk.reshape(nt, 2, nj, own_heads, width)
        cache = jnp.swapaxes(cache_blk.reshape(nt, 2, nj, page_len, width), 3, 4)
        any_space = pl.BlockSpec(memory_space=pl.ANY)
        dma = pltpu.SemaphoreType.DMA
        out, _ = pl.pallas_call(
            functools.partial(_kernel, side),
            out_shape=(jax.ShapeDtypeStruct((nj, heads, latent), jnp.bfloat16),
                       jax.ShapeDtypeStruct((nj, nt, width, page_len), jnp.bfloat16)),
            in_specs=[pl.BlockSpec(memory_space=pltpu.SMEM), pl.BlockSpec(memory_space=pltpu.VMEM), any_space],
            out_specs=(pl.BlockSpec(memory_space=pltpu.VMEM), any_space),
            scratch_shapes=[
                pltpu.VMEM((nt, nj, own_heads, width), jnp.bfloat16),
                pltpu.VMEM((nj, side, side, tiles, 2 * own_heads, 128), jnp.bfloat16),
                pltpu.VMEM((nj, side, side, heads, latent), jnp.float32),
                pltpu.VMEM((DEPTH, 2, width + ROPE_DIM, page_len), jnp.bfloat16),
                pltpu.VMEM((nj, 2, len(REDUCE), side, heads // 4, latent), jnp.float32),
                pltpu.VMEM((nj, 2, len(REDUCE), heads // 4, latent), jnp.float32),
                pltpu.VMEM((nj, 4, nt, heads), jnp.float32),
                pltpu.VMEM((nj, 4, nt, heads), jnp.float32),
                pltpu.VMEM((nt, heads), jnp.float32),
                dma((DEPTH, 2)), dma((nj,)), dma((nj,)), dma(()), dma(()),
                dma((nj, 2)), dma((nj, 2, 8)), dma((nj, 2)), dma((nj, 2, 2, 3)), dma((2, 2, 3)), dma((nj, 2)), dma((nj, 2)),
            ],
            compiler_params=pltpu.CompilerParams(collective_id=0, has_side_effects=True, vmem_limit_bytes=54_000_000),
        )(len_blk, q, cache)
        return out

    return jax.shard_map(local_step, mesh=mesh, in_specs=(P('dp', AXIS, None), P('dp', None, AXIS, None, None), P('dp')),
                         out_specs=P(('dp', AXIS), None, None), check_vma=False)
```

```python
import functools
import math

import jax
import jax.numpy as jnp
from jax import lax
from jax.experimental import pallas as pl
from jax.experimental.pallas import tpu as pltpu
from jax.sharding import PartitionSpec as P

ROPE_DIM = 64
QK_DIM = 192
AXIS = 'dcp'
DEPTH = 3
SLICES = 4

FIRST, SECOND = 0, 1
FULL, LOW, HIGH = 0, 1, 2
GATHER = (
    (FIRST, 1, (0, 0), FULL, 0),
    (FIRST, -1, (0, 0), FULL, 1),
    (FIRST, 1, (-1, 0), LOW, 2),
    (FIRST, -1, (1, 0), HIGH, 2),
    (SECOND, 1, (0, 0), FULL, 3),
    (SECOND, 1, (-1, 0), FULL, 4),
    (SECOND, 1, (1, 0), FULL, 7),
    (SECOND, 1, (2, 0), FULL, 7),
    (SECOND, -1, (0, 0), FULL, 7),
    (SECOND, -1, (-1, 0), FULL, 7),
    (SECOND, -1, (1, 0), FULL, 5),
    (SECOND, -1, (2, 0), FULL, 6),
    (SECOND, 1, (0, -1), FULL, 7),
    (SECOND, 1, (-1, -1), FULL, 7),
    (SECOND, -1, (1, 1), FULL, 7),
    (SECOND, -1, (2, 1), FULL, 7),
)
REDUCE = ((2, LOW, 1, 0), (1, HIGH, 1, 2), (2, HIGH, -1, 1), (-1, LOW, -1, 2), (1, LOW, 1, 2), (-1, HIGH, -1, 2))


def _kernel(side, len_ref, q_ref, cache_ref, out_ref, sib_ref, q_sib, q_all, part, page, xbuf, ybuf, lse_x, lse_y,
            wgt, page_sem, swap_send, swap_recv, qs_send, qs_recv, ag_send, ag_recv, rs_send, rs_recv, last_recv, ls_send,
            ls_recv):
    nt, nj, own_heads, width = q_sib.shape
    heads, latent = part.shape[3:]
    page_len = page.shape[3]
    half_h, quarter_h = heads // 2, heads // 4
    tiles = q_all.shape[3]
    quarter_q, half_q = tiles // 4, tiles // 2
    columns = latent // 128

    me = lax.axis_index(AXIS)
    core = lax.rem(me, 2)
    xpos = lax.rem(me // 2, side)
    ypos = me // (2 * side)
    sibling = me + 1 - 2 * core

    def wrap(pos, step):
        return lax.rem(pos + (step + side), side)

    def neighbour(axis, half, step):
        if axis == half:
            return (ypos * side + wrap(xpos, step)) * 2 + core
        return (wrap(ypos, step) * side + xpos) * 2 + core

    def peer(dev):
        return {AXIS: dev}

    def remote(ref, dst, send_sem, recv_sem, dev):
        return pltpu.make_async_remote_copy(src_ref=ref, dst_ref=dst, send_sem=send_sem, recv_sem=recv_sem,
                                            device_id=peer(dev), device_id_type=pl.DeviceIdType.MESH)

    def gather_block(j, half, first, second, rng):
        if half == 0:
            yy, xx = wrap(ypos, second), wrap(xpos, first)
        else:
            yy, xx = wrap(ypos, first), wrap(xpos, second)
        start = half * half_q + (quarter_q if rng == HIGH else 0)
        return q_all.at[j, yy, xx, pl.ds(start, half_q if rng == FULL else quarter_q)]

    def gather_send(j, *indices):
        for idx in indices:
            for half in (0, 1):
                axis, step, (first, second), rng, sem = GATHER[idx]
                ref = gather_block(j, half, first, second, rng)
                remote(ref, ref, ag_send.at[j, 0 if rng == FULL else 1], ag_recv.at[j, sem],
                       neighbour(axis, half, step)).start()

    def wait_bytes(ref, sem):
        pltpu.make_async_copy(ref, ref, sem).wait()

    def gather_wait(j, sem):
        wait_bytes(q_all.at[j, pl.ds(0, side // 2)] if sem == 7 else q_all.at[j, 0, 0], ag_recv.at[j, sem])

    def rows_of(half, rng):
        return half * half_h + (quarter_h if rng == HIGH else 0)

    def first_part(r, half, step, rng, i=None):
        hs = pl.ds(rows_of(half, rng), quarter_h)
        second = slice(None) if i is None else i
        if half == 0:
            return part.at[r, second, wrap(xpos, step), hs]
        return part.at[r, wrap(ypos, step), second, hs]

    def second_part(r, half, step, rng):
        hs = pl.ds(rows_of(half, rng), quarter_h)
        if half == 0:
            return part.at[r, wrap(ypos, step), xpos, hs]
        return part.at[r, ypos, wrap(xpos, step), hs]

    def reduce_send(r, axis, *indices):
        for idx in indices:
            for half in (0, 1):
                dest, rng, step, sem = REDUCE[idx]
                src = (first_part if axis == FIRST else second_part)(r, half, dest, rng)
                dst = (xbuf if axis == FIRST else ybuf).at[r, half, idx]
                remote(src, dst, rs_send.at[r, axis], rs_recv.at[r, axis, sem], neighbour(axis, half, step)).start()

    def reduce_wait(r, axis, sem):
        buf = xbuf if axis == FIRST else ybuf
        wait_bytes(buf.at[r, :, pl.ds(0, 4)] if sem == 2 else buf.at[r, 0, pl.ds(0, 2)], rs_recv.at[r, axis, sem])

    def lse_buf(axis):
        return lse_x if axis == 0 else lse_y

    def lse_send(j, axis):
        buf = lse_buf(axis)
        for idx, step in enumerate((1, -1, 2)):
            remote(buf.at[j, 0], buf.at[j, idx + 1], ls_send.at[j, axis], ls_recv.at[j, axis], neighbour(axis, 0, step)).start()

    def lse_wait(j, axis):
        wait_bytes(lse_buf(axis).at[j, pl.ds(0, 3)], ls_recv.at[j, axis])

    def swap_piece(j, n):
        ts = pl.ds(n * (nt // SLICES), nt // SLICES)
        remote(cache_ref.at[ts, 1 - core, j], sib_ref.at[j, ts], swap_send.at[j], swap_recv.at[j], sibling).start()

    def query_swap():
        return remote(q_ref.at[:, 1 - core], q_sib, qs_send, qs_recv, sibling)

    def load_pages(n):
        slot, j, t = lax.rem(n, DEPTH), n // nt, lax.rem(n, nt)
        for p, src in ((0, cache_ref.at[t, core, j]), (1, sib_ref.at[j, t])):
            pltpu.make_async_copy(src, page.at[slot, p, pl.ds(0, width)], page_sem.at[slot, p]).start()
            pltpu.make_async_copy(src.at[pl.ds(latent, ROPE_DIM)], page.at[slot, p, pl.ds(width, ROPE_DIM)],
                                  page_sem.at[slot, p]).start()

    def merge_queries(j):
        for t in range(nt):
            mine = q_ref[t, core, j].astype(jnp.float32)
            other = q_sib[t, j].astype(jnp.float32)
            both = jnp.concatenate([jnp.where(core == 0, mine, other), jnp.where(core == 0, other, mine)], axis=0)
            base, sub = (t // 4) * quarter_q, t % 4
            for i in range(columns):
                q_all[j, ypos, xpos, base + sub * columns + i] = both[:, i * 128:(i + 1) * 128].astype(jnp.bfloat16)
            rope = both[:, latent:]
            if sub < 2:
                low = (low if sub else []) + [rope]
            else:
                q_all[j, ypos, xpos, base + 4 * columns + sub - 2] = jnp.concatenate([low[sub - 2], rope], axis=1).astype(
                    jnp.bfloat16)

    def gather_first(j):
        for sem, sends in ((0, (2, 5, 9)), (1, (3, 6, 10))):
            gather_wait(j, sem)
            gather_send(j, *sends)

    def gather_turn(j):
        gather_wait(j, 2)
        gather_send(j, 7, 11)

    def gather_second(j, sem, send):
        gather_wait(j, sem)
        gather_send(j, send)

    def gather_end(j):
        gather_wait(j, 7)

    def swap_wait(j):
        wait_bytes(sib_ref.at[j], swap_recv.at[j])

    def attend(n):
        @pl.when(n + DEPTH - 1 < nj * nt)
        def _():
            load_pages(n + DEPTH - 1)

        slot, j, t = lax.rem(n, DEPTH), n // nt, lax.rem(n, nt)
        for p in (0, 1):
            wait_bytes(page.at[slot, p], page_sem.at[slot, p])
        base, sub = (t // 4) * quarter_q, lax.rem(t, 4)
        cols = [q_all[j, :, :, base + sub * columns + i].reshape(heads, 128) for i in range(columns)]
        rope = q_all[j, :, :, base + 4 * columns + lax.rem(sub, 2)].reshape(heads, 128)
        lane_half = lax.broadcasted_iota(jnp.int32, (heads, 128), 1) // ROPE_DIM
        cols.append(jnp.where(lane_half == sub // 2, rope, jnp.zeros_like(rope)))
        q = jnp.concatenate(cols, axis=1)
        limit = len_ref[(t * 2 + core) * nj + j]
        outs, lses = [], []
        for p in (0, 1):
            owner = me if p == 0 else sibling
            s = jnp.dot(q, page[slot, p], preferred_element_type=jnp.float32) * (QK_DIM ** -0.5)
            position = owner * page_len + lax.broadcasted_iota(jnp.int32, (1, page_len), 1)
            s = jnp.where(position < limit, s, -1e30)
            m = jnp.max(s, axis=1, keepdims=True)
            w = jnp.exp(s - m)
            l = jnp.sum(w, axis=1, keepdims=True)
            pv = lax.dot_general(w.astype(jnp.bfloat16), page[slot, p, :latent], (((1,), (1,)), ((), ())),
                                 preferred_element_type=jnp.float32)
            outs.append((pv * (1.0 / l)).astype(jnp.bfloat16).astype(jnp.float32))
            lses.append(m + jnp.log(l))
        top = jnp.maximum(lses[0], lses[1])
        both = top + jnp.log(jnp.exp(lses[0] - top) + jnp.exp(lses[1] - top))
        part[j, t // side, lax.rem(t, side)] = jnp.exp(lses[0] - both) * outs[0] + jnp.exp(lses[1] - both) * outs[1]
        row = jnp.broadcast_to(both, (heads, 128)).T
        lse_x[j, 0, pl.ds(t, 1), :] = row[0:1]

    def combine(v):
        top = jnp.max(v, axis=0)
        return top + jnp.log(jnp.sum(jnp.exp(v - top[None]), axis=0))

    def lse_turn(j):
        lse_wait(j, 0)
        lse_y[j, 0] = combine(lse_x[j])
        lse_send(j, 1)

    def weigh(j):
        lse_wait(j, 1)
        wgt[...] = jnp.exp(lse_x[j, 0] - combine(lse_y[j]))

        def body(t, _):
            w = jnp.broadcast_to(wgt[pl.ds(t, 1), :], (128, heads)).T
            yy, xx = t // side, lax.rem(t, side)
            for i in range(latent // 128):
                cols = pl.ds(i * 128, 128)
                part[j, yy, xx, :, cols] = part[j, yy, xx, :, cols] * w
            return 0

        lax.fori_loop(0, nt, body, 0)

    def reduce_turn(r, axis):
        for idx, dest, rng, nxt, sem in ((0, 1, LOW, 4, 0), (2, -1, HIGH, 5, 1)):
            reduce_wait(r, axis, sem)
            for half in (0, 1):
                if axis == FIRST:
                    def body(i, _):
                        ref = first_part(r, half, dest, rng, i)
                        ref[...] = ref[...] + xbuf[r, half, idx, i]
                        return 0
                    lax.fori_loop(0, side, body, 0)
                else:
                    ref = second_part(r, half, dest, rng)
                    ref[...] = ref[...] + ybuf[r, half, idx]
            reduce_send(r, axis, nxt)

    def reduce_end(r, axis):
        reduce_wait(r, axis, 2)
        for half in (0, 1):
            for rng, one, two in ((HIGH, 1, 5), (LOW, 3, 4)):
                if axis == FIRST:
                    def body(i, _):
                        ref = first_part(r, half, 0, rng, i)
                        ref[...] = ref[...] + (xbuf[r, half, one, i] + xbuf[r, half, two, i])
                        return 0
                    lax.fori_loop(0, side, body, 0)
                else:
                    total = second_part(r, half, 0, rng)[...] + (ybuf[r, half, one] + ybuf[r, half, two])
                    out_ref[r, pl.ds(rows_of(half, rng), quarter_h)] = total.astype(out_ref.dtype)

    PIECES = ((2,), (1, -1), (0,))

    def row_of(half, step):
        return wrap(ypos if half == 0 else xpos, step)

    def last_turn(r):
        for sem in (0, 1):
            reduce_wait(r, FIRST, sem)
        for n, piece in enumerate(PIECES):
            for step in piece:
                for lane, (idx, dest, rng, nxt) in enumerate(((0, 1, LOW, 4), (2, -1, HIGH, 5))):
                    for half in (0, 1):
                        i = row_of(half, step)
                        ref = first_part(r, half, dest, rng, i)
                        ref[...] = ref[...] + xbuf[r, half, idx, i]
                        remote(ref, xbuf.at[r, half, nxt, i], rs_send.at[r, FIRST], last_recv.at[lane, n],
                               neighbour(FIRST, half, REDUCE[nxt][2])).start()

    def last_piece(r, n):
        if n == 0:
            wait_bytes(xbuf.at[r, 0, pl.ds(0, 4)], rs_recv.at[r, FIRST, 2])
        for lane in (0, 1):
            wait_bytes(xbuf.at[r, 0, 0, pl.ds(0, 2 * len(PIECES[n]))], last_recv.at[lane, n])
        for half in (0, 1):
            for step in PIECES[n]:
                i = row_of(half, step)
                for rng, one, two in ((HIGH, 1, 5), (LOW, 3, 4)):
                    ref = first_part(r, half, 0, rng, i)
                    ref[...] = ref[...] + (xbuf[r, half, one, i] + xbuf[r, half, two, i])
        if n < 2:
            reduce_send(r, SECOND, *((0, 2), (1, 3))[n])

    barrier = pltpu.get_barrier_semaphore()
    peers = [sibling] + [neighbour(axis, 0, step) for axis in (0, 1) for step in (1, -1, 2)]
    for dev in peers:
        pl.semaphore_signal(barrier, inc=1, device_id=peer(dev), device_id_type=pl.DeviceIdType.MESH)
    with jax.named_scope('barrier'):
        pl.semaphore_wait(barrier, len(peers))

    query_swap().start()
    with jax.named_scope('merge0'):
        query_swap().wait_recv()
        merge_queries(0)
    gather_send(0, 0, 1, 4, 8)
    swap_piece(0, 0)
    swap_piece(0, 1)
    with jax.named_scope('merges'):
        lax.fori_loop(1, nj, lambda j, _: (merge_queries(j), 0)[1], 0)
    with jax.named_scope('chunk0'):
        gather_first(0)
        swap_piece(0, 2)
        gather_second(0, 3, 12)
        gather_turn(0)
        gather_send(1, 0, 1)
        swap_piece(0, 3)
        gather_second(0, 4, 13)
        gather_second(0, 5, 14)
        gather_second(0, 6, 15)
    with jax.named_scope('chunk1'):
        swap_piece(1, 0)
        gather_first(1)
        gather_send(1, 4, 8)
        gather_send(2, 0, 1)
        swap_piece(1, 1)
        swap_wait(0)
        for n in range(DEPTH - 1):
            load_pages(n)
        gather_end(0)

    def run(*steps):
        for fn, *args in steps:
            with jax.named_scope(fn.__name__ + '_' + '_'.join(str(a) for a in args)):
                fn(*args)

    def middle(j):
        run((gather_turn, j), (gather_second, j, 4, 13), (gather_second, j, 5, 14), (gather_second, j, 3, 12))

    slots = {
        0: ((swap_piece, 1, 2),),
        1: ((gather_send, 2, 4, 8), (gather_send, 3, 0, 1), (swap_piece, 1, 3)),
        2: ((gather_turn, 1), (gather_second, 1, 4, 13), (gather_second, 1, 5, 14), (swap_piece, 2, 0)),
        3: ((gather_second, 1, 3, 12), (gather_first, 2), (swap_wait, 1), (swap_piece, 2, 1)),
        4: ((lse_send, 0, 0), (gather_second, 1, 6, 15), (gather_second, 2, 3, 12), (gather_send, 3, 4, 8), (lse_turn, 0),
            (gather_turn, 2), (gather_end, 1), (gather_second, 2, 4, 13), (gather_second, 2, 5, 14), (gather_first, 3),
            (swap_piece, 2, 2)),
        5: ((gather_second, 2, 6, 15), (swap_piece, 2, 3)),
        6: ((gather_turn, 3), (gather_second, 3, 3, 12), (weigh, 0), (reduce_send, 0, FIRST, 0, 2), (swap_piece, 3, 0)),
        7: ((gather_second, 3, 4, 13), (gather_second, 3, 5, 14), (swap_wait, 2), (swap_piece, 3, 1)),
        8: ((lse_send, 1, 0), (gather_second, 3, 6, 15), (gather_end, 2), (swap_piece, 3, 2)),
        9: ((reduce_send, 0, FIRST, 1, 3), (swap_piece, 3, 3)),
        11: ((lse_turn, 1), (reduce_turn, 0, FIRST), (swap_wait, 3)),
        12: ((lse_send, 2, 0), (gather_end, 3)),
        13: ((weigh, 1), (reduce_send, 1, FIRST, 0, 2)),
        14: ((lse_turn, 2),),
        15: ((reduce_send, 1, FIRST, 1, 3),),
    }

    def slot_body(n, _):
        for at, steps in slots.items():
            pl.when(n == at)(functools.partial(run, *steps))
        with jax.named_scope('attend'):
            lax.fori_loop(n * (nt // SLICES), (n + 1) * (nt // SLICES), lambda i, _: (attend(i), 0)[1], 0)
        return 0

    lax.fori_loop(0, nj * SLICES, slot_body, 0)

    early = (0, 2, 1, 3)
    run((lse_send, 3, 0), (reduce_end, 0, FIRST), (reduce_send, 0, SECOND, *early))
    run((reduce_turn, 1, FIRST), (reduce_turn, 0, SECOND), (lse_turn, 3), (weigh, 2), (reduce_send, 2, FIRST, *early),
        (reduce_end, 1, FIRST), (reduce_send, 1, SECOND, *early), (reduce_end, 0, SECOND))
    run((reduce_turn, 2, FIRST), (reduce_turn, 1, SECOND), (weigh, 3), (reduce_send, 3, FIRST, *early),
        (reduce_end, 2, FIRST), (reduce_send, 2, SECOND, *early), (reduce_end, 1, SECOND))
    run((last_turn, 3), (reduce_turn, 2, SECOND), (last_piece, 3, 0), (last_piece, 3, 1), (last_piece, 3, 2))
    run((reduce_turn, 3, SECOND), (reduce_end, 2, SECOND), (reduce_end, 3, SECOND))

    def drain(j, _):
        wait_bytes(sib_ref.at[j], swap_send.at[j])
        wait_bytes(q_all.at[j, :, :, pl.ds(0, 14 * tiles // 16)], ag_send.at[j, 0])
        wait_bytes(q_all.at[j, 0, 0], ag_send.at[j, 1])
        wait_bytes(xbuf.at[j], rs_send.at[j, 0])
        wait_bytes(ybuf.at[j], rs_send.at[j, 1])
        for axis in (0, 1):
            wait_bytes(lse_buf(axis).at[j, pl.ds(0, 3)], ls_send.at[j, axis])
        return 0

    with jax.named_scope('drain'):
        query_swap().wait_send()
        lax.fori_loop(0, nj, drain, 0)


def solution(mesh):
    group_size = mesh.shape[AXIS]
    side = math.isqrt(group_size // 2)
    nt = side * side

    def local_step(q_blk, cache_blk, len_blk):
        batch_rows, own_heads, width = q_blk.shape
        page_len = cache_blk.shape[3]
        latent = width - ROPE_DIM
        nj = batch_rows // group_size
        heads = 2 * own_heads * nt
        tiles = nt * (latent // 128) + nt // 2
        q = q_blk.reshape(nt, 2, nj, own_heads, width)
        cache = jnp.swapaxes(cache_blk.reshape(nt, 2, nj, page_len, width), 3, 4)
        any_space = pl.BlockSpec(memory_space=pl.ANY)
        dma = pltpu.SemaphoreType.DMA
        out, _ = pl.pallas_call(
            functools.partial(_kernel, side),
            out_shape=(jax.ShapeDtypeStruct((nj, heads, latent), jnp.bfloat16),
                       jax.ShapeDtypeStruct((nj, nt, width, page_len), jnp.bfloat16)),
            in_specs=[pl.BlockSpec(memory_space=pltpu.SMEM), pl.BlockSpec(memory_space=pltpu.VMEM), any_space],
            out_specs=(pl.BlockSpec(memory_space=pltpu.VMEM), any_space),
            scratch_shapes=[
                pltpu.VMEM((nt, nj, own_heads, width), jnp.bfloat16),
                pltpu.VMEM((nj, side, side, tiles, 2 * own_heads, 128), jnp.bfloat16),
                pltpu.VMEM((nj, side, side, heads, latent), jnp.float32),
                pltpu.VMEM((DEPTH, 2, width + ROPE_DIM, page_len), jnp.bfloat16),
                pltpu.VMEM((nj, 2, len(REDUCE), side, heads // 4, latent), jnp.float32),
                pltpu.VMEM((nj, 2, len(REDUCE), heads // 4, latent), jnp.float32),
                pltpu.VMEM((nj, 4, nt, heads), jnp.float32),
                pltpu.VMEM((nj, 4, nt, heads), jnp.float32),
                pltpu.VMEM((nt, heads), jnp.float32),
                dma((DEPTH, 2)), dma((nj,)), dma((nj,)), dma(()), dma(()),
                dma((nj, 2)), dma((nj, 8)), dma((nj, 2)), dma((nj, 2, 3)), dma((2, 3)), dma((nj, 2)), dma((nj, 2)),
            ],
            compiler_params=pltpu.CompilerParams(collective_id=0, has_side_effects=True, vmem_limit_bytes=54_000_000),
        )(len_blk, q, cache)
        return out

    return jax.shard_map(local_step, mesh=mesh, in_specs=(P('dp', AXIS, None), P('dp', None, AXIS, None, None), P('dp')),
                         out_specs=P(('dp', AXIS), None, None), check_vma=False)
```

```python
import functools
import math

import jax
import jax.numpy as jnp
from jax import lax
from jax.experimental import pallas as pl
from jax.experimental.pallas import tpu as pltpu
from jax.sharding import PartitionSpec as P

ROPE_DIM = 64
QK_DIM = 192
AXIS = 'dcp'
DEPTH = 3
SLICES = 4

FIRST, SECOND = 0, 1
FULL, LOW, HIGH = 0, 1, 2
GATHER = (
    (FIRST, 1, (0, 0), FULL, 0),
    (FIRST, -1, (0, 0), FULL, 1),
    (FIRST, 1, (-1, 0), LOW, 2),
    (FIRST, -1, (1, 0), HIGH, 2),
    (SECOND, 1, (0, 0), FULL, 3),
    (SECOND, 1, (-1, 0), FULL, 4),
    (SECOND, 1, (1, 0), FULL, 7),
    (SECOND, 1, (2, 0), FULL, 7),
    (SECOND, -1, (0, 0), FULL, 7),
    (SECOND, -1, (-1, 0), FULL, 7),
    (SECOND, -1, (1, 0), FULL, 5),
    (SECOND, -1, (2, 0), FULL, 6),
    (SECOND, 1, (0, -1), FULL, 7),
    (SECOND, 1, (-1, -1), FULL, 7),
    (SECOND, -1, (1, 1), FULL, 7),
    (SECOND, -1, (2, 1), FULL, 7),
)
REDUCE = ((2, LOW, 1, 0), (1, HIGH, 1, 2), (2, HIGH, -1, 1), (-1, LOW, -1, 2), (1, LOW, 1, 2), (-1, HIGH, -1, 2))


def _kernel(side, len_ref, q_ref, cache_ref, out_ref, sib_ref, q_sib, q_all, part, page, xbuf, ybuf, lse_x, lse_y,
            wgt, page_sem, swap_send, swap_recv, qs_send, qs_recv, ag_send, ag_recv, rs_send, rs_recv, last_recv, ls_send,
            ls_recv):
    nt, nj, own_heads, width = q_sib.shape
    heads, latent = part.shape[3:]
    page_len = page.shape[3]
    half_h, quarter_h = heads // 2, heads // 4
    tiles = q_all.shape[3]
    quarter_q, half_q = tiles // 4, tiles // 2
    columns = latent // 128

    me = lax.axis_index(AXIS)
    core = lax.rem(me, 2)
    xpos = lax.rem(me // 2, side)
    ypos = me // (2 * side)
    sibling = me + 1 - 2 * core

    def wrap(pos, step):
        return lax.rem(pos + (step + side), side)

    def neighbour(axis, half, step):
        if axis == half:
            return (ypos * side + wrap(xpos, step)) * 2 + core
        return (wrap(ypos, step) * side + xpos) * 2 + core

    def peer(dev):
        return {AXIS: dev}

    def remote(ref, dst, send_sem, recv_sem, dev):
        return pltpu.make_async_remote_copy(src_ref=ref, dst_ref=dst, send_sem=send_sem, recv_sem=recv_sem,
                                            device_id=peer(dev), device_id_type=pl.DeviceIdType.MESH)

    def gather_block(j, half, first, second, rng):
        if half == 0:
            yy, xx = wrap(ypos, second), wrap(xpos, first)
        else:
            yy, xx = wrap(ypos, first), wrap(xpos, second)
        start = half * half_q + (quarter_q if rng == HIGH else 0)
        return q_all.at[j, yy, xx, pl.ds(start, half_q if rng == FULL else quarter_q)]

    def gather_send(j, *indices):
        for idx in indices:
            for half in (0, 1):
                axis, step, (first, second), rng, sem = GATHER[idx]
                ref = gather_block(j, half, first, second, rng)
                remote(ref, ref, ag_send.at[j, 0 if rng == FULL else 1], ag_recv.at[j, sem],
                       neighbour(axis, half, step)).start()

    def wait_bytes(ref, sem):
        pltpu.make_async_copy(ref, ref, sem).wait()

    def gather_wait(j, sem):
        wait_bytes(q_all.at[j, pl.ds(0, side // 2)] if sem == 7 else q_all.at[j, 0, 0], ag_recv.at[j, sem])

    def rows_of(half, rng):
        return half * half_h + (quarter_h if rng == HIGH else 0)

    def first_part(r, half, step, rng, i=None):
        hs = pl.ds(rows_of(half, rng), quarter_h)
        second = slice(None) if i is None else i
        if half == 0:
            return part.at[r, second, wrap(xpos, step), hs]
        return part.at[r, wrap(ypos, step), second, hs]

    def second_part(r, half, step, rng):
        hs = pl.ds(rows_of(half, rng), quarter_h)
        if half == 0:
            return part.at[r, wrap(ypos, step), xpos, hs]
        return part.at[r, ypos, wrap(xpos, step), hs]

    def reduce_send(r, axis, *indices):
        for idx in indices:
            for half in (0, 1):
                dest, rng, step, sem = REDUCE[idx]
                src = (first_part if axis == FIRST else second_part)(r, half, dest, rng)
                dst = (xbuf if axis == FIRST else ybuf).at[r, half, idx]
                remote(src, dst, rs_send.at[r, axis], rs_recv.at[r, axis, sem], neighbour(axis, half, step)).start()

    def reduce_wait(r, axis, sem):
        buf = xbuf if axis == FIRST else ybuf
        wait_bytes(buf.at[r, :, pl.ds(0, 4)] if sem == 2 else buf.at[r, 0, pl.ds(0, 2)], rs_recv.at[r, axis, sem])

    def lse_buf(axis):
        return lse_x if axis == 0 else lse_y

    def lse_send(j, axis):
        buf = lse_buf(axis)
        for idx, step in enumerate((1, -1, 2)):
            remote(buf.at[j, 0], buf.at[j, idx + 1], ls_send.at[j, axis], ls_recv.at[j, axis], neighbour(axis, 0, step)).start()

    def lse_wait(j, axis):
        wait_bytes(lse_buf(axis).at[j, pl.ds(0, 3)], ls_recv.at[j, axis])

    def swap_piece(j, n):
        ts = pl.ds(n * (nt // SLICES), nt // SLICES)
        remote(cache_ref.at[ts, 1 - core, j], sib_ref.at[j, ts], swap_send.at[j], swap_recv.at[j], sibling).start()

    def query_swap():
        return remote(q_ref.at[:, 1 - core], q_sib, qs_send, qs_recv, sibling)

    def load_pages(n):
        slot, j, t = lax.rem(n, DEPTH), n // nt, lax.rem(n, nt)
        for p, src in ((0, cache_ref.at[t, core, j]), (1, sib_ref.at[j, t])):
            pltpu.make_async_copy(src, page.at[slot, p, pl.ds(0, width)], page_sem.at[slot, p]).start()
            pltpu.make_async_copy(src.at[pl.ds(latent, ROPE_DIM)], page.at[slot, p, pl.ds(width, ROPE_DIM)],
                                  page_sem.at[slot, p]).start()

    def merge_queries(j):
        for t in range(nt):
            mine = q_ref[t, core, j].astype(jnp.float32)
            other = q_sib[t, j].astype(jnp.float32)
            both = jnp.concatenate([jnp.where(core == 0, mine, other), jnp.where(core == 0, other, mine)], axis=0)
            base, sub = (t // 4) * quarter_q, t % 4
            for i in range(columns):
                q_all[j, ypos, xpos, base + sub * columns + i] = both[:, i * 128:(i + 1) * 128].astype(jnp.bfloat16)
            rope = both[:, latent:]
            if sub < 2:
                low = (low if sub else []) + [rope]
            else:
                q_all[j, ypos, xpos, base + 4 * columns + sub - 2] = jnp.concatenate([low[sub - 2], rope], axis=1).astype(
                    jnp.bfloat16)

    def gather_first(j):
        for sem, sends in ((0, (2, 5, 9)), (1, (3, 6, 10))):
            gather_wait(j, sem)
            gather_send(j, *sends)

    def gather_turn(j):
        gather_wait(j, 2)
        gather_send(j, 7, 11)

    def gather_second(j, sem, send):
        gather_wait(j, sem)
        gather_send(j, send)

    def gather_end(j):
        gather_wait(j, 7)

    def swap_wait(j):
        wait_bytes(sib_ref.at[j], swap_recv.at[j])

    def attend(n):
        @pl.when(n + DEPTH - 1 < nj * nt)
        def _():
            load_pages(n + DEPTH - 1)

        slot, j, t = lax.rem(n, DEPTH), n // nt, lax.rem(n, nt)
        for p in (0, 1):
            wait_bytes(page.at[slot, p], page_sem.at[slot, p])
        base, sub = (t // 4) * quarter_q, lax.rem(t, 4)
        cols = [q_all[j, :, :, base + sub * columns + i].reshape(heads, 128) for i in range(columns)]
        rope = q_all[j, :, :, base + 4 * columns + lax.rem(sub, 2)].reshape(heads, 128)
        lane_half = lax.broadcasted_iota(jnp.int32, (heads, 128), 1) // ROPE_DIM
        cols.append(jnp.where(lane_half == sub // 2, rope, jnp.zeros_like(rope)))
        q = jnp.concatenate(cols, axis=1)
        limit = len_ref[(t * 2 + core) * nj + j]
        outs, lses = [], []
        for p in (0, 1):
            owner = me if p == 0 else sibling
            s = jnp.dot(q, page[slot, p], preferred_element_type=jnp.float32) * (QK_DIM ** -0.5)
            position = owner * page_len + lax.broadcasted_iota(jnp.int32, (1, page_len), 1)
            s = jnp.where(position < limit, s, -1e30)
            m = jnp.max(s, axis=1, keepdims=True)
            w = jnp.exp(s - m)
            l = jnp.sum(w, axis=1, keepdims=True)
            pv = lax.dot_general(w.astype(jnp.bfloat16), page[slot, p, :latent], (((1,), (1,)), ((), ())),
                                 preferred_element_type=jnp.float32)
            outs.append((pv * (1.0 / l)).astype(jnp.bfloat16).astype(jnp.float32))
            lses.append(m + jnp.log(l))
        top = jnp.maximum(lses[0], lses[1])
        both = top + jnp.log(jnp.exp(lses[0] - top) + jnp.exp(lses[1] - top))
        part[j, t // side, lax.rem(t, side)] = jnp.exp(lses[0] - both) * outs[0] + jnp.exp(lses[1] - both) * outs[1]
        row = jnp.broadcast_to(both, (heads, 128)).T
        lse_x[j, 0, pl.ds(t, 1), :] = row[0:1]

    def combine(v):
        top = jnp.max(v, axis=0)
        return top + jnp.log(jnp.sum(jnp.exp(v - top[None]), axis=0))

    def lse_turn(j):
        lse_wait(j, 0)
        lse_y[j, 0] = combine(lse_x[j])
        lse_send(j, 1)

    def weigh(j):
        lse_wait(j, 1)
        wgt[...] = jnp.exp(lse_x[j, 0] - combine(lse_y[j]))

        def body(t, _):
            w = jnp.broadcast_to(wgt[pl.ds(t, 1), :], (128, heads)).T
            yy, xx = t // side, lax.rem(t, side)
            for i in range(latent // 128):
                cols = pl.ds(i * 128, 128)
                part[j, yy, xx, :, cols] = part[j, yy, xx, :, cols] * w
            return 0

        lax.fori_loop(0, nt, body, 0)

    def reduce_turn(r, axis):
        for idx, dest, rng, nxt, sem in ((0, 1, LOW, 4, 0), (2, -1, HIGH, 5, 1)):
            reduce_wait(r, axis, sem)
            for half in (0, 1):
                if axis == FIRST:
                    def body(i, _):
                        ref = first_part(r, half, dest, rng, i)
                        ref[...] = ref[...] + xbuf[r, half, idx, i]
                        return 0
                    lax.fori_loop(0, side, body, 0)
                else:
                    ref = second_part(r, half, dest, rng)
                    ref[...] = ref[...] + ybuf[r, half, idx]
            reduce_send(r, axis, nxt)

    def reduce_end(r, axis):
        reduce_wait(r, axis, 2)
        for half in (0, 1):
            for rng, one, two in ((HIGH, 1, 5), (LOW, 3, 4)):
                if axis == FIRST:
                    def body(i, _):
                        ref = first_part(r, half, 0, rng, i)
                        ref[...] = ref[...] + (xbuf[r, half, one, i] + xbuf[r, half, two, i])
                        return 0
                    lax.fori_loop(0, side, body, 0)
                else:
                    total = second_part(r, half, 0, rng)[...] + (ybuf[r, half, one] + ybuf[r, half, two])
                    out_ref[r, pl.ds(rows_of(half, rng), quarter_h)] = total.astype(out_ref.dtype)

    PIECES = ((2,), (1, -1), (0,))

    def row_of(half, step):
        return wrap(ypos if half == 0 else xpos, step)

    def last_turn(r):
        for sem in (0, 1):
            reduce_wait(r, FIRST, sem)
        for n, piece in enumerate(PIECES):
            for step in piece:
                for lane, (idx, dest, rng, nxt) in enumerate(((0, 1, LOW, 4), (2, -1, HIGH, 5))):
                    for half in (0, 1):
                        i = row_of(half, step)
                        ref = first_part(r, half, dest, rng, i)
                        ref[...] = ref[...] + xbuf[r, half, idx, i]
                        remote(ref, xbuf.at[r, half, nxt, i], rs_send.at[r, FIRST], last_recv.at[lane, n],
                               neighbour(FIRST, half, REDUCE[nxt][2])).start()

    def last_piece(r, n):
        if n == 0:
            wait_bytes(xbuf.at[r, 0, pl.ds(0, 4)], rs_recv.at[r, FIRST, 2])
        for lane in (0, 1):
            wait_bytes(xbuf.at[r, 0, 0, pl.ds(0, 2 * len(PIECES[n]))], last_recv.at[lane, n])
        for half in (0, 1):
            for step in PIECES[n]:
                i = row_of(half, step)
                for rng, one, two in ((HIGH, 1, 5), (LOW, 3, 4)):
                    ref = first_part(r, half, 0, rng, i)
                    ref[...] = ref[...] + (xbuf[r, half, one, i] + xbuf[r, half, two, i])
        if n < 2:
            reduce_send(r, SECOND, *((0, 2), (1, 3))[n])

    barrier = pltpu.get_barrier_semaphore()
    peers = [sibling] + [neighbour(axis, 0, step) for axis in (0, 1) for step in (1, -1, 2)]
    for dev in peers:
        pl.semaphore_signal(barrier, inc=1, device_id=peer(dev), device_id_type=pl.DeviceIdType.MESH)
    with jax.named_scope('barrier'):
        pl.semaphore_wait(barrier, len(peers))

    query_swap().start()
    with jax.named_scope('merge0'):
        query_swap().wait_recv()
        merge_queries(0)
    gather_send(0, 0, 1, 4, 8)
    swap_piece(0, 0)
    swap_piece(0, 1)
    with jax.named_scope('merges'):
        lax.fori_loop(1, nj, lambda j, _: (merge_queries(j), 0)[1], 0)
    with jax.named_scope('chunk0'):
        gather_first(0)
        swap_piece(0, 2)
        gather_second(0, 3, 12)
        gather_turn(0)
        gather_send(1, 0, 1)
        swap_piece(0, 3)
        gather_second(0, 4, 13)
        gather_second(0, 5, 14)
        gather_second(0, 6, 15)
    with jax.named_scope('chunk1'):
        swap_piece(1, 0)
        gather_first(1)
        gather_send(1, 4, 8)
        gather_send(2, 0, 1)
        swap_piece(1, 1)
        swap_wait(0)
        for n in range(DEPTH - 1):
            load_pages(n)
        gather_end(0)

    def run(*steps):
        for fn, *args in steps:
            with jax.named_scope(fn.__name__ + '_' + '_'.join(str(a) for a in args)):
                fn(*args)

    def middle(j):
        run((gather_turn, j), (gather_second, j, 4, 13), (gather_second, j, 5, 14), (gather_second, j, 3, 12))

    slots = {
        0: ((swap_piece, 1, 2),),
        1: ((gather_send, 2, 4, 8), (gather_send, 3, 0, 1), (swap_piece, 1, 3)),
        2: ((gather_turn, 1), (gather_second, 1, 4, 13), (gather_second, 1, 5, 14), (swap_piece, 2, 0)),
        3: ((gather_second, 1, 3, 12), (gather_first, 2), (swap_wait, 1), (swap_piece, 2, 1)),
        4: ((lse_send, 0, 0), (gather_second, 1, 6, 15), (gather_second, 2, 3, 12), (gather_send, 3, 4, 8), (lse_turn, 0),
            (gather_turn, 2), (gather_end, 1), (gather_second, 2, 4, 13), (gather_second, 2, 5, 14), (gather_first, 3),
            (swap_piece, 2, 2)),
        5: ((gather_second, 2, 6, 15), (swap_piece, 2, 3)),
        6: ((gather_turn, 3), (gather_second, 3, 3, 12), (weigh, 0), (reduce_send, 0, FIRST, 0, 2), (swap_piece, 3, 0)),
        7: ((gather_second, 3, 4, 13), (gather_second, 3, 5, 14), (swap_wait, 2), (swap_piece, 3, 1)),
        8: ((lse_send, 1, 0), (gather_second, 3, 6, 15), (gather_end, 2), (swap_piece, 3, 2)),
        9: ((reduce_send, 0, FIRST, 1, 3), (swap_piece, 3, 3)),
        11: ((lse_turn, 1), (reduce_turn, 0, FIRST), (swap_wait, 3)),
        12: ((lse_send, 2, 0), (gather_end, 3)),
        13: ((weigh, 1), (reduce_send, 1, FIRST, 0, 2)),
        14: ((lse_turn, 2),),
        15: ((reduce_send, 1, FIRST, 1, 3),),
    }

    def slot_body(n, _):
        for at, steps in slots.items():
            pl.when(n == at)(functools.partial(run, *steps))
        with jax.named_scope('attend'):
            lax.fori_loop(n * (nt // SLICES), (n + 1) * (nt // SLICES), lambda i, _: (attend(i), 0)[1], 0)
        return 0

    lax.fori_loop(0, nj * SLICES, slot_body, 0)

    early = (0, 2, 1, 3)
    run((lse_send, 3, 0), (reduce_end, 0, FIRST), (reduce_send, 0, SECOND, *early))
    run((reduce_turn, 1, FIRST), (reduce_turn, 0, SECOND), (lse_turn, 3), (weigh, 2), (reduce_send, 2, FIRST, *early),
        (reduce_end, 1, FIRST), (reduce_send, 1, SECOND, *early), (reduce_end, 0, SECOND))
    run((reduce_turn, 2, FIRST), (reduce_turn, 1, SECOND), (weigh, 3), (reduce_send, 3, FIRST, *early),
        (reduce_end, 2, FIRST), (reduce_send, 2, SECOND, *early), (reduce_end, 1, SECOND))
    run((last_turn, 3), (last_piece, 3, 0), (reduce_turn, 2, SECOND), (last_piece, 3, 1), (last_piece, 3, 2))
    run((reduce_turn, 3, SECOND), (reduce_end, 2, SECOND), (reduce_end, 3, SECOND))

    def drain(j, _):
        wait_bytes(sib_ref.at[j], swap_send.at[j])
        wait_bytes(q_all.at[j, :, :, pl.ds(0, 14 * tiles // 16)], ag_send.at[j, 0])
        wait_bytes(q_all.at[j, 0, 0], ag_send.at[j, 1])
        wait_bytes(xbuf.at[j], rs_send.at[j, 0])
        wait_bytes(ybuf.at[j], rs_send.at[j, 1])
        for axis in (0, 1):
            wait_bytes(lse_buf(axis).at[j, pl.ds(0, 3)], ls_send.at[j, axis])
        return 0

    with jax.named_scope('drain'):
        query_swap().wait_send()
        lax.fori_loop(0, nj, drain, 0)


def solution(mesh):
    group_size = mesh.shape[AXIS]
    side = math.isqrt(group_size // 2)
    nt = side * side

    def local_step(q_blk, cache_blk, len_blk):
        batch_rows, own_heads, width = q_blk.shape
        page_len = cache_blk.shape[3]
        latent = width - ROPE_DIM
        nj = batch_rows // group_size
        heads = 2 * own_heads * nt
        tiles = nt * (latent // 128) + nt // 2
        q = q_blk.reshape(nt, 2, nj, own_heads, width)
        cache = jnp.swapaxes(cache_blk.reshape(nt, 2, nj, page_len, width), 3, 4)
        any_space = pl.BlockSpec(memory_space=pl.ANY)
        dma = pltpu.SemaphoreType.DMA
        out, _ = pl.pallas_call(
            functools.partial(_kernel, side),
            out_shape=(jax.ShapeDtypeStruct((nj, heads, latent), jnp.bfloat16),
                       jax.ShapeDtypeStruct((nj, nt, width, page_len), jnp.bfloat16)),
            in_specs=[pl.BlockSpec(memory_space=pltpu.SMEM), pl.BlockSpec(memory_space=pltpu.VMEM), any_space],
            out_specs=(pl.BlockSpec(memory_space=pltpu.VMEM), any_space),
            scratch_shapes=[
                pltpu.VMEM((nt, nj, own_heads, width), jnp.bfloat16),
                pltpu.VMEM((nj, side, side, tiles, 2 * own_heads, 128), jnp.bfloat16),
                pltpu.VMEM((nj, side, side, heads, latent), jnp.float32),
                pltpu.VMEM((DEPTH, 2, width + ROPE_DIM, page_len), jnp.bfloat16),
                pltpu.VMEM((nj, 2, len(REDUCE), side, heads // 4, latent), jnp.float32),
                pltpu.VMEM((nj, 2, len(REDUCE), heads // 4, latent), jnp.float32),
                pltpu.VMEM((nj, 4, nt, heads), jnp.float32),
                pltpu.VMEM((nj, 4, nt, heads), jnp.float32),
                pltpu.VMEM((nt, heads), jnp.float32),
                dma((DEPTH, 2)), dma((nj,)), dma((nj,)), dma(()), dma(()),
                dma((nj, 2)), dma((nj, 8)), dma((nj, 2)), dma((nj, 2, 3)), dma((2, 3)), dma((nj, 2)), dma((nj, 2)),
            ],
            compiler_params=pltpu.CompilerParams(collective_id=0, has_side_effects=True, vmem_limit_bytes=54_000_000),
        )(len_blk, q, cache)
        return out

    return jax.shard_map(local_step, mesh=mesh, in_specs=(P('dp', AXIS, None), P('dp', None, AXIS, None, None), P('dp')),
                         out_specs=P(('dp', AXIS), None, None), check_vma=False)
```

```python
import functools
import math

import jax
import jax.numpy as jnp
from jax import lax
from jax.experimental import pallas as pl
from jax.experimental.pallas import tpu as pltpu
from jax.sharding import PartitionSpec as P

ROPE_DIM = 64
QK_DIM = 192
AXIS = 'dcp'
DEPTH = 3
SLICES = 4

FIRST, SECOND = 0, 1
FULL, LOW, HIGH = 0, 1, 2
GATHER = (
    (FIRST, 1, (0, 0), FULL, 0),
    (FIRST, -1, (0, 0), FULL, 1),
    (FIRST, 1, (-1, 0), LOW, 2),
    (FIRST, -1, (1, 0), HIGH, 2),
    (SECOND, 1, (0, 0), FULL, 3),
    (SECOND, 1, (-1, 0), FULL, 4),
    (SECOND, 1, (1, 0), FULL, 7),
    (SECOND, 1, (2, 0), FULL, 7),
    (SECOND, -1, (0, 0), FULL, 7),
    (SECOND, -1, (-1, 0), FULL, 7),
    (SECOND, -1, (1, 0), FULL, 5),
    (SECOND, -1, (2, 0), FULL, 6),
    (SECOND, 1, (0, -1), FULL, 7),
    (SECOND, 1, (-1, -1), FULL, 7),
    (SECOND, -1, (1, 1), FULL, 7),
    (SECOND, -1, (2, 1), FULL, 7),
)
REDUCE = ((2, LOW, 1, 0), (1, HIGH, 1, 2), (2, HIGH, -1, 1), (-1, LOW, -1, 2), (1, LOW, 1, 2), (-1, HIGH, -1, 2))


def _kernel(side, len_ref, q_ref, cache_ref, out_ref, sib_ref, q_sib, q_all, part, page, xbuf, ybuf, lse_x, lse_y,
            wgt, page_sem, swap_send, swap_recv, qs_send, qs_recv, ag_send, ag_recv, rs_send, rs_recv, last_recv, ls_send,
            ls_recv):
    nt, nj, own_heads, width = q_sib.shape
    heads, latent = part.shape[3:]
    page_len = page.shape[3]
    half_h, quarter_h = heads // 2, heads // 4
    tiles = q_all.shape[3]
    quarter_q, half_q = tiles // 4, tiles // 2
    columns = latent // 128

    me = lax.axis_index(AXIS)
    core = lax.rem(me, 2)
    xpos = lax.rem(me // 2, side)
    ypos = me // (2 * side)
    sibling = me + 1 - 2 * core

    def wrap(pos, step):
        return lax.rem(pos + (step + side), side)

    def neighbour(axis, half, step):
        if axis == half:
            return (ypos * side + wrap(xpos, step)) * 2 + core
        return (wrap(ypos, step) * side + xpos) * 2 + core

    def peer(dev):
        return {AXIS: dev}

    def remote(ref, dst, send_sem, recv_sem, dev):
        return pltpu.make_async_remote_copy(src_ref=ref, dst_ref=dst, send_sem=send_sem, recv_sem=recv_sem,
                                            device_id=peer(dev), device_id_type=pl.DeviceIdType.MESH)

    def gather_block(j, half, first, second, rng):
        if half == 0:
            yy, xx = wrap(ypos, second), wrap(xpos, first)
        else:
            yy, xx = wrap(ypos, first), wrap(xpos, second)
        start = half * half_q + (quarter_q if rng == HIGH else 0)
        return q_all.at[j, yy, xx, pl.ds(start, half_q if rng == FULL else quarter_q)]

    def gather_send(j, *indices):
        for idx in indices:
            for half in (0, 1):
                axis, step, (first, second), rng, sem = GATHER[idx]
                ref = gather_block(j, half, first, second, rng)
                remote(ref, ref, ag_send.at[j, 0 if rng == FULL else 1], ag_recv.at[j, sem],
                       neighbour(axis, half, step)).start()

    def wait_bytes(ref, sem):
        pltpu.make_async_copy(ref, ref, sem).wait()

    def gather_wait(j, sem):
        wait_bytes(q_all.at[j, pl.ds(0, side // 2)] if sem == 7 else q_all.at[j, 0, 0], ag_recv.at[j, sem])

    def rows_of(half, rng):
        return half * half_h + (quarter_h if rng == HIGH else 0)

    def first_part(r, half, step, rng, i=None):
        hs = pl.ds(rows_of(half, rng), quarter_h)
        second = slice(None) if i is None else i
        if half == 0:
            return part.at[r, second, wrap(xpos, step), hs]
        return part.at[r, wrap(ypos, step), second, hs]

    def second_part(r, half, step, rng):
        hs = pl.ds(rows_of(half, rng), quarter_h)
        if half == 0:
            return part.at[r, wrap(ypos, step), xpos, hs]
        return part.at[r, ypos, wrap(xpos, step), hs]

    def reduce_send(r, axis, *indices):
        for idx in indices:
            for half in (0, 1):
                dest, rng, step, sem = REDUCE[idx]
                src = (first_part if axis == FIRST else second_part)(r, half, dest, rng)
                dst = (xbuf if axis == FIRST else ybuf).at[r, half, idx]
                remote(src, dst, rs_send.at[r, axis], rs_recv.at[r, axis, sem], neighbour(axis, half, step)).start()

    def reduce_wait(r, axis, sem):
        buf = xbuf if axis == FIRST else ybuf
        wait_bytes(buf.at[r, :, pl.ds(0, 4)] if sem == 2 else buf.at[r, 0, pl.ds(0, 2)], rs_recv.at[r, axis, sem])

    def lse_buf(axis):
        return lse_x if axis == 0 else lse_y

    def lse_send(j, axis):
        buf = lse_buf(axis)
        for idx, step in enumerate((1, -1, 2)):
            remote(buf.at[j, 0], buf.at[j, idx + 1], ls_send.at[j, axis], ls_recv.at[j, axis], neighbour(axis, 0, step)).start()

    def lse_wait(j, axis):
        wait_bytes(lse_buf(axis).at[j, pl.ds(0, 3)], ls_recv.at[j, axis])

    def swap_piece(j, n):
        ts = pl.ds(n * (nt // SLICES), nt // SLICES)
        remote(cache_ref.at[ts, 1 - core, j], sib_ref.at[j, ts], swap_send.at[j], swap_recv.at[j], sibling).start()

    def query_swap():
        return remote(q_ref.at[:, 1 - core], q_sib, qs_send, qs_recv, sibling)

    def load_pages(n):
        slot, j, t = lax.rem(n, DEPTH), n // nt, lax.rem(n, nt)
        for p, src in ((0, cache_ref.at[t, core, j]), (1, sib_ref.at[j, t])):
            pltpu.make_async_copy(src, page.at[slot, p, pl.ds(0, width)], page_sem.at[slot, p]).start()
            pltpu.make_async_copy(src.at[pl.ds(latent, ROPE_DIM)], page.at[slot, p, pl.ds(width, ROPE_DIM)],
                                  page_sem.at[slot, p]).start()

    def merge_queries(j):
        for t in range(nt):
            mine = q_ref[t, core, j].astype(jnp.float32)
            other = q_sib[t, j].astype(jnp.float32)
            both = jnp.concatenate([jnp.where(core == 0, mine, other), jnp.where(core == 0, other, mine)], axis=0)
            base, sub = (t // 4) * quarter_q, t % 4
            for i in range(columns):
                q_all[j, ypos, xpos, base + sub * columns + i] = both[:, i * 128:(i + 1) * 128].astype(jnp.bfloat16)
            rope = both[:, latent:]
            if sub < 2:
                low = (low if sub else []) + [rope]
            else:
                q_all[j, ypos, xpos, base + 4 * columns + sub - 2] = jnp.concatenate([low[sub - 2], rope], axis=1).astype(
                    jnp.bfloat16)

    def gather_first(j):
        for sem, sends in ((0, (2, 5, 9)), (1, (3, 6, 10))):
            gather_wait(j, sem)
            gather_send(j, *sends)

    def gather_turn(j):
        gather_wait(j, 2)
        gather_send(j, 7, 11)

    def gather_second(j, sem, send):
        gather_wait(j, sem)
        gather_send(j, send)

    def gather_end(j):
        gather_wait(j, 7)

    def swap_wait(j):
        wait_bytes(sib_ref.at[j], swap_recv.at[j])

    def attend(n):
        @pl.when(n + DEPTH - 1 < nj * nt)
        def _():
            load_pages(n + DEPTH - 1)

        slot, j, t = lax.rem(n, DEPTH), n // nt, lax.rem(n, nt)
        for p in (0, 1):
            wait_bytes(page.at[slot, p], page_sem.at[slot, p])
        base, sub = (t // 4) * quarter_q, lax.rem(t, 4)
        cols = [q_all[j, :, :, base + sub * columns + i].reshape(heads, 128) for i in range(columns)]
        rope = q_all[j, :, :, base + 4 * columns + lax.rem(sub, 2)].reshape(heads, 128)
        lane_half = lax.broadcasted_iota(jnp.int32, (heads, 128), 1) // ROPE_DIM
        cols.append(jnp.where(lane_half == sub // 2, rope, jnp.zeros_like(rope)))
        q = jnp.concatenate(cols, axis=1)
        limit = len_ref[(t * 2 + core) * nj + j]
        outs, lses = [], []
        for p in (0, 1):
            owner = me if p == 0 else sibling
            s = jnp.dot(q, page[slot, p], preferred_element_type=jnp.float32) * (QK_DIM ** -0.5)
            position = owner * page_len + lax.broadcasted_iota(jnp.int32, (1, page_len), 1)
            s = jnp.where(position < limit, s, -1e30)
            m = jnp.max(s, axis=1, keepdims=True)
            w = jnp.exp(s - m)
            l = jnp.sum(w, axis=1, keepdims=True)
            pv = lax.dot_general(w.astype(jnp.bfloat16), page[slot, p, :latent], (((1,), (1,)), ((), ())),
                                 preferred_element_type=jnp.float32)
            outs.append((pv * (1.0 / l)).astype(jnp.bfloat16).astype(jnp.float32))
            lses.append(m + jnp.log(l))
        top = jnp.maximum(lses[0], lses[1])
        both = top + jnp.log(jnp.exp(lses[0] - top) + jnp.exp(lses[1] - top))
        part[j, t // side, lax.rem(t, side)] = jnp.exp(lses[0] - both) * outs[0] + jnp.exp(lses[1] - both) * outs[1]
        row = jnp.broadcast_to(both, (heads, 128)).T
        lse_x[j, 0, pl.ds(t, 1), :] = row[0:1]

    def combine(v):
        top = jnp.max(v, axis=0)
        return top + jnp.log(jnp.sum(jnp.exp(v - top[None]), axis=0))

    def lse_turn(j):
        lse_wait(j, 0)
        lse_y[j, 0] = combine(lse_x[j])
        lse_send(j, 1)

    def weigh(j):
        lse_wait(j, 1)
        wgt[...] = jnp.exp(lse_x[j, 0] - combine(lse_y[j]))

        def body(t, _):
            w = jnp.broadcast_to(wgt[pl.ds(t, 1), :], (128, heads)).T
            yy, xx = t // side, lax.rem(t, side)
            for i in range(latent // 128):
                cols = pl.ds(i * 128, 128)
                part[j, yy, xx, :, cols] = part[j, yy, xx, :, cols] * w
            return 0

        lax.fori_loop(0, nt, body, 0)

    def reduce_turn(r, axis):
        for idx, dest, rng, nxt, sem in ((0, 1, LOW, 4, 0), (2, -1, HIGH, 5, 1)):
            reduce_wait(r, axis, sem)
            for half in (0, 1):
                if axis == FIRST:
                    def body(i, _):
                        ref = first_part(r, half, dest, rng, i)
                        ref[...] = ref[...] + xbuf[r, half, idx, i]
                        return 0
                    lax.fori_loop(0, side, body, 0)
                else:
                    ref = second_part(r, half, dest, rng)
                    ref[...] = ref[...] + ybuf[r, half, idx]
            reduce_send(r, axis, nxt)

    def reduce_end(r, axis):
        reduce_wait(r, axis, 2)
        for half in (0, 1):
            for rng, one, two in ((HIGH, 1, 5), (LOW, 3, 4)):
                if axis == FIRST:
                    def body(i, _):
                        ref = first_part(r, half, 0, rng, i)
                        ref[...] = ref[...] + (xbuf[r, half, one, i] + xbuf[r, half, two, i])
                        return 0
                    lax.fori_loop(0, side, body, 0)
                else:
                    total = second_part(r, half, 0, rng)[...] + (ybuf[r, half, one] + ybuf[r, half, two])
                    out_ref[r, pl.ds(rows_of(half, rng), quarter_h)] = total.astype(out_ref.dtype)

    PIECES = ((2,), (1, -1), (0,))

    def row_of(half, step):
        return wrap(ypos if half == 0 else xpos, step)

    def last_turn(r):
        for sem in (0, 1):
            reduce_wait(r, FIRST, sem)
        for n, piece in enumerate(PIECES):
            for step in piece:
                for lane, (idx, dest, rng, nxt) in enumerate(((0, 1, LOW, 4), (2, -1, HIGH, 5))):
                    for half in (0, 1):
                        i = row_of(half, step)
                        ref = first_part(r, half, dest, rng, i)
                        ref[...] = ref[...] + xbuf[r, half, idx, i]
                        remote(ref, xbuf.at[r, half, nxt, i], rs_send.at[r, FIRST], last_recv.at[lane, n],
                               neighbour(FIRST, half, REDUCE[nxt][2])).start()

    def last_piece(r, n):
        if n == 0:
            wait_bytes(xbuf.at[r, 0, pl.ds(0, 4)], rs_recv.at[r, FIRST, 2])
        for lane in (0, 1):
            wait_bytes(xbuf.at[r, 0, 0, pl.ds(0, 2 * len(PIECES[n]))], last_recv.at[lane, n])
        for half in (0, 1):
            for step in PIECES[n]:
                i = row_of(half, step)
                for rng, one, two in ((HIGH, 1, 5), (LOW, 3, 4)):
                    ref = first_part(r, half, 0, rng, i)
                    ref[...] = ref[...] + (xbuf[r, half, one, i] + xbuf[r, half, two, i])
        if n < 2:
            reduce_send(r, SECOND, *((0, 2), (1, 3))[n])

    barrier = pltpu.get_barrier_semaphore()
    peers = [sibling] + [neighbour(axis, 0, step) for axis in (0, 1) for step in (1, -1, 2)]
    for dev in peers:
        pl.semaphore_signal(barrier, inc=1, device_id=peer(dev), device_id_type=pl.DeviceIdType.MESH)
    with jax.named_scope('barrier'):
        pl.semaphore_wait(barrier, len(peers))

    query_swap().start()
    with jax.named_scope('merge0'):
        query_swap().wait_recv()
        merge_queries(0)
    gather_send(0, 0, 1, 4, 8)
    swap_piece(0, 0)
    swap_piece(0, 1)
    with jax.named_scope('merges'):
        lax.fori_loop(1, nj, lambda j, _: (merge_queries(j), 0)[1], 0)
    with jax.named_scope('chunk0'):
        gather_first(0)
        swap_piece(0, 2)
        gather_second(0, 3, 12)
        gather_turn(0)
        gather_send(1, 0, 1)
        swap_piece(0, 3)
        gather_second(0, 4, 13)
        gather_second(0, 5, 14)
        gather_second(0, 6, 15)
    with jax.named_scope('chunk1'):
        swap_piece(1, 0)
        gather_first(1)
        gather_send(1, 4, 8)
        gather_send(2, 0, 1)
        swap_piece(1, 1)
        swap_wait(0)
        for n in range(DEPTH - 1):
            load_pages(n)
        gather_end(0)

    def run(*steps):
        for fn, *args in steps:
            with jax.named_scope(fn.__name__ + '_' + '_'.join(str(a) for a in args)):
                fn(*args)

    def middle(j):
        run((gather_turn, j), (gather_second, j, 4, 13), (gather_second, j, 5, 14), (gather_second, j, 3, 12))

    slots = {
        0: ((swap_piece, 1, 2),),
        1: ((gather_send, 2, 4, 8), (gather_send, 3, 0, 1), (swap_piece, 1, 3)),
        2: ((gather_turn, 1), (gather_second, 1, 4, 13), (gather_second, 1, 5, 14), (swap_piece, 2, 0)),
        3: ((gather_second, 1, 3, 12), (gather_first, 2), (swap_wait, 1), (swap_piece, 2, 1)),
        4: ((lse_send, 0, 0), (gather_second, 1, 6, 15), (gather_second, 2, 3, 12), (gather_send, 3, 4, 8), (gather_turn, 2),
            (gather_end, 1), (swap_piece, 2, 2)),
        5: ((lse_turn, 0), (gather_second, 2, 4, 13), (gather_second, 2, 5, 14), (gather_first, 3), (swap_piece, 2, 3)),
        6: ((gather_second, 2, 6, 15), (gather_second, 3, 3, 12), (weigh, 0), (reduce_send, 0, FIRST, 0, 2), (swap_piece, 3, 0)),
        7: ((gather_turn, 3), (gather_second, 3, 4, 13), (gather_second, 3, 5, 14), (swap_wait, 2), (swap_piece, 3, 1)),
        8: ((lse_send, 1, 0), (gather_end, 2), (swap_piece, 3, 2)),
        9: ((reduce_send, 0, FIRST, 1, 3), (swap_piece, 3, 3)),
        10: ((gather_second, 3, 6, 15),),
        11: ((lse_turn, 1), (reduce_turn, 0, FIRST), (swap_wait, 3)),
        12: ((lse_send, 2, 0), (gather_end, 3), (weigh, 1), (reduce_send, 1, FIRST, 0, 2)),
        14: ((lse_turn, 2), (reduce_send, 1, FIRST, 1, 3)),
    }

    def slot_body(n, _):
        for at, steps in slots.items():
            pl.when(n == at)(functools.partial(run, *steps))
        with jax.named_scope('attend'):
            lax.fori_loop(n * (nt // SLICES), (n + 1) * (nt // SLICES), lambda i, _: (attend(i), 0)[1], 0)
        return 0

    lax.fori_loop(0, nj * SLICES, slot_body, 0)

    early = (0, 2, 1, 3)
    run((lse_send, 3, 0), (reduce_end, 0, FIRST), (reduce_send, 0, SECOND, *early))
    run((reduce_turn, 1, FIRST), (reduce_turn, 0, SECOND), (lse_turn, 3), (weigh, 2), (reduce_send, 2, FIRST, *early),
        (reduce_end, 1, FIRST), (reduce_send, 1, SECOND, *early), (reduce_end, 0, SECOND))
    run((reduce_turn, 2, FIRST), (reduce_turn, 1, SECOND), (weigh, 3), (reduce_send, 3, FIRST, *early),
        (reduce_end, 2, FIRST), (reduce_send, 2, SECOND, *early), (reduce_end, 1, SECOND))
    run((last_turn, 3), (last_piece, 3, 0), (reduce_turn, 2, SECOND), (last_piece, 3, 1), (last_piece, 3, 2))
    run((reduce_turn, 3, SECOND), (reduce_end, 2, SECOND), (reduce_end, 3, SECOND))

    def drain(j, _):
        wait_bytes(sib_ref.at[j], swap_send.at[j])
        wait_bytes(q_all.at[j, :, :, pl.ds(0, 14 * tiles // 16)], ag_send.at[j, 0])
        wait_bytes(q_all.at[j, 0, 0], ag_send.at[j, 1])
        wait_bytes(xbuf.at[j], rs_send.at[j, 0])
        wait_bytes(ybuf.at[j], rs_send.at[j, 1])
        for axis in (0, 1):
            wait_bytes(lse_buf(axis).at[j, pl.ds(0, 3)], ls_send.at[j, axis])
        return 0

    with jax.named_scope('drain'):
        query_swap().wait_send()
        lax.fori_loop(0, nj, drain, 0)


def solution(mesh):
    group_size = mesh.shape[AXIS]
    side = math.isqrt(group_size // 2)
    nt = side * side

    def local_step(q_blk, cache_blk, len_blk):
        batch_rows, own_heads, width = q_blk.shape
        page_len = cache_blk.shape[3]
        latent = width - ROPE_DIM
        nj = batch_rows // group_size
        heads = 2 * own_heads * nt
        tiles = nt * (latent // 128) + nt // 2
        q = q_blk.reshape(nt, 2, nj, own_heads, width)
        cache = jnp.swapaxes(cache_blk.reshape(nt, 2, nj, page_len, width), 3, 4)
        any_space = pl.BlockSpec(memory_space=pl.ANY)
        dma = pltpu.SemaphoreType.DMA
        out, _ = pl.pallas_call(
            functools.partial(_kernel, side),
            out_shape=(jax.ShapeDtypeStruct((nj, heads, latent), jnp.bfloat16),
                       jax.ShapeDtypeStruct((nj, nt, width, page_len), jnp.bfloat16)),
            in_specs=[pl.BlockSpec(memory_space=pltpu.SMEM), pl.BlockSpec(memory_space=pltpu.VMEM), any_space],
            out_specs=(pl.BlockSpec(memory_space=pltpu.VMEM), any_space),
            scratch_shapes=[
                pltpu.VMEM((nt, nj, own_heads, width), jnp.bfloat16),
                pltpu.VMEM((nj, side, side, tiles, 2 * own_heads, 128), jnp.bfloat16),
                pltpu.VMEM((nj, side, side, heads, latent), jnp.float32),
                pltpu.VMEM((DEPTH, 2, width + ROPE_DIM, page_len), jnp.bfloat16),
                pltpu.VMEM((nj, 2, len(REDUCE), side, heads // 4, latent), jnp.float32),
                pltpu.VMEM((nj, 2, len(REDUCE), heads // 4, latent), jnp.float32),
                pltpu.VMEM((nj, 4, nt, heads), jnp.float32),
                pltpu.VMEM((nj, 4, nt, heads), jnp.float32),
                pltpu.VMEM((nt, heads), jnp.float32),
                dma((DEPTH, 2)), dma((nj,)), dma((nj,)), dma(()), dma(()),
                dma((nj, 2)), dma((nj, 8)), dma((nj, 2)), dma((nj, 2, 3)), dma((2, 3)), dma((nj, 2)), dma((nj, 2)),
            ],
            compiler_params=pltpu.CompilerParams(collective_id=0, has_side_effects=True, vmem_limit_bytes=54_000_000),
        )(len_blk, q, cache)
        return out

    return jax.shard_map(local_step, mesh=mesh, in_specs=(P('dp', AXIS, None), P('dp', None, AXIS, None, None), P('dp')),
                         out_specs=P(('dp', AXIS), None, None), check_vma=False)
```

```python
import functools
import math

import jax
import jax.numpy as jnp
from jax import lax
from jax.experimental import pallas as pl
from jax.experimental.pallas import tpu as pltpu
from jax.sharding import PartitionSpec as P

ROPE_DIM = 64
QK_DIM = 192
AXIS = 'dcp'
DEPTH = 3
SLICES = 4

FIRST, SECOND = 0, 1
FULL, LOW, HIGH = 0, 1, 2
GATHER = (
    (FIRST, 1, (0, 0), FULL, 0),
    (FIRST, -1, (0, 0), FULL, 1),
    (FIRST, 1, (-1, 0), LOW, 2),
    (FIRST, -1, (1, 0), HIGH, 2),
    (SECOND, 1, (0, 0), FULL, 3),
    (SECOND, 1, (-1, 0), FULL, 4),
    (SECOND, 1, (1, 0), FULL, 7),
    (SECOND, 1, (2, 0), FULL, 7),
    (SECOND, -1, (0, 0), FULL, 7),
    (SECOND, -1, (-1, 0), FULL, 7),
    (SECOND, -1, (1, 0), FULL, 5),
    (SECOND, -1, (2, 0), FULL, 6),
    (SECOND, 1, (0, -1), FULL, 7),
    (SECOND, 1, (-1, -1), FULL, 7),
    (SECOND, -1, (1, 1), FULL, 7),
    (SECOND, -1, (2, 1), FULL, 7),
)
REDUCE = ((2, LOW, 1, 0), (1, HIGH, 1, 2), (2, HIGH, -1, 1), (-1, LOW, -1, 2), (1, LOW, 1, 2), (-1, HIGH, -1, 2))


def _kernel(side, len_ref, q_ref, cache_ref, out_ref, sib_ref, q_sib, q_all, part, page, xbuf, ybuf, lse_x, lse_y,
            wgt, page_sem, swap_send, swap_recv, qs_send, qs_recv, ag_send, ag_recv, rs_send, rs_recv, last_recv, ls_send,
            ls_recv):
    nt, nj, own_heads, width = q_sib.shape
    heads, latent = part.shape[3:]
    page_len = page.shape[3]
    half_h, quarter_h = heads // 2, heads // 4
    tiles = q_all.shape[3]
    quarter_q, half_q = tiles // 4, tiles // 2
    columns = latent // 128

    me = lax.axis_index(AXIS)
    core = lax.rem(me, 2)
    xpos = lax.rem(me // 2, side)
    ypos = me // (2 * side)
    sibling = me + 1 - 2 * core

    def wrap(pos, step):
        return lax.rem(pos + (step + side), side)

    def neighbour(axis, half, step):
        if axis == half:
            return (ypos * side + wrap(xpos, step)) * 2 + core
        return (wrap(ypos, step) * side + xpos) * 2 + core

    def peer(dev):
        return {AXIS: dev}

    def remote(ref, dst, send_sem, recv_sem, dev):
        return pltpu.make_async_remote_copy(src_ref=ref, dst_ref=dst, send_sem=send_sem, recv_sem=recv_sem,
                                            device_id=peer(dev), device_id_type=pl.DeviceIdType.MESH)

    def gather_block(j, half, first, second, rng):
        if half == 0:
            yy, xx = wrap(ypos, second), wrap(xpos, first)
        else:
            yy, xx = wrap(ypos, first), wrap(xpos, second)
        start = half * half_q + (quarter_q if rng == HIGH else 0)
        return q_all.at[j, yy, xx, pl.ds(start, half_q if rng == FULL else quarter_q)]

    def gather_send(j, *indices):
        for idx in indices:
            for half in (0, 1):
                axis, step, (first, second), rng, sem = GATHER[idx]
                ref = gather_block(j, half, first, second, rng)
                remote(ref, ref, ag_send.at[0 if rng == FULL else 1], ag_recv.at[j, sem],
                       neighbour(axis, half, step)).start()

    def wait_bytes(ref, sem):
        pltpu.make_async_copy(ref, ref, sem).wait()

    def gather_wait(j, sem):
        wait_bytes(q_all.at[j, pl.ds(0, side // 2)] if sem == 7 else q_all.at[j, 0, 0], ag_recv.at[j, sem])

    def rows_of(half, rng):
        return half * half_h + (quarter_h if rng == HIGH else 0)

    def first_part(r, half, step, rng, i=None):
        hs = pl.ds(rows_of(half, rng), quarter_h)
        second = slice(None) if i is None else i
        if half == 0:
            return part.at[r, second, wrap(xpos, step), hs]
        return part.at[r, wrap(ypos, step), second, hs]

    def second_part(r, half, step, rng):
        hs = pl.ds(rows_of(half, rng), quarter_h)
        if half == 0:
            return part.at[r, wrap(ypos, step), xpos, hs]
        return part.at[r, ypos, wrap(xpos, step), hs]

    def reduce_send(r, axis, *indices):
        for idx in indices:
            for half in (0, 1):
                dest, rng, step, sem = REDUCE[idx]
                src = (first_part if axis == FIRST else second_part)(r, half, dest, rng)
                dst = (xbuf if axis == FIRST else ybuf).at[r, half, idx]
                remote(src, dst, rs_send.at[axis], rs_recv.at[r, axis, sem], neighbour(axis, half, step)).start()

    def reduce_wait(r, axis, sem):
        buf = xbuf if axis == FIRST else ybuf
        wait_bytes(buf.at[r, :, pl.ds(0, 4)] if sem == 2 else buf.at[r, 0, pl.ds(0, 2)], rs_recv.at[r, axis, sem])

    def lse_buf(axis):
        return lse_x if axis == 0 else lse_y

    def lse_send(j, axis):
        buf = lse_buf(axis)
        for idx, step in enumerate((1, -1, 2)):
            remote(buf.at[j, 0], buf.at[j, idx + 1], ls_send.at[axis], ls_recv.at[j, axis], neighbour(axis, 0, step)).start()

    def lse_wait(j, axis):
        wait_bytes(lse_buf(axis).at[j, pl.ds(0, 3)], ls_recv.at[j, axis])

    def swap_piece(j, n):
        ts = pl.ds(n * (nt // SLICES), nt // SLICES)
        remote(cache_ref.at[ts, 1 - core, j], sib_ref.at[j, ts], swap_send, swap_recv.at[j], sibling).start()

    def query_swap():
        return remote(q_ref.at[:, 1 - core], q_sib, qs_send, qs_recv, sibling)

    def load_pages(n):
        slot, j, t = lax.rem(n, DEPTH), n // nt, lax.rem(n, nt)
        for p, src in ((0, cache_ref.at[t, core, j]), (1, sib_ref.at[j, t])):
            pltpu.make_async_copy(src, page.at[slot, p, pl.ds(0, width)], page_sem.at[slot, p]).start()
            pltpu.make_async_copy(src.at[pl.ds(latent, ROPE_DIM)], page.at[slot, p, pl.ds(width, ROPE_DIM)],
                                  page_sem.at[slot, p]).start()

    def merge_queries(j):
        for t in range(nt):
            mine = q_ref[t, core, j].astype(jnp.float32)
            other = q_sib[t, j].astype(jnp.float32)
            both = jnp.concatenate([jnp.where(core == 0, mine, other), jnp.where(core == 0, other, mine)], axis=0)
            base, sub = (t // 4) * quarter_q, t % 4
            for i in range(columns):
                q_all[j, ypos, xpos, base + sub * columns + i] = both[:, i * 128:(i + 1) * 128].astype(jnp.bfloat16)
            rope = both[:, latent:]
            if sub < 2:
                low = (low if sub else []) + [rope]
            else:
                q_all[j, ypos, xpos, base + 4 * columns + sub - 2] = jnp.concatenate([low[sub - 2], rope], axis=1).astype(
                    jnp.bfloat16)

    def gather_first(j):
        for sem, sends in ((0, (2, 5, 9)), (1, (3, 6, 10))):
            gather_wait(j, sem)
            gather_send(j, *sends)

    def gather_turn(j):
        gather_wait(j, 2)
        gather_send(j, 7, 11)

    def gather_second(j, sem, send):
        gather_wait(j, sem)
        gather_send(j, send)

    def gather_end(j):
        gather_wait(j, 7)

    def swap_wait(j):
        wait_bytes(sib_ref.at[j], swap_recv.at[j])

    def attend(n):
        @pl.when(n + DEPTH - 1 < nj * nt)
        def _():
            load_pages(n + DEPTH - 1)

        slot, j, t = lax.rem(n, DEPTH), n // nt, lax.rem(n, nt)
        for p in (0, 1):
            wait_bytes(page.at[slot, p], page_sem.at[slot, p])
        base, sub = (t // 4) * quarter_q, lax.rem(t, 4)
        cols = [q_all[j, :, :, base + sub * columns + i].reshape(heads, 128) for i in range(columns)]
        rope = q_all[j, :, :, base + 4 * columns + lax.rem(sub, 2)].reshape(heads, 128)
        lane_half = lax.broadcasted_iota(jnp.int32, (heads, 128), 1) // ROPE_DIM
        cols.append(jnp.where(lane_half == sub // 2, rope, jnp.zeros_like(rope)))
        q = jnp.concatenate(cols, axis=1)
        limit = len_ref[(t * 2 + core) * nj + j]
        outs, lses = [], []
        for p in (0, 1):
            owner = me if p == 0 else sibling
            s = jnp.dot(q, page[slot, p], preferred_element_type=jnp.float32) * (QK_DIM ** -0.5)
            position = owner * page_len + lax.broadcasted_iota(jnp.int32, (1, page_len), 1)
            s = jnp.where(position < limit, s, -1e30)
            m = jnp.max(s, axis=1, keepdims=True)
            w = jnp.exp(s - m)
            l = jnp.sum(w, axis=1, keepdims=True)
            pv = lax.dot_general(w.astype(jnp.bfloat16), page[slot, p, :latent], (((1,), (1,)), ((), ())),
                                 preferred_element_type=jnp.float32)
            outs.append((pv * (1.0 / l)).astype(jnp.bfloat16).astype(jnp.float32))
            lses.append(m + jnp.log(l))
        top = jnp.maximum(lses[0], lses[1])
        both = top + jnp.log(jnp.exp(lses[0] - top) + jnp.exp(lses[1] - top))
        part[j, t // side, lax.rem(t, side)] = jnp.exp(lses[0] - both) * outs[0] + jnp.exp(lses[1] - both) * outs[1]
        row = jnp.broadcast_to(both, (heads, 128)).T
        lse_x[j, 0, pl.ds(t, 1), :] = row[0:1]

    def combine(v):
        top = jnp.max(v, axis=0)
        return top + jnp.log(jnp.sum(jnp.exp(v - top[None]), axis=0))

    def lse_turn(j):
        lse_wait(j, 0)
        lse_y[j, 0] = combine(lse_x[j])
        lse_send(j, 1)

    def weigh(j):
        lse_wait(j, 1)
        wgt[...] = jnp.exp(lse_x[j, 0] - combine(lse_y[j]))

        def body(t, _):
            w = jnp.broadcast_to(wgt[pl.ds(t, 1), :], (128, heads)).T
            yy, xx = t // side, lax.rem(t, side)
            for i in range(latent // 128):
                cols = pl.ds(i * 128, 128)
                part[j, yy, xx, :, cols] = part[j, yy, xx, :, cols] * w
            return 0

        lax.fori_loop(0, nt, body, 0)

    def reduce_turn(r, axis):
        for idx, dest, rng, nxt, sem in ((0, 1, LOW, 4, 0), (2, -1, HIGH, 5, 1)):
            reduce_wait(r, axis, sem)
            for half in (0, 1):
                if axis == FIRST:
                    def body(i, _):
                        ref = first_part(r, half, dest, rng, i)
                        ref[...] = ref[...] + xbuf[r, half, idx, i]
                        return 0
                    lax.fori_loop(0, side, body, 0)
                else:
                    ref = second_part(r, half, dest, rng)
                    ref[...] = ref[...] + ybuf[r, half, idx]
            reduce_send(r, axis, nxt)

    def reduce_end(r, axis):
        reduce_wait(r, axis, 2)
        for half in (0, 1):
            for rng, one, two in ((HIGH, 1, 5), (LOW, 3, 4)):
                if axis == FIRST:
                    def body(i, _):
                        ref = first_part(r, half, 0, rng, i)
                        ref[...] = ref[...] + (xbuf[r, half, one, i] + xbuf[r, half, two, i])
                        return 0
                    lax.fori_loop(0, side, body, 0)
                else:
                    total = second_part(r, half, 0, rng)[...] + (ybuf[r, half, one] + ybuf[r, half, two])
                    out_ref[r, pl.ds(rows_of(half, rng), quarter_h)] = total.astype(out_ref.dtype)

    PIECES = ((2,), (1, -1), (0,))

    def row_of(half, step):
        return wrap(ypos if half == 0 else xpos, step)

    def last_turn(r):
        for sem in (0, 1):
            reduce_wait(r, FIRST, sem)
        for n, piece in enumerate(PIECES):
            for step in piece:
                for lane, (idx, dest, rng, nxt) in enumerate(((0, 1, LOW, 4), (2, -1, HIGH, 5))):
                    for half in (0, 1):
                        i = row_of(half, step)
                        ref = first_part(r, half, dest, rng, i)
                        ref[...] = ref[...] + xbuf[r, half, idx, i]
                        remote(ref, xbuf.at[r, half, nxt, i], rs_send.at[FIRST], last_recv.at[lane, n],
                               neighbour(FIRST, half, REDUCE[nxt][2])).start()

    def last_piece(r, n):
        if n == 0:
            wait_bytes(xbuf.at[r, 0, pl.ds(0, 4)], rs_recv.at[r, FIRST, 2])
        for lane in (0, 1):
            wait_bytes(xbuf.at[r, 0, 0, pl.ds(0, 2 * len(PIECES[n]))], last_recv.at[lane, n])
        for half in (0, 1):
            for step in PIECES[n]:
                i = row_of(half, step)
                for rng, one, two in ((HIGH, 1, 5), (LOW, 3, 4)):
                    ref = first_part(r, half, 0, rng, i)
                    ref[...] = ref[...] + (xbuf[r, half, one, i] + xbuf[r, half, two, i])
        if n < 2:
            reduce_send(r, SECOND, *((0, 2), (1, 3))[n])

    barrier = pltpu.get_barrier_semaphore()
    peers = [sibling] + [neighbour(axis, 0, step) for axis in (0, 1) for step in (1, -1, 2)]
    for dev in peers:
        pl.semaphore_signal(barrier, inc=1, device_id=peer(dev), device_id_type=pl.DeviceIdType.MESH)
    with jax.named_scope('barrier'):
        pl.semaphore_wait(barrier, len(peers))

    query_swap().start()
    with jax.named_scope('merge0'):
        query_swap().wait_recv()
        merge_queries(0)
    gather_send(0, 0, 1, 4, 8)
    swap_piece(0, 0)
    swap_piece(0, 1)
    with jax.named_scope('merges'):
        lax.fori_loop(1, nj, lambda j, _: (merge_queries(j), 0)[1], 0)
    with jax.named_scope('chunk0'):
        gather_first(0)
        swap_piece(0, 2)
        gather_second(0, 3, 12)
        gather_turn(0)
        gather_send(1, 0, 1)
        swap_piece(0, 3)
        gather_second(0, 4, 13)
        gather_second(0, 5, 14)
        gather_second(0, 6, 15)
    with jax.named_scope('chunk1'):
        swap_piece(1, 0)
        gather_first(1)
        gather_send(1, 4, 8)
        gather_send(2, 0, 1)
        swap_piece(1, 1)
        swap_wait(0)
        for n in range(DEPTH - 1):
            load_pages(n)
        gather_end(0)

    def run(*steps):
        for fn, *args in steps:
            with jax.named_scope(fn.__name__ + '_' + '_'.join(str(a) for a in args)):
                fn(*args)

    def middle(j):
        run((gather_turn, j), (gather_second, j, 4, 13), (gather_second, j, 5, 14), (gather_second, j, 3, 12))

    slots = {
        0: ((swap_piece, 1, 2),),
        1: ((gather_send, 2, 4, 8), (gather_send, 3, 0, 1), (swap_piece, 1, 3)),
        2: ((gather_turn, 1), (gather_second, 1, 4, 13), (gather_second, 1, 5, 14), (swap_piece, 2, 0)),
        3: ((gather_second, 1, 3, 12), (gather_first, 2), (swap_wait, 1), (swap_piece, 2, 1)),
        4: ((lse_send, 0, 0), (gather_second, 1, 6, 15), (gather_second, 2, 3, 12), (gather_send, 3, 4, 8), (lse_turn, 0),
            (gather_turn, 2), (gather_end, 1), (gather_second, 2, 4, 13), (gather_second, 2, 5, 14), (gather_first, 3),
            (swap_piece, 2, 2)),
        5: ((gather_second, 2, 6, 15), (swap_piece, 2, 3)),
        6: ((gather_turn, 3), (gather_second, 3, 3, 12), (weigh, 0), (reduce_send, 0, FIRST, 0, 2), (swap_piece, 3, 0)),
        7: ((gather_second, 3, 4, 13), (gather_second, 3, 5, 14), (swap_wait, 2), (swap_piece, 3, 1)),
        8: ((lse_send, 1, 0), (gather_second, 3, 6, 15), (gather_end, 2), (swap_piece, 3, 2)),
        9: ((reduce_send, 0, FIRST, 1, 3), (swap_piece, 3, 3)),
        11: ((lse_turn, 1), (reduce_turn, 0, FIRST), (swap_wait, 3)),
        12: ((lse_send, 2, 0), (gather_end, 3)),
        13: ((weigh, 1), (reduce_send, 1, FIRST, 0, 2)),
        14: ((lse_turn, 2),),
        15: ((reduce_send, 1, FIRST, 1, 3),),
    }

    def slot_body(n, _):
        for at, steps in slots.items():
            pl.when(n == at)(functools.partial(run, *steps))
        with jax.named_scope('attend'):
            lax.fori_loop(n * (nt // SLICES), (n + 1) * (nt // SLICES), lambda i, _: (attend(i), 0)[1], 0)
        return 0

    lax.fori_loop(0, nj * SLICES, slot_body, 0)

    early = (0, 2, 1, 3)
    run((lse_send, 3, 0), (reduce_end, 0, FIRST), (reduce_send, 0, SECOND, *early))
    run((reduce_turn, 1, FIRST), (reduce_turn, 0, SECOND), (lse_turn, 3), (weigh, 2), (reduce_send, 2, FIRST, *early),
        (reduce_end, 1, FIRST), (reduce_send, 1, SECOND, *early), (reduce_end, 0, SECOND))
    run((reduce_turn, 2, FIRST), (reduce_turn, 1, SECOND), (weigh, 3), (reduce_send, 3, FIRST, *early),
        (reduce_end, 2, FIRST), (reduce_send, 2, SECOND, *early), (reduce_end, 1, SECOND))
    run((last_turn, 3), (last_piece, 3, 0), (reduce_turn, 2, SECOND), (last_piece, 3, 1), (last_piece, 3, 2))
    run((reduce_turn, 3, SECOND), (reduce_end, 2, SECOND), (reduce_end, 3, SECOND))

    query_swap().wait_send()
    wait_bytes(sib_ref, swap_send)
    wait_bytes(q_all.at[:, :, :, pl.ds(0, 14 * tiles // 16)], ag_send.at[0])
    wait_bytes(q_all.at[:, 0, 0], ag_send.at[1])
    wait_bytes(xbuf, rs_send.at[0])
    wait_bytes(ybuf, rs_send.at[1])
    for axis in (0, 1):
        wait_bytes(lse_buf(axis).at[:, pl.ds(0, 3)], ls_send.at[axis])


def solution(mesh):
    group_size = mesh.shape[AXIS]
    side = math.isqrt(group_size // 2)
    nt = side * side

    def local_step(q_blk, cache_blk, len_blk):
        batch_rows, own_heads, width = q_blk.shape
        page_len = cache_blk.shape[3]
        latent = width - ROPE_DIM
        nj = batch_rows // group_size
        heads = 2 * own_heads * nt
        tiles = nt * (latent // 128) + nt // 2
        q = q_blk.reshape(nt, 2, nj, own_heads, width)
        cache = jnp.swapaxes(cache_blk.reshape(nt, 2, nj, page_len, width), 3, 4)
        any_space = pl.BlockSpec(memory_space=pl.ANY)
        dma = pltpu.SemaphoreType.DMA
        out, _ = pl.pallas_call(
            functools.partial(_kernel, side),
            out_shape=(jax.ShapeDtypeStruct((nj, heads, latent), jnp.bfloat16),
                       jax.ShapeDtypeStruct((nj, nt, width, page_len), jnp.bfloat16)),
            in_specs=[pl.BlockSpec(memory_space=pltpu.SMEM), pl.BlockSpec(memory_space=pltpu.VMEM), any_space],
            out_specs=(pl.BlockSpec(memory_space=pltpu.VMEM), any_space),
            scratch_shapes=[
                pltpu.VMEM((nt, nj, own_heads, width), jnp.bfloat16),
                pltpu.VMEM((nj, side, side, tiles, 2 * own_heads, 128), jnp.bfloat16),
                pltpu.VMEM((nj, side, side, heads, latent), jnp.float32),
                pltpu.VMEM((DEPTH, 2, width + ROPE_DIM, page_len), jnp.bfloat16),
                pltpu.VMEM((nj, 2, len(REDUCE), side, heads // 4, latent), jnp.float32),
                pltpu.VMEM((nj, 2, len(REDUCE), heads // 4, latent), jnp.float32),
                pltpu.VMEM((nj, 4, nt, heads), jnp.float32),
                pltpu.VMEM((nj, 4, nt, heads), jnp.float32),
                pltpu.VMEM((nt, heads), jnp.float32),
                dma((DEPTH, 2)), dma(()), dma((nj,)), dma(()), dma(()),
                dma((2,)), dma((nj, 8)), dma((2,)), dma((nj, 2, 3)), dma((2, 3)), dma((2,)), dma((nj, 2)),
            ],
            compiler_params=pltpu.CompilerParams(collective_id=0, has_side_effects=True, vmem_limit_bytes=54_000_000),
        )(len_blk, q, cache)
        return out

    return jax.shard_map(local_step, mesh=mesh, in_specs=(P('dp', AXIS, None), P('dp', None, AXIS, None, None), P('dp')),
                         out_specs=P(('dp', AXIS), None, None), check_vma=False)
```
